256 devices in a mesh: dp: 4 (over z_lo, core), mp: 64 (over y, z_hi, x).
Axes of the slice: x: 4, y: 4, z: 8 (z_hi: 4, z_lo: 2; z = z_hi * 2 + z_lo), core: 2. Of those that a mesh axis runs over, the one named last changes fastest.
Arguments:
- attn_out: bfloat16 [512, 8192], P('dp', 'mp'), may hold values from -6 to 6
- residual: bfloat16 [512, 8192], P('dp', 'mp'), may hold values from -40 to 40
- output_weight: bfloat16 [8192, 8192], P('mp', 'dp'), may hold values from -0.0625 to 0.0625
- prune_mask: int32 [8192, 128], P('mp'), may hold values 0 or 1
- inverse_factor: float32 [128, 8192], P(None, 'dp'), may hold values from -2 to 2, as said below
- norm_gain: bfloat16 [8192], P('mp'), may hold values from 0.5 to 1.5
- gate_up_weight: bfloat16 [8192, 2, 14336], P('dp', None, 'mp'), may hold values from -0.0625 to 0.0625
Outputs:
- pruned_weight: bfloat16 [8192, 8192], P('mp', 'dp')
- stream: bfloat16 [512, 8192], P('dp', 'mp')
- hessian: float32 [14336, 14336], P('mp', 'dp')
The draws below stay inside these ranges and needn't reach their ends.
Inputs may be any that keep to these rules, and one draw needn't show every extreme that they name: inverse_factor is zero below its diagonal, and its diagonal lies between 0.5 and 2.
All inputs are finite; a program needn't handle non-finite values. No bound on the sum of `prune_mask` on one device may be relied on, other than what follows from the above.
Results may differ from the reference program's by a relative error of at most 0.012.
Values may be sent and summed in bfloat16 or wider, within the bound.
No kernel may reach another device: no remote copies, remote signals or barrier semaphores. Data moves between devices by JAX's collectives and lax.ppermute only.
A program may use at most 64 MiB of HBM per device.

```python
import math
import jax
import jax.numpy as jnp
from jax import lax

D = 8192
BLK = 128
TOKENS = 512
HU = 14336


def draw_residual(key, part):
    subkeys = jax.random.split(key, 3)
    row_scale = jnp.exp(jax.random.uniform(subkeys[0], (TOKENS, 1), jnp.float32, math.log(0.3), math.log(3.0)))
    rising = 0.6 + 1.2 * jnp.arange(D, dtype=jnp.float32)[None, :] / D
    ragged = jnp.exp(jax.random.uniform(subkeys[1], (1, D), jnp.float32, math.log(0.7), math.log(1.4)))
    sample = jnp.clip(jax.random.normal(subkeys[2], (TOKENS, D), jnp.float32), -5.0, 5.0)
    return (row_scale * rising * ragged * sample).astype(jnp.bfloat16)


def draw_inverse_factor(key, part):
    subkeys = jax.random.split(key, 2)
    pivots = jnp.exp(jax.random.uniform(subkeys[0], (BLK, 1), jnp.float32, math.log(0.5), math.log(2.0)))
    spread = jnp.clip(jax.random.normal(subkeys[1], (BLK, D), jnp.float32), -4.0, 4.0)
    spread = spread / math.sqrt(BLK)
    row_index = jnp.arange(BLK)[:, None]
    col_index = jnp.arange(D)[None, :]
    shaped = jnp.where(col_index == row_index, 1.0, jnp.where(col_index > row_index, spread, 0.0))
    return (pivots * shaped).astype(jnp.float32)


def with_ends(result, key, smallest, top_value):
    extent = result.shape
    index_at = [jax.random.randint(jax.random.fold_in(key, axis), (), 0, extent[axis]) for axis in range(len(extent))]
    result = result.at[tuple(index_at)].set(smallest)
    longest = extent.index(max(extent))
    index_at[longest] = (index_at[longest] + 1) % extent[longest]
    return result.at[tuple(index_at)].set(top_value)


def steps_of(rng, dims, pieces, least, top_value):
    factor_of = 1.0
    for axis_at, blocks in pieces:
        heights = jax.random.uniform(jax.random.fold_in(jax.random.fold_in(rng, 6), axis_at), (blocks,), jnp.float32, least / len(pieces), top_value / len(pieces))
        factor_of = factor_of * jnp.repeat(jnp.exp(heights), dims[axis_at] // blocks).reshape((-1,) + (1,) * (len(dims) - 1 - axis_at))
    return factor_of


def scatter_about(rng, shape, deviation, reach, pieces=(), kind=jnp.bfloat16):
    level = steps_of(rng, shape, pieces, -0.22, 0.18) if pieces else 1.0
    values = jax.random.normal(rng, shape, jnp.float32) * deviation * level
    return jnp.minimum(jnp.maximum(values, -reach), reach).astype(kind)


def setup_inputs(seed: int = 0) -> dict:
    splits = jax.random.split(jax.random.key(seed), 8)
    return {
        "attn_out": scatter_about(splits[0], (TOKENS, D), 1.0, 6.0, ((0, 4), (1, 64))),
        "residual": draw_residual(jax.random.fold_in(splits[7], 71), 0),
        "output_weight": scatter_about(splits[2], (D, D), D ** -0.5, 0.0625, ((0, 64), (1, 4))),
        "prune_mask": with_ends((jax.random.randint(splits[3], (D, BLK), 0, 2) < 1).astype(jnp.int32), jax.random.fold_in(splits[3], 1), 0, 1),
        "inverse_factor": draw_inverse_factor(jax.random.fold_in(splits[7], 71), 0),
        "norm_gain": jnp.clip(1.0 + 0.1 * jax.random.normal(splits[5], (D,), jnp.float32), 0.5, 1.5).astype(jnp.bfloat16),
        "gate_up_weight": scatter_about(splits[6], (D, 2, HU), D ** -0.5, 0.0625, ((0, 4), (2, 64))),
    }


def reference(attn_out, residual, output_weight, prune_mask, inverse_factor, norm_gain, gate_up_weight):
    width_block = prune_mask.shape[1]
    weights = output_weight.astype(jnp.float32)
    kept_mask = prune_mask.astype(jnp.float32)

    def advance(column, errors):
        place = column.astype(jnp.int32)
        factor_column = lax.dynamic_slice_in_dim(inverse_factor, place, 1, 1)[:, 0]
        current = lax.dynamic_slice_in_dim(weights, place, 1, 1)[:, 0] - jnp.dot(errors, factor_column, precision=lax.Precision.HIGHEST)
        mask_column = lax.dynamic_slice_in_dim(kept_mask, place, 1, 1)[:, 0]
        fresh = (1.0 - mask_column) / factor_column[place] * current
        return lax.dynamic_update_slice_in_dim(errors, fresh[:, None], place, 1)
    errors = lax.fori_loop(0, width_block, advance, jnp.zeros((weights.shape[0], width_block), jnp.float32))
    updated = weights - jnp.dot(errors, inverse_factor, precision=lax.Precision.HIGHEST, preferred_element_type=jnp.float32)
    leading = updated[:, :width_block] * kept_mask
    pruned_weight = jnp.concatenate([leading, updated[:, width_block:]], axis=1).astype(jnp.bfloat16)
    projected = jnp.dot(attn_out, pruned_weight.T, preferred_element_type=jnp.float32)
    stream = (residual.astype(jnp.float32) + projected).astype(jnp.bfloat16)
    stream_float = stream.astype(jnp.float32)
    inverse = lax.rsqrt(lax.optimization_barrier(jnp.mean(stream_float * stream_float, axis=1, keepdims=True)) + 1e-05)
    normed = (stream_float * inverse * norm_gain.astype(jnp.float32)[None, :]).astype(jnp.bfloat16)
    gate_part = jnp.dot(normed, gate_up_weight[:, 0, :], preferred_element_type=jnp.float32)
    up_part = jnp.dot(normed, gate_up_weight[:, 1, :], preferred_element_type=jnp.float32)
    hidden = (jax.nn.silu(gate_part) * up_part).astype(jnp.bfloat16)
    hessian = 2.0 / hidden.shape[0] * jnp.dot(hidden.T, hidden, preferred_element_type=jnp.float32)
    return (pruned_weight, stream, hessian)
```

```python
import jax
import jax.numpy as jnp
from jax import lax
from jax.experimental import pallas as pl
from jax.experimental.pallas import tpu as pltpu
from jax.sharding import Mesh
from jax.sharding import PartitionSpec as P

MP = ("mp_0", "mp_1", "mp_2")
NT = (((1,), (1,)), ((), ()))
VMEM = pl.BlockSpec(memory_space=pltpu.VMEM)
LANES = 128


def copy_for_each(x, axis):
    size = lax.axis_size(axis)
    return lax.all_to_all(jnp.broadcast_to(x[None], (size, *x.shape)), axis, 0, 0, tiled=True)


def turned(x):
    got = []
    for shift in range(4):
        pairs = []
        for d in range(4):
            for y in range(4):
                for z in range(4):
                    source = (d * 4 + y) * 4 + z
                    target = (y * 4 + d) * 4 + (z + shift) % 4
                    pairs.append((source, target))
        got.append(lax.ppermute(x, ("dp", "mp_0", "mp_1"), pairs))
    here = lax.axis_index("mp_1")
    ordered = []
    for z in range(4):
        shift = (here - z) % 4
        block = got[3]
        for k in range(3):
            block = jnp.where(shift == k, got[k], block)
        ordered.append(block)
    return jnp.stack(ordered)


def gathered(x):
    return copy_for_each(turned(x), ("mp_0", "mp_2"))


def solve_kernel(weight_ref, mask_ref, factor_ref, errors_ref):
    size = factor_ref.shape[0]
    step = 8
    count = size // step
    factor = factor_ref[...]
    row = lax.broadcasted_iota(jnp.int32, (size, size), 0)
    col = lax.broadcasted_iota(jnp.int32, (size, size), 1)
    pivots = jnp.sum(jnp.where(row == col, factor, 0.0), axis=1, keepdims=True)
    kept = mask_ref[...].astype(jnp.float32).T
    cutting = (1.0 - kept) / pivots
    current = weight_ref[...].astype(jnp.float32).T
    turned_factor = factor.T
    cur = [current[b * step : (b + 1) * step] for b in range(count)]
    fac = [turned_factor[b * step : (b + 1) * step] for b in range(count)]
    wide = (step, current.shape[1])
    place = lax.broadcasted_iota(jnp.int32, wide, 0)
    done = []
    for b in range(count):
        block = cur[b]
        cut_block = cutting[b * step : (b + 1) * step]
        fresh = []
        for i in range(step):
            j = b * step + i
            value = jnp.broadcast_to(cut_block[i : i + 1] * block[i : i + 1], wide)
            fresh.append(value)
            if i + 1 < step:
                reach = jnp.broadcast_to(fac[b][:, j : j + 1], wide)
                block = block - jnp.where(place > i, reach, 0.0) * value
        for v in range(b + 1, count):
            total = cur[v]
            for i in range(step):
                j = b * step + i
                total = total - jnp.broadcast_to(fac[v][:, j : j + 1], wide) * fresh[i]
            cur[v] = total
        rows = fresh[0]
        for i in range(1, step):
            rows = jnp.where(place == i, fresh[i], rows)
        done.append(rows)
    errors_ref[...] = jnp.concatenate(done, axis=0).T


def solved_errors(first_weight, mask, factor):
    return pl.pallas_call(
        solve_kernel,
        out_shape=jax.ShapeDtypeStruct(first_weight.shape, jnp.float32),
        in_specs=[VMEM] * 3,
        out_specs=VMEM,
        name="solve",
        cost_estimate=pl.CostEstimate(flops=20_000_000, bytes_accessed=300_000, transcendentals=0),
    )(first_weight, mask, factor)


def side_by_side(ref, y, rows):
    return jnp.concatenate(
        [ref[y * 4 + x, z, :rows, :] for z in range(4) for x in range(4)], axis=1
    )


def project_kernel(attn_ref, weight_ref, out_ref):
    weight = weight_ref[...]
    for y in range(4):
        tokens = side_by_side(attn_ref, y, LANES)
        out_ref[y] = lax.dot_general(
            tokens, weight, NT, preferred_element_type=jnp.float32
        ).astype(out_ref.dtype)


def gate_up_kernel(stream_ref, weight_ref, out_ref):
    weight = weight_ref[...]
    units = weight.shape[0]
    ones = jnp.ones((8, LANES), jnp.float32)
    for y in range(4):
        tokens = side_by_side(stream_ref, y, LANES)
        part = lax.dot_general(weight, tokens, NT, preferred_element_type=jnp.float32)
        wide = tokens.astype(jnp.float32)
        square = wide * wide
        folded = square[:, :LANES]
        for k in range(1, square.shape[1] // LANES):
            folded = folded + square[:, k * LANES : (k + 1) * LANES]
        total = lax.dot_general(
            ones, folded, NT, precision=lax.Precision.HIGHEST, preferred_element_type=jnp.float32
        )
        high = total.astype(jnp.bfloat16)
        low = (total - high.astype(jnp.float32)).astype(jnp.bfloat16)
        out_ref[y, :units, :] = part.astype(jnp.bfloat16)
        out_ref[y, units:, :] = jnp.concatenate([high, low], axis=0)


def hessian_kernel(rows_ref, columns_ref, out_ref):
    count = rows_ref.shape[1]
    left = jnp.concatenate([rows_ref[t] for t in range(4)], axis=1)
    scale = 2.0 / 512
    right = jnp.concatenate(
        [
            jnp.concatenate([columns_ref[y * 4 + x, 0] for x in range(4)], axis=0)
            for y in range(4)
        ],
        axis=1,
    )
    out_ref[...] = scale * lax.dot_general(left, right, NT, preferred_element_type=jnp.float32)


def body(attn_out, residual, output_weight, prune_mask, inverse_factor, norm_gain, gate_up_weight):
    width_block = prune_mask.shape[1]
    kept_mask = prune_mask.astype(jnp.float32)
    is_first = lax.axis_index("dp") == 0

    gain_rows = jnp.broadcast_to(norm_gain[None, :], (8, norm_gain.shape[0]))
    attn_all = gathered(jnp.concatenate([attn_out, gain_rows], axis=0))

    solved = solved_errors(
        output_weight[:, :width_block], prune_mask, inverse_factor[:, :width_block]
    )
    errors = lax.all_gather(solved, "dp")[0]
    weight_cols = output_weight.astype(jnp.float32)
    updated = weight_cols - jnp.dot(
        errors, inverse_factor, precision=lax.Precision.HIGHEST, preferred_element_type=jnp.float32
    )
    leading = jnp.where(is_first, updated[:, :width_block] * kept_mask, updated[:, :width_block])
    pruned_weight = lax.dynamic_update_slice_in_dim(updated, leading, 0, 1).astype(jnp.bfloat16)

    parts = pl.pallas_call(
        project_kernel,
        out_shape=jax.ShapeDtypeStruct((4, 128, 128), jnp.bfloat16),
        in_specs=[VMEM] * 2,
        out_specs=VMEM,
        name="project",
        cost_estimate=pl.CostEstimate(flops=268_000_000, bytes_accessed=2_700_000, transcendentals=0),
    )(attn_all, pruned_weight)
    parts = lax.all_to_all(parts, "dp", 0, 0, tiled=True)
    projected = jnp.sum(parts.astype(jnp.float32), axis=0)
    stream = (residual.astype(jnp.float32) + projected).astype(jnp.bfloat16)

    stream_all = gathered(stream)
    gain = attn_all[:4, :, 128, :].transpose(1, 0, 2).reshape(-1).astype(jnp.float32)
    units = gate_up_weight.shape[2]
    flat_weight = gate_up_weight.transpose(1, 2, 0).reshape(2 * units, -1)
    scaled_weight = (flat_weight.astype(jnp.float32) * gain[None, :]).astype(jnp.bfloat16)
    parts = pl.pallas_call(
        gate_up_kernel,
        out_shape=jax.ShapeDtypeStruct((4, 2 * units + 16, 128), jnp.bfloat16),
        in_specs=[VMEM] * 2,
        out_specs=VMEM,
        name="gate_up",
        cost_estimate=pl.CostEstimate(flops=940_000_000, bytes_accessed=4_300_000, transcendentals=0),
    )(stream_all, scaled_weight)
    parts = lax.all_to_all(parts, "dp", 0, 0, tiled=True)
    sums = jnp.sum(parts.astype(jnp.float32), axis=0)
    square = sums[2 * units : 2 * units + 1] + sums[2 * units + 8 : 2 * units + 9]
    inverse = lax.rsqrt(square / 8192 + 1e-05)
    gate_part = sums[:units] * inverse
    up_part = sums[units : 2 * units] * inverse
    hidden = (jax.nn.silu(gate_part) * up_part).astype(jnp.bfloat16)

    hidden_rows = lax.all_gather(hidden, "dp")
    hidden_columns = gathered(hidden)
    hessian = pl.pallas_call(
        hessian_kernel,
        grid=(4,),
        out_shape=jax.ShapeDtypeStruct((units, 16 * units), jnp.float32),
        in_specs=[
            pl.BlockSpec((4, units, 128), lambda z: (0, 0, 0)),
            pl.BlockSpec((16, 1, units, 128), lambda z: (0, z, 0, 0)),
        ],
        out_specs=pl.BlockSpec((units, 4 * units), lambda z: (0, z)),
        name="hessian",
        cost_estimate=pl.CostEstimate(flops=822_000_000, bytes_accessed=7_100_000, transcendentals=0),
    )(hidden_rows, hidden_columns)
    return (pruned_weight, stream, hessian)


def solution(mesh):
    split = Mesh(mesh.devices.reshape(mesh.shape["dp"], 4, 4, 4), ("dp", "mp_0", "mp_1", "mp_2"))
    return jax.shard_map(
        body,
        mesh=split,
        in_specs=(
            P("dp", MP),
            P("dp", MP),
            P(MP, "dp"),
            P(MP, None),
            P(None, "dp"),
            P(MP),
            P("dp", None, MP),
        ),
        out_specs=(P(MP, "dp"), P("dp", MP), P(MP, "dp")),
        check_vma=False,
    )
```

```python
import jax
import jax.numpy as jnp
from jax import lax
from jax.experimental import pallas as pl
from jax.experimental.pallas import tpu as pltpu
from jax.sharding import Mesh
from jax.sharding import PartitionSpec as P

DP = ("z_low", "core")
MP = ("y", "z_high", "x")
NT = (((1,), (1,)), ((), ()))
VMEM = pl.BlockSpec(memory_space=pltpu.VMEM)
SMEM = pl.BlockSpec(memory_space=pltpu.SMEM)
LANES = 128
STEPS = (1, 3, 2)


def params(mib):
    return pltpu.CompilerParams(vmem_limit_bytes=mib << 20)


def copy_for_each(x, axis):
    size = lax.axis_size(axis)
    return lax.all_to_all(jnp.broadcast_to(x[None], (size, *x.shape)), axis, 0, 0, tiled=True)


def turned(x):
    pairs = [(d * 4 + y, y * 4 + d) for d in range(4) for y in range(4)]
    return lax.ppermute(x, (*DP, "y"), pairs)


def round_x(x):
    return [x] + [
        lax.ppermute(x, "x", [(k, (k + step) % 4) for k in range(4)]) for step in STEPS
    ]


def over_y_and_x(x):
    half = x.shape[1] // 2
    lower = jnp.stack(round_x(x[:, half:]))
    upper = copy_for_each(x[:, :half], "y")
    return round_x(upper), copy_for_each(lower, "y")


def senders():
    here = lax.axis_index("x")
    return jnp.stack([here] + [(here + 4 - step) % 4 for step in STEPS]).astype(jnp.int32)


def solve_kernel(weight_ref, mask_ref, factor_ref, errors_ref):
    size = factor_ref.shape[0]
    step = 8
    count = size // step
    factor = factor_ref[...]
    row = lax.broadcasted_iota(jnp.int32, (size, size), 0)
    col = lax.broadcasted_iota(jnp.int32, (size, size), 1)
    pivots = jnp.sum(jnp.where(row == col, factor, 0.0), axis=1, keepdims=True)
    kept = mask_ref[...].astype(jnp.float32).T
    cutting = (1.0 - kept) / pivots
    current = weight_ref[...].astype(jnp.float32).T
    turned_factor = factor.T
    cur = [current[b * step : (b + 1) * step] for b in range(count)]
    fac = [turned_factor[b * step : (b + 1) * step] for b in range(count)]
    wide = (step, current.shape[1])
    place = lax.broadcasted_iota(jnp.int32, wide, 0)
    done = []
    for b in range(count):
        block = cur[b]
        cut_block = cutting[b * step : (b + 1) * step]
        fresh = []
        for i in range(step):
            j = b * step + i
            value = jnp.broadcast_to(cut_block[i : i + 1] * block[i : i + 1], wide)
            fresh.append(value)
            if i + 1 < step:
                reach = jnp.broadcast_to(fac[b][:, j : j + 1], wide)
                block = block - jnp.where(place > i, reach, 0.0) * value
        for v in range(b + 1, count):
            total = cur[v]
            for i in range(step):
                j = b * step + i
                total = total - jnp.broadcast_to(fac[v][:, j : j + 1], wide) * fresh[i]
            cur[v] = total
        rows = fresh[0]
        for i in range(1, step):
            rows = jnp.where(place == i, fresh[i], rows)
        done.append(rows)
    errors_ref[...] = jnp.concatenate(done, axis=0).T


def solved_errors(first_weight, mask, factor):
    return pl.pallas_call(
        solve_kernel,
        out_shape=jax.ShapeDtypeStruct(first_weight.shape, jnp.float32),
        in_specs=[VMEM] * 3,
        out_specs=VMEM,
        name="solve",
        compiler_params=params(8),
        cost_estimate=pl.CostEstimate(flops=20_000_000, bytes_accessed=300_000, transcendentals=0),
    )(first_weight, mask, factor)


def columns_at(ref, block):
    return ref[:, pl.ds(pl.multiple_of(block * LANES, LANES), LANES)]


def project_kernel(from_ref, a0, a1, a2, a3, lower_ref, weight_ref, out_ref):
    upper = (a0, a1, a2, a3)
    weight = jnp.concatenate(
        [columns_at(weight_ref, z * 4 + from_ref[r]) for r in range(4) for z in range(4)], axis=1
    )
    for y in range(4):
        high = jnp.concatenate([upper[r][y, z] for r in range(4) for z in range(4)], axis=1)
        low = jnp.concatenate([lower_ref[y, r, z] for r in range(4) for z in range(4)], axis=1)
        tokens = jnp.concatenate([high, low], axis=0)
        out_ref[y] = lax.dot_general(
            tokens, weight, NT, preferred_element_type=jnp.float32
        ).astype(out_ref.dtype)


def scale_kernel(from_ref, weight_ref, gain_ref, out_ref):
    for r in range(4):
        for z in range(4):
            block = z * 4 + from_ref[r]
            gain = gain_ref[block][:1].astype(jnp.float32)
            k = r * 4 + z
            out_ref[:, k * LANES : (k + 1) * LANES] = (
                columns_at(weight_ref, block).astype(jnp.float32) * gain
            ).astype(jnp.bfloat16)


def gate_up_kernel(core_ref, *refs):
    mine, other, weight_ref, out_ref = refs[:4], refs[4:8], refs[8], refs[9]
    weight = weight_ref[...]
    units = weight.shape[0]
    ones = jnp.ones((8, LANES), jnp.float32)
    for low in range(2):
        for source, core in ((mine, core_ref[0]), (other, 1 - core_ref[0])):
            tokens = jnp.concatenate(
                [source[r][z * 2 + low] for r in range(4) for z in range(4)], axis=1
            )
            part = lax.dot_general(weight, tokens, NT, preferred_element_type=jnp.float32)
            wide = tokens.astype(jnp.float32)
            square = wide * wide
            folded = square[:, :LANES]
            for k in range(1, square.shape[1] // LANES):
                folded = folded + square[:, k * LANES : (k + 1) * LANES]
            total = lax.dot_general(
                ones,
                folded,
                NT,
                precision=lax.Precision.HIGHEST,
                preferred_element_type=jnp.float32,
            )
            high = total.astype(jnp.bfloat16)
            rest = (total - high.astype(jnp.float32)).astype(jnp.bfloat16)
            group = low * 2 + core
            out_ref[group, :units, :] = part.astype(jnp.bfloat16)
            out_ref[group, units:, :] = jnp.concatenate([high, rest], axis=0)


def hessian_kernel(from_ref, rows_ref, a0, a1, a2, a3, lower_ref, out_ref, right_ref):
    upper = (a0, a1, a2, a3)
    units = rows_ref.shape[1]
    half = units // 2
    for r in range(4):
        base = from_ref[r] * units
        for y in range(4):
            lanes = slice(y * LANES, (y + 1) * LANES)
            right_ref[pl.ds(pl.multiple_of(base, 16), half), lanes] = upper[r][y, 0]
            right_ref[pl.ds(pl.multiple_of(base + half, 16), half), lanes] = lower_ref[y, r, 0]
    left = jnp.concatenate([rows_ref[t] for t in range(4)], axis=1)
    out_ref[...] = (2.0 / 512) * lax.dot_general(
        left, right_ref[...], NT, preferred_element_type=jnp.float32
    )


def body(attn_out, residual, output_weight, prune_mask, inverse_factor, norm_gain, gate_up_weight):
    width_block = prune_mask.shape[1]
    units = gate_up_weight.shape[2]
    kept_mask = prune_mask.astype(jnp.float32)
    is_first = (lax.axis_index("z_low") == 0) & (lax.axis_index("core") == 0)
    order = senders()
    core = lax.axis_index("core").astype(jnp.int32)[None]

    upper, lower = over_y_and_x(copy_for_each(turned(attn_out), "z_high"))
    flat_weight = turned(gate_up_weight.transpose(1, 2, 0).reshape(2 * units, -1))
    gains = copy_for_each(
        jnp.broadcast_to(norm_gain[None], (8, norm_gain.shape[0])), ("z_high", "x")
    )

    solved = solved_errors(
        output_weight[:, :width_block], prune_mask, inverse_factor[:, :width_block]
    )
    errors = lax.all_gather(solved, DP)[0]
    weight_cols = output_weight.astype(jnp.float32)
    updated = weight_cols - jnp.dot(
        errors, inverse_factor, precision=lax.Precision.HIGHEST, preferred_element_type=jnp.float32
    )
    leading = jnp.where(is_first, updated[:, :width_block] * kept_mask, updated[:, :width_block])
    pruned_weight = lax.dynamic_update_slice_in_dim(updated, leading, 0, 1).astype(jnp.bfloat16)

    parts = pl.pallas_call(
        project_kernel,
        out_shape=jax.ShapeDtypeStruct((4, 128, 128), jnp.bfloat16),
        in_specs=[SMEM] + [VMEM] * 6,
        out_specs=VMEM,
        name="project",
        compiler_params=params(24),
        cost_estimate=pl.CostEstimate(flops=268_000_000, bytes_accessed=2_700_000, transcendentals=0),
    )(order, *upper, lower, pruned_weight)
    parts = lax.all_to_all(parts, DP, 0, 0, tiled=True)
    projected = jnp.sum(parts.astype(jnp.float32), axis=0)
    stream = (residual.astype(jnp.float32) + projected).astype(jnp.bfloat16)

    scaled_weight = pl.pallas_call(
        scale_kernel,
        out_shape=jax.ShapeDtypeStruct(flat_weight.shape, jnp.bfloat16),
        in_specs=[SMEM] + [VMEM] * 2,
        out_specs=VMEM,
        name="scale",
        compiler_params=params(16),
        cost_estimate=pl.CostEstimate(flops=2_000_000, bytes_accessed=3_700_000, transcendentals=0),
    )(order, flat_weight, gains)
    mine = round_x(copy_for_each(stream, ("z_high", "z_low")))
    other = [lax.ppermute(block, "core", [(0, 1), (1, 0)]) for block in mine]
    parts = pl.pallas_call(
        gate_up_kernel,
        out_shape=jax.ShapeDtypeStruct((4, 2 * units + 16, 128), jnp.bfloat16),
        in_specs=[SMEM] + [VMEM] * 9,
        out_specs=VMEM,
        name="gate_up",
        compiler_params=params(24),
        cost_estimate=pl.CostEstimate(flops=940_000_000, bytes_accessed=4_300_000, transcendentals=0),
    )(core, *mine, *other, scaled_weight)
    parts = lax.all_to_all(parts, "y", 0, 0, tiled=True)
    sums = jnp.sum(parts.astype(jnp.float32), axis=0)
    square = sums[2 * units : 2 * units + 1] + sums[2 * units + 8 : 2 * units + 9]
    inverse = lax.rsqrt(square / 8192 + 1e-05)
    gate_part = sums[:units] * inverse
    up_part = sums[units : 2 * units] * inverse
    hidden = (jax.nn.silu(gate_part) * up_part).astype(jnp.bfloat16)

    upper, lower = over_y_and_x(copy_for_each(hidden, "z_high"))
    hidden_rows = lax.all_gather(turned(hidden), DP)
    piece = pl.BlockSpec((4, 1, units // 2, 128), lambda z: (0, z, 0, 0))
    hessian = pl.pallas_call(
        hessian_kernel,
        grid=(4,),
        out_shape=jax.ShapeDtypeStruct((units, 16 * units), jnp.float32),
        in_specs=[
            SMEM,
            pl.BlockSpec((4, units, 128), lambda z: (0, 0, 0)),
            *[piece] * 4,
            pl.BlockSpec((4, 4, 1, units // 2, 128), lambda z: (0, 0, z, 0, 0)),
        ],
        out_specs=pl.BlockSpec((units, 4 * units), lambda z: (0, z)),
        scratch_shapes=[pltpu.VMEM((4 * units, 4 * LANES), jnp.bfloat16)],
        name="hessian",
        compiler_params=params(24),
        cost_estimate=pl.CostEstimate(flops=822_000_000, bytes_accessed=7_100_000, transcendentals=0),
    )(order, hidden_rows, *upper, lower)
    return (pruned_weight, stream, hessian)


def solution(mesh):
    split = Mesh(mesh.devices.reshape(2, 2, 4, 4, 4), (*DP, *MP))
    return jax.shard_map(
        body,
        mesh=split,
        in_specs=(
            P(DP, MP),
            P(DP, MP),
            P(MP, DP),
            P(MP, None),
            P(None, DP),
            P(MP),
            P(DP, None, MP),
        ),
        out_specs=(P(MP, DP), P(DP, MP), P(MP, DP)),
        check_vma=False,
    )
```

```python
import jax
import jax.numpy as jnp
from jax import lax
from jax.experimental import pallas as pl
from jax.experimental.pallas import tpu as pltpu
from jax.sharding import Mesh
from jax.sharding import PartitionSpec as P


DP = ("z_low", "core")
MP = ("y", "z_high", "x")
NT = (((1,), (1,)), ((), ()))
VMEM = pl.BlockSpec(memory_space=pltpu.VMEM)
SMEM = pl.BlockSpec(memory_space=pltpu.SMEM)
LANES = 128
STEPS = (1, 3, 2)


def params(mib):
    return pltpu.CompilerParams(vmem_limit_bytes=mib << 20)


def copy_for_each(x, axis):
    size = lax.axis_size(axis)
    return lax.all_to_all(jnp.broadcast_to(x[None], (size, *x.shape)), axis, 0, 0, tiled=True)


def turned(x):
    pairs = [(d * 4 + y, y * 4 + d) for d in range(4) for y in range(4)]
    return lax.ppermute(x, (*DP, "y"), pairs)


def round_x(x):
    return [x] + [
        lax.ppermute(x, "x", [(k, (k + step) % 4) for k in range(4)]) for step in STEPS
    ]


def over_y_and_x(x):
    half = x.shape[1] // 2
    lower = jnp.stack(round_x(x[:, half:]))
    upper = copy_for_each(x[:, :half], "y")
    upper = round_x(upper)
    lower = copy_for_each(lower, "y")
    return upper, lower


def gathered_z(x):
    x = turned(x)
    return copy_for_each(x, "z_high")


def senders():
    here = lax.axis_index("x")
    return jnp.stack([here] + [(here + 4 - step) % 4 for step in STEPS]).astype(jnp.int32)


def solve_kernel(weight_ref, mask_ref, factor_ref, errors_ref):
    size = factor_ref.shape[0]
    step = 8
    count = size // step
    factor = factor_ref[...]
    row = lax.broadcasted_iota(jnp.int32, (size, size), 0)
    col = lax.broadcasted_iota(jnp.int32, (size, size), 1)
    pivots = jnp.sum(jnp.where(row == col, factor, 0.0), axis=1, keepdims=True)
    kept = mask_ref[...].astype(jnp.float32).T
    cutting = (1.0 - kept) / pivots
    current = weight_ref[...].astype(jnp.float32).T
    turned_factor = factor.T
    cur = [current[b * step : (b + 1) * step] for b in range(count)]
    fac = [turned_factor[b * step : (b + 1) * step] for b in range(count)]
    wide = (step, current.shape[1])
    place = lax.broadcasted_iota(jnp.int32, wide, 0)
    done = []
    for b in range(count):
        block = cur[b]
        cut_block = cutting[b * step : (b + 1) * step]
        fresh = []
        for i in range(step):
            j = b * step + i
            value = jnp.broadcast_to(cut_block[i : i + 1] * block[i : i + 1], wide)
            fresh.append(value)
            if i + 1 < step:
                reach = jnp.broadcast_to(fac[b][:, j : j + 1], wide)
                block = block - jnp.where(place > i, reach, 0.0) * value
        for v in range(b + 1, count):
            total = cur[v]
            for i in range(step):
                j = b * step + i
                total = total - jnp.broadcast_to(fac[v][:, j : j + 1], wide) * fresh[i]
            cur[v] = total
        rows = fresh[0]
        for i in range(1, step):
            rows = jnp.where(place == i, fresh[i], rows)
        done.append(rows)
    errors_ref[...] = jnp.concatenate(done, axis=0).T


def solved_errors(first_weight, mask, factor):
    return pl.pallas_call(
        solve_kernel,
        out_shape=jax.ShapeDtypeStruct(first_weight.shape, jnp.float32),
        in_specs=[VMEM] * 3,
        out_specs=VMEM,
        name="solve",
        compiler_params=params(8),
        cost_estimate=pl.CostEstimate(flops=20_000_000, bytes_accessed=300_000, transcendentals=0),
    )(first_weight, mask, factor)


def columns_at(ref, block):
    return ref[:, pl.ds(pl.multiple_of(block * LANES, LANES), LANES)]


def side_by_side(upper, lower_ref, y):
    high = jnp.concatenate([upper[r][y, z] for r in range(4) for z in range(4)], axis=1)
    low = jnp.concatenate([lower_ref[y, r, z] for r in range(4) for z in range(4)], axis=1)
    return jnp.concatenate([high, low], axis=0)


def project_kernel(from_ref, a0, a1, a2, a3, lower_ref, weight_ref, out_ref):
    upper = (a0, a1, a2, a3)
    weight = jnp.concatenate(
        [columns_at(weight_ref, z * 4 + from_ref[r]) for r in range(4) for z in range(4)], axis=1
    )
    for y in range(4):
        tokens = side_by_side(upper, lower_ref, y)
        out_ref[y] = lax.dot_general(
            tokens, weight, NT, preferred_element_type=jnp.float32
        )[:LANES].astype(out_ref.dtype)


def scale_kernel(from_ref, weight_ref, gain_ref, out_ref):
    for r in range(4):
        for z in range(4):
            gain = gain_ref[r, z, :1].astype(jnp.float32)
            k = r * 4 + z
            out_ref[:, k * LANES : (k + 1) * LANES] = (
                columns_at(weight_ref, z * 4 + from_ref[r]).astype(jnp.float32) * gain
            ).astype(jnp.bfloat16)


def gate_up_kernel(a0, a1, a2, a3, lower_ref, weight_ref, out_ref):
    weight = weight_ref[...]
    units = weight.shape[0]
    ones = jnp.ones((8, LANES), jnp.float32)
    for y in range(4):
        tokens = side_by_side((a0, a1, a2, a3), lower_ref, y)
        part = lax.dot_general(weight, tokens, NT, preferred_element_type=jnp.float32)
        wide = tokens.astype(jnp.float32)
        square = wide * wide
        folded = square[:, :LANES]
        for k in range(1, square.shape[1] // LANES):
            folded = folded + square[:, k * LANES : (k + 1) * LANES]
        total = lax.dot_general(
            ones, folded, NT, precision=lax.Precision.HIGHEST, preferred_element_type=jnp.float32
        )
        high = total.astype(jnp.bfloat16)
        rest = (total - high.astype(jnp.float32)).astype(jnp.bfloat16)
        out_ref[y, :units, :] = part.astype(jnp.bfloat16)
        out_ref[y, units:, :] = jnp.concatenate([high, rest], axis=0)


def hessian_kernel(from_ref, rows_ref, a0, a1, a2, a3, lower_ref, out_ref, right_ref):
    upper = (a0, a1, a2, a3)
    units = rows_ref.shape[1]
    half = units // 2
    for r in range(4):
        base = from_ref[r] * units
        for y in range(4):
            lanes = slice(y * LANES, (y + 1) * LANES)
            right_ref[pl.ds(pl.multiple_of(base, 16), half), lanes] = upper[r][y, 0]
            right_ref[pl.ds(pl.multiple_of(base + half, 16), half), lanes] = lower_ref[y, r, 0]
    left = jnp.concatenate([rows_ref[t] for t in range(4)], axis=1)
    out_ref[...] = (2.0 / 512) * lax.dot_general(
        left, right_ref[...], NT, preferred_element_type=jnp.float32
    )


def body(attn_out, residual, output_weight, prune_mask, inverse_factor, norm_gain, gate_up_weight):
    width_block = prune_mask.shape[1]
    units = gate_up_weight.shape[2]
    kept_mask = prune_mask.astype(jnp.float32)
    is_first = (lax.axis_index("z_low") == 0) & (lax.axis_index("core") == 0)
    order = senders()

    gain_rows = jnp.broadcast_to(norm_gain[None], (16, norm_gain.shape[0]))
    upper, lower = over_y_and_x(gathered_z(jnp.concatenate([attn_out, gain_rows], axis=0)))
    flat_weight = gate_up_weight.transpose(1, 2, 0).reshape(2 * units, -1)

    solved = solved_errors(
        output_weight[:, :width_block], prune_mask, inverse_factor[:, :width_block]
    )
    errors = lax.all_gather(solved, DP)[0]
    weight_cols = output_weight.astype(jnp.float32)
    updated = weight_cols - jnp.dot(
        errors, inverse_factor, precision=lax.Precision.HIGHEST, preferred_element_type=jnp.float32
    )
    leading = jnp.where(is_first, updated[:, :width_block] * kept_mask, updated[:, :width_block])
    pruned_weight = lax.dynamic_update_slice_in_dim(updated, leading, 0, 1).astype(jnp.bfloat16)

    parts = pl.pallas_call(
        project_kernel,
        out_shape=jax.ShapeDtypeStruct((4, 128, 128), jnp.bfloat16),
        in_specs=[SMEM] + [VMEM] * 6,
        out_specs=VMEM,
        name="project",
        compiler_params=params(10),
        cost_estimate=pl.CostEstimate(flops=268_000_000, bytes_accessed=2_700_000, transcendentals=0),
    )(order, *upper, lower, pruned_weight)
    parts = lax.all_to_all(parts, DP, 0, 0, tiled=True)
    projected = jnp.sum(parts.astype(jnp.float32), axis=0)
    stream = (residual.astype(jnp.float32) + projected).astype(jnp.bfloat16)

    gains = lower[0, :, :, -16:]
    scaled_weight = pl.pallas_call(
        scale_kernel,
        out_shape=jax.ShapeDtypeStruct(flat_weight.shape, jnp.bfloat16),
        in_specs=[SMEM] + [VMEM] * 2,
        out_specs=VMEM,
        name="scale",
        compiler_params=params(16),
        cost_estimate=pl.CostEstimate(flops=2_000_000, bytes_accessed=3_700_000, transcendentals=0),
    )(order, flat_weight, gains)
    upper, lower = over_y_and_x(gathered_z(stream))
    parts = pl.pallas_call(
        gate_up_kernel,
        out_shape=jax.ShapeDtypeStruct((4, 2 * units + 16, 128), jnp.bfloat16),
        in_specs=[VMEM] * 6,
        out_specs=VMEM,
        name="gate_up",
        compiler_params=params(14),
        cost_estimate=pl.CostEstimate(flops=940_000_000, bytes_accessed=4_300_000, transcendentals=0),
    )(*upper, lower, scaled_weight)
    parts = lax.all_to_all(parts, DP, 0, 0, tiled=True)
    sums = jnp.sum(parts.astype(jnp.float32), axis=0)
    square = sums[2 * units : 2 * units + 1] + sums[2 * units + 8 : 2 * units + 9]
    inverse = lax.rsqrt(square / 8192 + 1e-05)
    gate_part = sums[:units] * inverse
    up_part = sums[units : 2 * units] * inverse
    hidden = (jax.nn.silu(gate_part) * up_part).astype(jnp.bfloat16)

    upper, lower = over_y_and_x(gathered_z(hidden))
    hidden_rows = lax.all_gather(hidden, DP)
    piece = pl.BlockSpec((4, 1, units // 2, 128), lambda z: (0, z, 0, 0))
    hessian = pl.pallas_call(
        hessian_kernel,
        grid=(4,),
        out_shape=jax.ShapeDtypeStruct((units, 16 * units), jnp.float32),
        in_specs=[
            SMEM,
            pl.BlockSpec((4, units, 128), lambda z: (0, 0, 0)),
            *[piece] * 4,
            pl.BlockSpec((4, 4, 1, units // 2, 128), lambda z: (0, 0, z, 0, 0)),
        ],
        out_specs=pl.BlockSpec((units, 4 * units), lambda z: (0, z)),
        scratch_shapes=[pltpu.VMEM((4 * units, 4 * LANES), jnp.bfloat16)],
        name="hessian",
        compiler_params=params(14),
        cost_estimate=pl.CostEstimate(flops=822_000_000, bytes_accessed=7_100_000, transcendentals=0),
    )(order, hidden_rows, *upper, lower)
    return (pruned_weight, stream, hessian)


def solution(mesh):
    split = Mesh(mesh.devices.reshape(2, 2, 4, 4, 4), (*DP, *MP))
    return jax.shard_map(
        body,
        mesh=split,
        in_specs=(
            P(DP, MP),
            P(DP, MP),
            P(MP, DP),
            P(MP, None),
            P(None, DP),
            P(MP),
            P(DP, None, MP),
        ),
        out_specs=(P(MP, DP), P(DP, MP), P(MP, DP)),
        check_vma=False,
    )
```

```python
import jax
import jax.numpy as jnp
from jax import lax
from jax.experimental import pallas as pl
from jax.experimental.pallas import tpu as pltpu
from jax.sharding import Mesh
from jax.sharding import PartitionSpec as P


DP = ("z_low", "core")
MP = ("y", "z_high", "x")
NT = (((1,), (1,)), ((), ()))
VMEM = pl.BlockSpec(memory_space=pltpu.VMEM)
SMEM = pl.BlockSpec(memory_space=pltpu.SMEM)
LANES = 128
STEPS = (1, 3, 2)


def params(mib):
    return pltpu.CompilerParams(vmem_limit_bytes=mib << 20)


def copy_for_each(x, axis):
    size = lax.axis_size(axis)
    return lax.all_to_all(jnp.broadcast_to(x[None], (size, *x.shape)), axis, 0, 0, tiled=True)


def turned(x):
    pairs = [(d * 4 + y, y * 4 + d) for d in range(4) for y in range(4)]
    return lax.ppermute(x, (*DP, "y"), pairs)


def round_x(x):
    return [x] + [
        lax.ppermute(x, "x", [(k, (k + step) % 4) for k in range(4)]) for step in STEPS
    ]


def over_y_and_x(x, half):
    lower = jnp.stack(round_x(x[:, half:]))
    upper = copy_for_each(x[:, :half], "y")
    upper = round_x(upper)
    lower = copy_for_each(lower, "y")
    return upper, lower


def over_z(x):
    return copy_for_each(x, "z_high")


def senders():
    here = lax.axis_index("x")
    return jnp.stack([here] + [(here + 4 - step) % 4 for step in STEPS]).astype(jnp.int32)


def solve_kernel(weight_ref, mask_ref, factor_ref, errors_ref):
    size = factor_ref.shape[0]
    step = 8
    count = size // step
    factor = factor_ref[...]
    row = lax.broadcasted_iota(jnp.int32, (size, size), 0)
    col = lax.broadcasted_iota(jnp.int32, (size, size), 1)
    pivots = jnp.sum(jnp.where(row == col, factor, 0.0), axis=1, keepdims=True)
    kept = mask_ref[...].astype(jnp.float32).T
    cutting = (1.0 - kept) / pivots
    current = weight_ref[...].astype(jnp.float32).T
    turned_factor = factor.T
    cur = [current[b * step : (b + 1) * step] for b in range(count)]
    fac = [turned_factor[b * step : (b + 1) * step] for b in range(count)]
    wide = (step, current.shape[1])
    place = lax.broadcasted_iota(jnp.int32, wide, 0)
    done = []
    for b in range(count):
        block = cur[b]
        cut_block = cutting[b * step : (b + 1) * step]
        fresh = []
        for i in range(step):
            j = b * step + i
            value = jnp.broadcast_to(cut_block[i : i + 1] * block[i : i + 1], wide)
            fresh.append(value)
            if i + 1 < step:
                reach = jnp.broadcast_to(fac[b][:, j : j + 1], wide)
                block = block - jnp.where(place > i, reach, 0.0) * value
        for v in range(b + 1, count):
            total = cur[v]
            for i in range(step):
                j = b * step + i
                total = total - jnp.broadcast_to(fac[v][:, j : j + 1], wide) * fresh[i]
            cur[v] = total
        rows = fresh[0]
        for i in range(1, step):
            rows = jnp.where(place == i, fresh[i], rows)
        done.append(rows)
    errors_ref[...] = jnp.concatenate(done, axis=0).T


def solved_errors(first_weight, mask, factor):
    return pl.pallas_call(
        solve_kernel,
        out_shape=jax.ShapeDtypeStruct(first_weight.shape, jnp.float32),
        in_specs=[VMEM] * 3,
        out_specs=VMEM,
        name="solve",
        compiler_params=params(8),
        cost_estimate=pl.CostEstimate(flops=20_000_000, bytes_accessed=300_000, transcendentals=0),
    )(first_weight, mask, factor)


def columns_at(ref, block):
    return ref[:, pl.ds(pl.multiple_of(block * LANES, LANES), LANES)]


def ordered_columns(ref, from_ref):
    return jnp.concatenate(
        [columns_at(ref, z * 4 + from_ref[r]) for r in range(4) for z in range(4)], axis=1
    )


def project_kernel(from_ref, core_ref, *refs):
    mine, other, weight_ref, out_ref = refs[:4], refs[4:8], refs[8], refs[9]
    weight = ordered_columns(weight_ref, from_ref)
    for low in range(2):
        for source, core in ((mine, core_ref[0]), (other, 1 - core_ref[0])):
            tokens = jnp.concatenate(
                [source[r][z * 2 + low] for r in range(4) for z in range(4)], axis=1
            )
            out_ref[low * 2 + core] = lax.dot_general(
                tokens, weight, NT, preferred_element_type=jnp.float32
            ).astype(out_ref.dtype)


def stream_kernel(parts_ref, residual_ref, stream_ref, block_ref):
    rows = stream_ref.shape[0]
    total = residual_ref[:rows].astype(jnp.float32)
    for k in range(4):
        total = total + parts_ref[k].astype(jnp.float32)
    stream = total.astype(jnp.bfloat16)
    stream_ref[...] = stream
    wide = stream.astype(jnp.float32)
    gain = residual_ref[rows : rows + 16].astype(jnp.float32)[:1]
    square = lax.dot_general(
        jnp.ones((8, LANES), jnp.float32),
        wide * wide,
        NT,
        precision=lax.Precision.HIGHEST,
        preferred_element_type=jnp.float32,
    )
    high = square.astype(jnp.bfloat16).astype(jnp.float32)
    first = lax.broadcasted_iota(jnp.int32, square.shape, 0) == 0
    pair = jnp.where(first, high, square - high)
    block_ref[...] = jnp.concatenate([wide * gain, pair], axis=0).astype(jnp.bfloat16)


def gate_up_kernel(from_ref, a0, a1, a2, a3, lower_ref, weight_ref, out_ref):
    upper = (a0, a1, a2, a3)
    half = a0.shape[2]
    weight = ordered_columns(weight_ref, from_ref)
    units = weight.shape[0]
    places = [(r, z) for r in range(4) for z in range(4)]
    for y in range(4):
        high = jnp.concatenate([upper[r][y, z] for r, z in places], axis=1)
        low = jnp.concatenate([lower_ref[y, r, z, :half] for r, z in places], axis=1)
        part = lax.dot_general(
            weight,
            jnp.concatenate([high, low], axis=0),
            NT,
            preferred_element_type=jnp.float32,
        )
        square = jnp.zeros((8, LANES), jnp.float32)
        for r, z in places:
            square = square + lower_ref[y, r, z, half:].astype(jnp.float32)
        total = jnp.broadcast_to(square[0:1] + square[1:2], square.shape)
        big = total.astype(jnp.bfloat16)
        rest = (total - big.astype(jnp.float32)).astype(jnp.bfloat16)
        out_ref[y, :units, :] = part.astype(jnp.bfloat16)
        out_ref[y, units:, :] = jnp.concatenate([big, rest], axis=0)


def hessian_kernel(from_ref, rows_ref, a0, a1, a2, a3, lower_ref, out_ref, right_ref):
    upper = (a0, a1, a2, a3)
    units = rows_ref.shape[1]
    half = units // 2
    for r in range(4):
        base = from_ref[r] * units
        for y in range(4):
            lanes = slice(y * LANES, (y + 1) * LANES)
            right_ref[pl.ds(pl.multiple_of(base, 16), half), lanes] = upper[r][y, 0]
            right_ref[pl.ds(pl.multiple_of(base + half, 16), half), lanes] = lower_ref[y, r, 0]
    left = jnp.concatenate([rows_ref[t] for t in range(4)], axis=1)
    out_ref[...] = (2.0 / 512) * lax.dot_general(
        left, right_ref[...], NT, preferred_element_type=jnp.float32
    )


def body(attn_out, residual, output_weight, prune_mask, inverse_factor, norm_gain, gate_up_weight):
    width_block = prune_mask.shape[1]
    units = gate_up_weight.shape[2]
    kept_mask = prune_mask.astype(jnp.float32)
    is_first = (lax.axis_index("z_low") == 0) & (lax.axis_index("core") == 0)
    order = senders()
    core = lax.axis_index("core").astype(jnp.int32)[None]

    mine = copy_for_each(attn_out, ("z_high", "z_low"))
    mine = round_x(mine)
    other = [lax.ppermute(block, "core", [(0, 1), (1, 0)]) for block in mine]
    gain_rows = jnp.broadcast_to(norm_gain[None], (16, norm_gain.shape[0]))
    residual_turned = turned(jnp.concatenate([residual, gain_rows], axis=0))

    solved = solved_errors(
        output_weight[:, :width_block], prune_mask, inverse_factor[:, :width_block]
    )
    errors = lax.all_gather(solved, DP)[0]
    weight_cols = output_weight.astype(jnp.float32)
    updated = weight_cols - jnp.dot(
        errors,
        inverse_factor,
        precision=lax.Precision.HIGHEST,
        preferred_element_type=jnp.float32,
    )
    leading = jnp.where(is_first, updated[:, :width_block] * kept_mask, updated[:, :width_block])
    pruned_weight = lax.dynamic_update_slice_in_dim(updated, leading, 0, 1).astype(
        jnp.bfloat16
    )
    weight_turned = turned(pruned_weight)

    parts = pl.pallas_call(
        project_kernel,
        out_shape=jax.ShapeDtypeStruct((4, 128, 128), jnp.bfloat16),
        in_specs=[SMEM] * 2 + [VMEM] * 9,
        out_specs=VMEM,
        name="project",
        compiler_params=params(10),
        cost_estimate=pl.CostEstimate(flops=268_000_000, bytes_accessed=2_700_000, transcendentals=0),
    )(order, core, *mine, *other, weight_turned)
    parts = lax.all_to_all(parts, "y", 0, 0, tiled=True)
    stream_turned, block = pl.pallas_call(
        stream_kernel,
        out_shape=(
            jax.ShapeDtypeStruct((128, 128), jnp.bfloat16),
            jax.ShapeDtypeStruct((136, 128), jnp.bfloat16),
        ),
        in_specs=[VMEM] * 2,
        out_specs=[VMEM] * 2,
        name="stream",
        compiler_params=params(4),
        cost_estimate=pl.CostEstimate(flops=300_000, bytes_accessed=250_000, transcendentals=0),
    )(parts, residual_turned)
    stream = turned(stream_turned)

    flat_weight = gate_up_weight.transpose(1, 2, 0).reshape(2 * units, -1)
    upper, lower = over_y_and_x(over_z(block), 64)
    parts = pl.pallas_call(
        gate_up_kernel,
        out_shape=jax.ShapeDtypeStruct((4, 2 * units + 16, 128), jnp.bfloat16),
        in_specs=[SMEM] + [VMEM] * 6,
        out_specs=VMEM,
        name="gate_up",
        compiler_params=params(14),
        cost_estimate=pl.CostEstimate(flops=940_000_000, bytes_accessed=4_300_000, transcendentals=0),
    )(order, *upper, lower, flat_weight)
    parts = lax.all_to_all(parts, DP, 0, 0, tiled=True)
    sums = jnp.sum(parts.astype(jnp.float32), axis=0)
    square = sums[2 * units : 2 * units + 1] + sums[2 * units + 8 : 2 * units + 9]
    inverse = lax.rsqrt(square / 8192 + 1e-05)
    gate_part = sums[:units] * inverse
    up_part = sums[units : 2 * units] * inverse
    hidden = (jax.nn.silu(gate_part) * up_part).astype(jnp.bfloat16)

    hidden_turned = turned(hidden)
    upper, lower = over_y_and_x(over_z(hidden_turned), units // 2)
    hidden_rows = lax.all_gather(hidden, DP)
    piece = pl.BlockSpec((4, 1, units // 2, 128), lambda z: (0, z, 0, 0))
    hessian = pl.pallas_call(
        hessian_kernel,
        grid=(4,),
        out_shape=jax.ShapeDtypeStruct((units, 16 * units), jnp.float32),
        in_specs=[
            SMEM,
            pl.BlockSpec((4, units, 128), lambda z: (0, 0, 0)),
            *[piece] * 4,
            pl.BlockSpec((4, 4, 1, units // 2, 128), lambda z: (0, 0, z, 0, 0)),
        ],
        out_specs=pl.BlockSpec((units, 4 * units), lambda z: (0, z)),
        scratch_shapes=[pltpu.VMEM((4 * units, 4 * LANES), jnp.bfloat16)],
        name="hessian",
        compiler_params=params(14),
        cost_estimate=pl.CostEstimate(flops=822_000_000, bytes_accessed=7_100_000, transcendentals=0),
    )(order, hidden_rows, *upper, lower)
    return (pruned_weight, stream, hessian)


def solution(mesh):
    split = Mesh(mesh.devices.reshape(2, 2, 4, 4, 4), (*DP, *MP))
    return jax.shard_map(
        body,
        mesh=split,
        in_specs=(
            P(DP, MP),
            P(DP, MP),
            P(MP, DP),
            P(MP, None),
            P(None, DP),
            P(MP),
            P(DP, None, MP),
        ),
        out_specs=(P(MP, DP), P(DP, MP), P(MP, DP)),
        check_vma=False,
    )
```

```python
import jax
import jax.numpy as jnp
from jax import lax
from jax.experimental import pallas as pl
from jax.experimental.pallas import tpu as pltpu
from jax.sharding import Mesh
from jax.sharding import PartitionSpec as P


DP = ("z_low", "core")
MP = ("y", "z_high", "x")
NT = (((1,), (1,)), ((), ()))
VMEM = pl.BlockSpec(memory_space=pltpu.VMEM)
SMEM = pl.BlockSpec(memory_space=pltpu.SMEM)
LANES = 128
STEPS = (1, 3, 2)


def params(mib):
    return pltpu.CompilerParams(vmem_limit_bytes=mib << 20)


def copy_for_each(x, axis):
    size = lax.axis_size(axis)
    return lax.all_to_all(jnp.broadcast_to(x[None], (size, *x.shape)), axis, 0, 0, tiled=True)


def turned(x):
    pairs = [(d * 4 + y, y * 4 + d) for d in range(4) for y in range(4)]
    return lax.ppermute(x, (*DP, "y"), pairs)


def round_x(x):
    return [x] + [
        lax.ppermute(x, "x", [(k, (k + step) % 4) for k in range(4)]) for step in STEPS
    ]


def over_y_and_x(x, half):
    lower = jnp.stack(round_x(x[:, half:]))
    upper = copy_for_each(x[:, :half], "y")
    upper = round_x(upper)
    lower = copy_for_each(lower, "y")
    return upper, lower


def over_z(x):
    return copy_for_each(x, "z_high")


def senders():
    here = lax.axis_index("x")
    return jnp.stack([here] + [(here + 4 - step) % 4 for step in STEPS]).astype(jnp.int32)


def solve_kernel(weight_ref, mask_ref, factor_ref, errors_ref):
    size = factor_ref.shape[0]
    step = 8
    count = size // step
    factor = factor_ref[...]
    row = lax.broadcasted_iota(jnp.int32, (size, size), 0)
    col = lax.broadcasted_iota(jnp.int32, (size, size), 1)
    pivots = jnp.sum(jnp.where(row == col, factor, 0.0), axis=1, keepdims=True)
    kept = mask_ref[...].astype(jnp.float32).T
    cutting = (1.0 - kept) / pivots
    current = weight_ref[...].astype(jnp.float32).T
    turned_factor = factor.T
    cur = [current[b * step : (b + 1) * step] for b in range(count)]
    fac = [turned_factor[b * step : (b + 1) * step] for b in range(count)]
    wide = (step, current.shape[1])
    place = lax.broadcasted_iota(jnp.int32, wide, 0)
    done = []
    for b in range(count):
        block = cur[b]
        cut_block = cutting[b * step : (b + 1) * step]
        fresh = []
        for i in range(step):
            j = b * step + i
            value = jnp.broadcast_to(cut_block[i : i + 1] * block[i : i + 1], wide)
            fresh.append(value)
            if i + 1 < step:
                reach = jnp.broadcast_to(fac[b][:, j : j + 1], wide)
                block = block - jnp.where(place > i, reach, 0.0) * value
        for v in range(b + 1, count):
            total = cur[v]
            for i in range(step):
                j = b * step + i
                total = total - jnp.broadcast_to(fac[v][:, j : j + 1], wide) * fresh[i]
            cur[v] = total
        rows = fresh[0]
        for i in range(1, step):
            rows = jnp.where(place == i, fresh[i], rows)
        done.append(rows)
    errors_ref[...] = jnp.concatenate(done, axis=0).T


def corner(shape):
    return pl.BlockSpec(shape, lambda i: (0,) * len(shape))


def solved_errors(weight, mask, factor):
    block = corner(mask.shape)
    return pl.pallas_call(
        solve_kernel,
        grid=(1,),
        out_shape=jax.ShapeDtypeStruct(mask.shape, jnp.float32),
        in_specs=[block] * 3,
        out_specs=block,
        name="solve",
        compiler_params=params(8),
        cost_estimate=pl.CostEstimate(flops=20_000_000, bytes_accessed=300_000, transcendentals=0),
    )(weight, mask, factor)


def update_kernel(first_ref, errors_ref, factor_ref, weight_ref, mask_ref, out_ref):
    updated = weight_ref[...].astype(jnp.float32) - lax.dot_general(
        errors_ref[0],
        factor_ref[...],
        (((1,), (0,)), ((), ())),
        precision=lax.Precision.HIGHEST,
        preferred_element_type=jnp.float32,
    )
    width = mask_ref.shape[1]
    kept = jnp.where(first_ref[0] == 1, mask_ref[...].astype(jnp.float32), 1.0)
    out_ref[:, :width] = (updated[:, :width] * kept).astype(jnp.bfloat16)
    out_ref[:, width:] = updated[:, width:].astype(jnp.bfloat16)


def updated_weight(is_first, errors, factor, weight, mask):
    return pl.pallas_call(
        update_kernel,
        grid=(1,),
        out_shape=jax.ShapeDtypeStruct(weight.shape, jnp.bfloat16),
        in_specs=[
            SMEM,
            corner((1, *errors.shape[1:])),
            corner(factor.shape),
            corner(weight.shape),
            corner(mask.shape),
        ],
        out_specs=corner(weight.shape),
        name="update",
        compiler_params=params(12),
        cost_estimate=pl.CostEstimate(flops=400_000_000, bytes_accessed=2_200_000, transcendentals=0),
    )(is_first, errors, factor, weight, mask)


def columns_at(ref, block):
    return ref[:, pl.ds(pl.multiple_of(block * LANES, LANES), LANES)]


def ordered_columns(ref, from_ref):
    return jnp.concatenate(
        [columns_at(ref, z * 4 + from_ref[r]) for r in range(4) for z in range(4)], axis=1
    )


def project_kernel(from_ref, core_ref, *refs):
    mine, other, weight_ref, out_ref = refs[:4], refs[4:8], refs[8], refs[9]
    weight = ordered_columns(weight_ref, from_ref)
    for low in range(2):
        for source, core in ((mine, core_ref[0]), (other, 1 - core_ref[0])):
            tokens = jnp.concatenate(
                [source[r][z * 2 + low] for r in range(4) for z in range(4)], axis=1
            )
            out_ref[low * 2 + core] = lax.dot_general(
                tokens, weight, NT, preferred_element_type=jnp.float32
            ).astype(out_ref.dtype)


def stream_kernel(parts_ref, residual_ref, stream_ref, block_ref):
    rows = stream_ref.shape[0]
    total = residual_ref[:rows].astype(jnp.float32)
    for k in range(4):
        total = total + parts_ref[k].astype(jnp.float32)
    stream = total.astype(jnp.bfloat16)
    stream_ref[...] = stream
    wide = stream.astype(jnp.float32)
    gain = residual_ref[rows : rows + 16].astype(jnp.float32)[:1]
    square = lax.dot_general(
        jnp.ones((8, LANES), jnp.float32),
        wide * wide,
        NT,
        precision=lax.Precision.HIGHEST,
        preferred_element_type=jnp.float32,
    )
    high = square.astype(jnp.bfloat16).astype(jnp.float32)
    first = lax.broadcasted_iota(jnp.int32, square.shape, 0) == 0
    pair = jnp.where(first, high, square - high)
    block_ref[...] = jnp.concatenate([wide * gain, pair], axis=0).astype(jnp.bfloat16)


def copy_kernel(in_ref, out_ref):
    out_ref[...] = in_ref[...]


def order_kernel(from_ref, weight_ref, out_ref):
    out_ref[...] = ordered_columns(weight_ref, from_ref)


def gate_up_kernel(a0, a1, a2, a3, lower_ref, weight_ref, out_ref):
    upper = (a0, a1, a2, a3)
    half = a0.shape[2]
    weight = weight_ref[...]
    units = weight.shape[0]
    places = [(r, z) for r in range(4) for z in range(4)]
    for y in range(4):
        high = jnp.concatenate([upper[r][y, z] for r, z in places], axis=1)
        low = jnp.concatenate([lower_ref[y, r, z, :half] for r, z in places], axis=1)
        part = lax.dot_general(
            weight,
            jnp.concatenate([high, low], axis=0),
            NT,
            preferred_element_type=jnp.float32,
        )
        square = jnp.zeros((8, LANES), jnp.float32)
        for r, z in places:
            square = square + lower_ref[y, r, z, half:].astype(jnp.float32)
        total = jnp.broadcast_to(square[0:1] + square[1:2], square.shape)
        big = total.astype(jnp.bfloat16)
        rest = (total - big.astype(jnp.float32)).astype(jnp.bfloat16)
        out_ref[y, :units, :] = part.astype(jnp.bfloat16)
        out_ref[y, units:, :] = jnp.concatenate([big, rest], axis=0)


def hessian_kernel(from_ref, rows_ref, a0, a1, a2, a3, lower_ref, out_ref, right_ref):
    upper = (a0, a1, a2, a3)
    units = rows_ref.shape[1]
    half = units // 2
    for r in range(4):
        base = from_ref[r] * units
        for y in range(4):
            lanes = slice(y * LANES, (y + 1) * LANES)
            right_ref[pl.ds(pl.multiple_of(base, 16), half), lanes] = upper[r][y, 0]
            right_ref[pl.ds(pl.multiple_of(base + half, 16), half), lanes] = lower_ref[y, r, 0]
    left = jnp.concatenate([rows_ref[t] for t in range(4)], axis=1)
    out_ref[...] = (2.0 / 512) * lax.dot_general(
        left, right_ref[...], NT, preferred_element_type=jnp.float32
    )


def body(attn_out, residual, output_weight, prune_mask, inverse_factor, norm_gain, gate_up_weight):
    units = gate_up_weight.shape[2]
    is_first = (lax.axis_index(DP) == 0).astype(jnp.int32)[None]
    order = senders()
    core = lax.axis_index("core").astype(jnp.int32)[None]

    mine = copy_for_each(attn_out, ("z_high", "z_low"))
    mine = round_x(mine)
    other = [lax.ppermute(block, "core", [(0, 1), (1, 0)]) for block in mine]
    gain_rows = jnp.broadcast_to(norm_gain[None], (16, norm_gain.shape[0]))
    residual_turned = turned(jnp.concatenate([residual, gain_rows], axis=0))

    solved = solved_errors(output_weight, prune_mask, inverse_factor)
    errors = lax.all_gather(solved, DP)
    pruned_weight = updated_weight(is_first, errors, inverse_factor, output_weight, prune_mask)
    weight_turned = turned(pruned_weight)

    parts = pl.pallas_call(
        project_kernel,
        out_shape=jax.ShapeDtypeStruct((4, 128, 128), jnp.bfloat16),
        in_specs=[SMEM] * 2 + [VMEM] * 9,
        out_specs=VMEM,
        name="project",
        compiler_params=params(10),
        cost_estimate=pl.CostEstimate(flops=268_000_000, bytes_accessed=2_700_000, transcendentals=0),
    )(order, core, *mine, *other, weight_turned)
    parts = lax.all_to_all(parts, "y", 0, 0, tiled=True)
    stream_turned, block = pl.pallas_call(
        stream_kernel,
        out_shape=(
            jax.ShapeDtypeStruct((128, 128), jnp.bfloat16),
            jax.ShapeDtypeStruct((136, 128), jnp.bfloat16),
        ),
        in_specs=[VMEM] * 2,
        out_specs=[VMEM] * 2,
        name="stream",
        compiler_params=params(4),
        cost_estimate=pl.CostEstimate(flops=300_000, bytes_accessed=250_000, transcendentals=0),
    )(parts, residual_turned)
    stream = turned(stream_turned)
    stream = pl.pallas_call(
        copy_kernel,
        out_shape=jax.ShapeDtypeStruct(stream.shape, stream.dtype),
        in_specs=[VMEM],
        out_specs=VMEM,
        compiler_params=params(1),
    )(stream)

    flat_weight = gate_up_weight.transpose(1, 2, 0).reshape(2 * units, -1)
    flat_weight = pl.pallas_call(
        order_kernel,
        out_shape=jax.ShapeDtypeStruct(flat_weight.shape, jnp.bfloat16),
        in_specs=[SMEM, VMEM],
        out_specs=VMEM,
        name="order",
        compiler_params=params(8),
        cost_estimate=pl.CostEstimate(flops=0, bytes_accessed=3_700_000, transcendentals=0),
    )(order, flat_weight)
    upper, lower = over_y_and_x(over_z(block), 64)
    parts = pl.pallas_call(
        gate_up_kernel,
        out_shape=jax.ShapeDtypeStruct((4, 2 * units + 16, 128), jnp.bfloat16),
        in_specs=[VMEM] * 6,
        out_specs=VMEM,
        name="gate_up",
        compiler_params=params(14),
        cost_estimate=pl.CostEstimate(
            flops=940_000_000, bytes_accessed=4_300_000, transcendentals=0
        ),
    )(*upper, lower, flat_weight)
    parts = lax.all_to_all(parts, DP, 0, 0, tiled=True)
    sums = jnp.sum(parts.astype(jnp.float32), axis=0)
    square = sums[2 * units : 2 * units + 1] + sums[2 * units + 8 : 2 * units + 9]
    inverse = lax.rsqrt(square / 8192 + 1e-05)
    gate_part = sums[:units] * inverse
    up_part = sums[units : 2 * units] * inverse
    hidden = (jax.nn.silu(gate_part) * up_part).astype(jnp.bfloat16)

    hidden_turned = turned(hidden)
    upper, lower = over_y_and_x(over_z(hidden_turned), units // 2)
    hidden_rows = lax.all_gather(hidden, DP)
    piece = pl.BlockSpec((4, 1, units // 2, 128), lambda z: (0, z, 0, 0))
    hessian = pl.pallas_call(
        hessian_kernel,
        grid=(4,),
        out_shape=jax.ShapeDtypeStruct((units, 16 * units), jnp.float32),
        in_specs=[
            SMEM,
            pl.BlockSpec((4, units, 128), lambda z: (0, 0, 0)),
            *[piece] * 4,
            pl.BlockSpec((4, 4, 1, units // 2, 128), lambda z: (0, 0, z, 0, 0)),
        ],
        out_specs=pl.BlockSpec((units, 4 * units), lambda z: (0, z)),
        scratch_shapes=[pltpu.VMEM((4 * units, 4 * LANES), jnp.bfloat16)],
        name="hessian",
        compiler_params=params(14),
        cost_estimate=pl.CostEstimate(flops=822_000_000, bytes_accessed=7_100_000, transcendentals=0),
    )(order, hidden_rows, *upper, lower)
    return (pruned_weight, stream, hessian)


def solution(mesh):
    split = Mesh(mesh.devices.reshape(2, 2, 4, 4, 4), (*DP, *MP))
    return jax.shard_map(
        body,
        mesh=split,
        in_specs=(
            P(DP, MP),
            P(DP, MP),
            P(MP, DP),
            P(MP, None),
            P(None, DP),
            P(MP),
            P(DP, None, MP),
        ),
        out_specs=(P(MP, DP), P(DP, MP), P(MP, DP)),
        check_vma=False,
    )
```

```python
import jax
import jax.numpy as jnp
from jax import lax
from jax.experimental import pallas as pl
from jax.experimental.pallas import tpu as pltpu
from jax.sharding import Mesh
from jax.sharding import PartitionSpec as P


DP = ("z_low", "core")
MP = ("y", "z_high", "x")
NT = (((1,), (1,)), ((), ()))
VMEM = pl.BlockSpec(memory_space=pltpu.VMEM)
SMEM = pl.BlockSpec(memory_space=pltpu.SMEM)
LANES = 128
STEPS = (1, 3, 2)


def params(mib):
    return pltpu.CompilerParams(vmem_limit_bytes=mib << 20)


def copy_for_each(x, axis):
    size = lax.axis_size(axis)
    return lax.all_to_all(jnp.broadcast_to(x[None], (size, *x.shape)), axis, 0, 0, tiled=True)


def turned(x):
    pairs = [(d * 4 + y, y * 4 + d) for d in range(4) for y in range(4)]
    return lax.ppermute(x, (*DP, "y"), pairs)


def round_x(x):
    return [x] + [
        lax.ppermute(x, "x", [(k, (k + step) % 4) for k in range(4)]) for step in STEPS
    ]


def over_y_and_x(x, half):
    lower = jnp.stack(round_x(x[:, half:]))
    upper = copy_for_each(x[:, :half], "y")
    upper = round_x(upper)
    lower = copy_for_each(lower, "y")
    return upper, lower


def over_z(x):
    return copy_for_each(x, "z_high")


def senders():
    here = lax.axis_index("x")
    return jnp.stack([here] + [(here + 4 - step) % 4 for step in STEPS]).astype(jnp.int32)


def solve_kernel(weight_hbm, mask_hbm, factor_hbm, errors_ref, weight_ref, mask_ref, factor_ref, sems):
    size = factor_ref.shape[0]
    copies = [
        pltpu.make_async_copy(source.at[:, pl.ds(0, size)], target, sems.at[k])
        for k, (source, target) in enumerate(
            ((weight_hbm, weight_ref), (mask_hbm, mask_ref), (factor_hbm, factor_ref))
        )
    ]
    for copy in copies:
        copy.start()
    for copy in copies:
        copy.wait()
    step = 8
    count = size // step
    factor = factor_ref[...]
    row = lax.broadcasted_iota(jnp.int32, (size, size), 0)
    col = lax.broadcasted_iota(jnp.int32, (size, size), 1)
    pivots = jnp.sum(jnp.where(row == col, factor, 0.0), axis=1, keepdims=True)
    kept = mask_ref[...].astype(jnp.float32).T
    cutting = (1.0 - kept) / pivots
    current = weight_ref[...].astype(jnp.float32).T
    turned_factor = factor.T
    cur = [current[b * step : (b + 1) * step] for b in range(count)]
    fac = [turned_factor[b * step : (b + 1) * step] for b in range(count)]
    wide = (step, current.shape[1])
    place = lax.broadcasted_iota(jnp.int32, wide, 0)
    done = []
    for b in range(count):
        block = cur[b]
        cut_block = cutting[b * step : (b + 1) * step]
        fresh = []
        for i in range(step):
            j = b * step + i
            value = jnp.broadcast_to(cut_block[i : i + 1] * block[i : i + 1], wide)
            fresh.append(value)
            if i + 1 < step:
                reach = jnp.broadcast_to(fac[b][:, j : j + 1], wide)
                block = block - jnp.where(place > i, reach, 0.0) * value
        for v in range(b + 1, count):
            total = cur[v]
            for i in range(step):
                j = b * step + i
                total = total - jnp.broadcast_to(fac[v][:, j : j + 1], wide) * fresh[i]
            cur[v] = total
        rows = fresh[0]
        for i in range(1, step):
            rows = jnp.where(place == i, fresh[i], rows)
        done.append(rows)
    errors_ref[...] = jnp.concatenate(done, axis=0).T


def corner(shape):
    return pl.BlockSpec(shape, lambda i: (0,) * len(shape))


def solved_errors(weight, mask, factor):
    return pl.pallas_call(
        solve_kernel,
        out_shape=jax.ShapeDtypeStruct(mask.shape, jnp.float32),
        in_specs=[pl.BlockSpec(memory_space=pltpu.HBM)] * 3,
        out_specs=VMEM,
        scratch_shapes=[
            pltpu.VMEM(mask.shape, weight.dtype),
            pltpu.VMEM(mask.shape, mask.dtype),
            pltpu.VMEM(mask.shape, factor.dtype),
            pltpu.SemaphoreType.DMA((3,)),
        ],
        name="solve",
        compiler_params=params(60),
        cost_estimate=pl.CostEstimate(flops=20_000_000, bytes_accessed=300_000, transcendentals=0),
    )(weight, mask, factor)


def update_kernel(first_ref, errors_ref, factor_ref, weight_ref, mask_ref, out_ref):
    updated = weight_ref[...].astype(jnp.float32) - lax.dot_general(
        errors_ref[0],
        factor_ref[...],
        (((1,), (0,)), ((), ())),
        precision=lax.Precision.HIGHEST,
        preferred_element_type=jnp.float32,
    )
    width = mask_ref.shape[1]
    kept = jnp.where(first_ref[0] == 1, mask_ref[...].astype(jnp.float32), 1.0)
    out_ref[:, :width] = (updated[:, :width] * kept).astype(jnp.bfloat16)
    out_ref[:, width:] = updated[:, width:].astype(jnp.bfloat16)


def updated_weight(is_first, errors, factor, weight, mask):
    return pl.pallas_call(
        update_kernel,
        grid=(1,),
        out_shape=jax.ShapeDtypeStruct(weight.shape, jnp.bfloat16),
        in_specs=[
            SMEM,
            corner((1, *errors.shape[1:])),
            corner(factor.shape),
            corner(weight.shape),
            corner(mask.shape),
        ],
        out_specs=corner(weight.shape),
        name="update",
        compiler_params=params(12),
        cost_estimate=pl.CostEstimate(flops=400_000_000, bytes_accessed=2_200_000, transcendentals=0),
    )(is_first, errors, factor, weight, mask)


def columns_at(ref, block):
    return ref[:, pl.ds(pl.multiple_of(block * LANES, LANES), LANES)]


def ordered_columns(ref, from_ref):
    return jnp.concatenate(
        [columns_at(ref, z * 4 + from_ref[r]) for r in range(4) for z in range(4)], axis=1
    )


def project_kernel(from_ref, core_ref, *refs):
    mine, other, weight_ref, out_ref = refs[:4], refs[4:8], refs[8], refs[9]
    weight = ordered_columns(weight_ref, from_ref)
    for low in range(2):
        for source, core in ((mine, core_ref[0]), (other, 1 - core_ref[0])):
            tokens = jnp.concatenate(
                [source[r][z * 2 + low] for r in range(4) for z in range(4)], axis=1
            )
            out_ref[low * 2 + core] = lax.dot_general(
                tokens, weight, NT, preferred_element_type=jnp.float32
            ).astype(out_ref.dtype)


def stream_kernel(parts_ref, residual_ref, stream_ref, block_ref):
    rows = stream_ref.shape[0]
    total = residual_ref[:rows].astype(jnp.float32)
    for k in range(4):
        total = total + parts_ref[k].astype(jnp.float32)
    stream = total.astype(jnp.bfloat16)
    stream_ref[...] = stream
    wide = stream.astype(jnp.float32)
    gain = residual_ref[rows : rows + 16].astype(jnp.float32)[:1]
    square = lax.dot_general(
        jnp.ones((8, LANES), jnp.float32),
        wide * wide,
        NT,
        precision=lax.Precision.HIGHEST,
        preferred_element_type=jnp.float32,
    )
    high = square.astype(jnp.bfloat16).astype(jnp.float32)
    first = lax.broadcasted_iota(jnp.int32, square.shape, 0) == 0
    pair = jnp.where(first, high, square - high)
    block_ref[...] = jnp.concatenate([wide * gain, pair], axis=0).astype(jnp.bfloat16)


def copy_kernel(in_ref, out_ref):
    rows = out_ref.shape[0]
    out_ref[...] = in_ref[in_ref.shape[0] - rows :]


def order_kernel(from_ref, weight_ref, out_ref):
    out_ref[...] = ordered_columns(weight_ref, from_ref)


def gate_up_kernel(a0, a1, a2, a3, lower_ref, weight_ref, out_ref):
    upper = (a0, a1, a2, a3)
    half = a0.shape[2]
    weight = weight_ref[...]
    units = weight.shape[0]
    places = [(r, z) for r in range(4) for z in range(4)]
    for y in range(4):
        high = jnp.concatenate([upper[r][y, z] for r, z in places], axis=1)
        low = jnp.concatenate([lower_ref[y, r, z, :half] for r, z in places], axis=1)
        part = lax.dot_general(
            weight,
            jnp.concatenate([high, low], axis=0),
            NT,
            preferred_element_type=jnp.float32,
        )
        square = jnp.zeros((8, LANES), jnp.float32)
        for r, z in places:
            square = square + lower_ref[y, r, z, half:].astype(jnp.float32)
        total = jnp.broadcast_to(square[0:1] + square[1:2], square.shape)
        big = total.astype(jnp.bfloat16)
        rest = (total - big.astype(jnp.float32)).astype(jnp.bfloat16)
        out_ref[y, :units, :] = part.astype(jnp.bfloat16)
        out_ref[y, units:, :] = jnp.concatenate([big, rest], axis=0)


def hidden_kernel(parts_ref, stream_ref, hidden_ref, both_ref):
    units = hidden_ref.shape[0]
    sums = parts_ref[0].astype(jnp.float32)
    for k in range(1, 4):
        sums = sums + parts_ref[k].astype(jnp.float32)
    square = sums[2 * units : 2 * units + 8] + sums[2 * units + 8 :]
    inverse = lax.rsqrt(square / 8192 + 1e-05)[:1]
    gate = sums[:units] * inverse
    up = sums[units : 2 * units] * inverse
    hidden = (gate / (1.0 + jnp.exp(-gate)) * up).astype(jnp.bfloat16)
    hidden_ref[...] = hidden
    both_ref[:units] = hidden
    both_ref[units:] = stream_ref[...]


def hessian_kernel(from_ref, rows_ref, a0, a1, a2, a3, lower_ref, out_ref, right_ref):
    upper = (a0, a1, a2, a3)
    units = rows_ref.shape[1]
    half = units // 2
    for r in range(4):
        base = from_ref[r] * units
        for y in range(4):
            lanes = slice(y * LANES, (y + 1) * LANES)
            right_ref[pl.ds(pl.multiple_of(base, 16), half), lanes] = upper[r][y, 0]
            right_ref[pl.ds(pl.multiple_of(base + half, 16), half), lanes] = lower_ref[y, r, 0]
    left = jnp.concatenate([rows_ref[t] for t in range(4)], axis=1)
    out_ref[...] = (2.0 / 512) * lax.dot_general(
        left, right_ref[...], NT, preferred_element_type=jnp.float32
    )


def body(attn_out, residual, output_weight, prune_mask, inverse_factor, norm_gain, gate_up_weight):
    units = gate_up_weight.shape[2]
    is_first = (lax.axis_index(DP) == 0).astype(jnp.int32)[None]
    order = senders()
    core = lax.axis_index("core").astype(jnp.int32)[None]

    mine = copy_for_each(attn_out, ("z_high", "z_low"))
    mine = round_x(mine)
    other = [lax.ppermute(block, "core", [(0, 1), (1, 0)]) for block in mine]
    gain_rows = jnp.broadcast_to(norm_gain[None], (16, norm_gain.shape[0]))
    residual_turned = turned(jnp.concatenate([residual, gain_rows], axis=0))

    solved = solved_errors(output_weight, prune_mask, inverse_factor)
    errors = lax.all_gather(solved, DP)
    pruned_weight = updated_weight(is_first, errors, inverse_factor, output_weight, prune_mask)
    weight_turned = turned(pruned_weight)

    parts = pl.pallas_call(
        project_kernel,
        out_shape=jax.ShapeDtypeStruct((4, 128, 128), jnp.bfloat16),
        in_specs=[SMEM] * 2 + [VMEM] * 9,
        out_specs=VMEM,
        name="project",
        compiler_params=params(10),
        cost_estimate=pl.CostEstimate(flops=268_000_000, bytes_accessed=2_700_000, transcendentals=0),
    )(order, core, *mine, *other, weight_turned)
    parts = lax.all_to_all(parts, "y", 0, 0, tiled=True)
    stream_turned, block = pl.pallas_call(
        stream_kernel,
        out_shape=(
            jax.ShapeDtypeStruct((128, 128), jnp.bfloat16),
            jax.ShapeDtypeStruct((136, 128), jnp.bfloat16),
        ),
        in_specs=[VMEM] * 2,
        out_specs=[VMEM] * 2,
        name="stream",
        compiler_params=params(4),
        cost_estimate=pl.CostEstimate(flops=300_000, bytes_accessed=250_000, transcendentals=0),
    )(parts, residual_turned)
    flat_weight = gate_up_weight.transpose(1, 2, 0).reshape(2 * units, -1)
    flat_weight = pl.pallas_call(
        order_kernel,
        out_shape=jax.ShapeDtypeStruct(flat_weight.shape, jnp.bfloat16),
        in_specs=[SMEM, VMEM],
        out_specs=VMEM,
        name="order",
        compiler_params=params(8),
        cost_estimate=pl.CostEstimate(flops=0, bytes_accessed=3_700_000, transcendentals=0),
    )(order, flat_weight)
    upper, lower = over_y_and_x(over_z(block), 64)
    parts = pl.pallas_call(
        gate_up_kernel,
        out_shape=jax.ShapeDtypeStruct((4, 2 * units + 16, 128), jnp.bfloat16),
        in_specs=[VMEM] * 6,
        out_specs=VMEM,
        name="gate_up",
        compiler_params=params(14),
        cost_estimate=pl.CostEstimate(
            flops=940_000_000, bytes_accessed=4_300_000, transcendentals=0
        ),
    )(*upper, lower, flat_weight)
    parts = lax.all_to_all(parts, DP, 0, 0, tiled=True)
    hidden, both = pl.pallas_call(
        hidden_kernel,
        out_shape=(
            jax.ShapeDtypeStruct((units, 128), jnp.bfloat16),
            jax.ShapeDtypeStruct((units + 128, 128), jnp.bfloat16),
        ),
        in_specs=[VMEM] * 2,
        out_specs=[VMEM] * 2,
        name="hidden",
        compiler_params=params(6),
        cost_estimate=pl.CostEstimate(
            flops=1_000_000, bytes_accessed=700_000, transcendentals=60_000
        ),
    )(parts, stream_turned)

    both = turned(both)
    stream = pl.pallas_call(
        copy_kernel,
        out_shape=jax.ShapeDtypeStruct((128, 128), jnp.bfloat16),
        in_specs=[VMEM],
        out_specs=VMEM,
        compiler_params=params(1),
    )(both)
    hidden_turned = both[:units]
    upper, lower = over_y_and_x(over_z(hidden_turned), units // 2)
    hidden_rows = lax.all_gather(hidden, DP)
    piece = pl.BlockSpec((4, 1, units // 2, 128), lambda z: (0, z, 0, 0))
    hessian = pl.pallas_call(
        hessian_kernel,
        grid=(4,),
        out_shape=jax.ShapeDtypeStruct((units, 16 * units), jnp.float32),
        in_specs=[
            SMEM,
            pl.BlockSpec((4, units, 128), lambda z: (0, 0, 0)),
            *[piece] * 4,
            pl.BlockSpec((4, 4, 1, units // 2, 128), lambda z: (0, 0, z, 0, 0)),
        ],
        out_specs=pl.BlockSpec((units, 4 * units), lambda z: (0, z)),
        scratch_shapes=[pltpu.VMEM((4 * units, 4 * LANES), jnp.bfloat16)],
        name="hessian",
        compiler_params=params(14),
        cost_estimate=pl.CostEstimate(flops=822_000_000, bytes_accessed=7_100_000, transcendentals=0),
    )(order, hidden_rows, *upper, lower)
    return (pruned_weight, stream, hessian)


def solution(mesh):
    split = Mesh(mesh.devices.reshape(2, 2, 4, 4, 4), (*DP, *MP))
    return jax.shard_map(
        body,
        mesh=split,
        in_specs=(
            P(DP, MP),
            P(DP, MP),
            P(MP, DP),
            P(MP, None),
            P(None, DP),
            P(MP),
            P(DP, None, MP),
        ),
        out_specs=(P(MP, DP), P(DP, MP), P(MP, DP)),
        check_vma=False,
    )
```

```python
import jax
import jax.numpy as jnp
from jax import lax
from jax.experimental import pallas as pl
from jax.experimental.pallas import tpu as pltpu
from jax.sharding import Mesh
from jax.sharding import PartitionSpec as P


DP = ("z_low", "core")
MP = ("y", "z_high", "x")
NT = (((1,), (1,)), ((), ()))
VMEM = pl.BlockSpec(memory_space=pltpu.VMEM)
SMEM = pl.BlockSpec(memory_space=pltpu.SMEM)
LANES = 128
STEPS = (1, 3, 2)


def params(mib):
    return pltpu.CompilerParams(vmem_limit_bytes=mib << 20)


def copy_for_each(x, axis):
    size = lax.axis_size(axis)
    return lax.all_to_all(jnp.broadcast_to(x[None], (size, *x.shape)), axis, 0, 0, tiled=True)


def turned(x):
    pairs = [(d * 4 + y, y * 4 + d) for d in range(4) for y in range(4)]
    return lax.ppermute(x, (*DP, "y"), pairs)


def round_trip(x, axis):
    return [x] + [
        lax.ppermute(x, axis, [(k, (k + step) % 4) for k in range(4)]) for step in STEPS
    ]


def over_y_and_x(x, half):
    lower = jnp.stack(round_trip(x[:, half:], "x"))
    upper = jnp.stack(round_trip(x[:, :half], "y"))
    upper = round_trip(upper, "x")
    lower = round_trip(lower, "y")
    return upper, lower


def over_z(x):
    return copy_for_each(x, "z_high")


def senders(axis):
    here = lax.axis_index(axis)
    return jnp.stack([here] + [(here + 4 - step) % 4 for step in STEPS]).astype(jnp.int32)


def solve_kernel(weight_hbm, mask_hbm, factor_hbm, errors_ref, weight_ref, mask_ref, factor_ref, sems):
    size = factor_ref.shape[0]
    copies = [
        pltpu.make_async_copy(source.at[:, pl.ds(0, size)], target, sems.at[k])
        for k, (source, target) in enumerate(
            ((weight_hbm, weight_ref), (mask_hbm, mask_ref), (factor_hbm, factor_ref))
        )
    ]
    for copy in copies:
        copy.start()
    for copy in copies:
        copy.wait()
    step = 8
    count = size // step
    factor = factor_ref[...]
    row = lax.broadcasted_iota(jnp.int32, (size, size), 0)
    col = lax.broadcasted_iota(jnp.int32, (size, size), 1)
    pivots = jnp.sum(jnp.where(row == col, factor, 0.0), axis=1, keepdims=True)
    kept = mask_ref[...].astype(jnp.float32).T
    cutting = (1.0 - kept) / pivots
    current = weight_ref[...].astype(jnp.float32).T
    turned_factor = factor.T
    cur = [current[b * step : (b + 1) * step] for b in range(count)]
    fac = [turned_factor[b * step : (b + 1) * step] for b in range(count)]
    wide = (step, current.shape[1])
    place = lax.broadcasted_iota(jnp.int32, wide, 0)
    done = []
    for b in range(count):
        block = cur[b]
        cut_block = cutting[b * step : (b + 1) * step]
        fresh = []
        for i in range(step):
            j = b * step + i
            value = jnp.broadcast_to(cut_block[i : i + 1] * block[i : i + 1], wide)
            fresh.append(value)
            if i + 1 < step:
                reach = jnp.broadcast_to(fac[b][:, j : j + 1], wide)
                block = block - jnp.where(place > i, reach, 0.0) * value
        for v in range(b + 1, count):
            total = cur[v]
            for i in range(step):
                j = b * step + i
                total = total - jnp.broadcast_to(fac[v][:, j : j + 1], wide) * fresh[i]
            cur[v] = total
        rows = fresh[0]
        for i in range(1, step):
            rows = jnp.where(place == i, fresh[i], rows)
        done.append(rows)
    errors_ref[...] = jnp.concatenate(done, axis=0).T


def corner(shape):
    return pl.BlockSpec(shape, lambda i: (0,) * len(shape))


def solved_errors(weight, mask, factor):
    return pl.pallas_call(
        solve_kernel,
        out_shape=jax.ShapeDtypeStruct(mask.shape, jnp.float32),
        in_specs=[pl.BlockSpec(memory_space=pltpu.HBM)] * 3,
        out_specs=VMEM,
        scratch_shapes=[
            pltpu.VMEM(mask.shape, weight.dtype),
            pltpu.VMEM(mask.shape, mask.dtype),
            pltpu.VMEM(mask.shape, factor.dtype),
            pltpu.SemaphoreType.DMA((3,)),
        ],
        name="solve",
        compiler_params=params(60),
        cost_estimate=pl.CostEstimate(flops=20_000_000, bytes_accessed=300_000, transcendentals=0),
    )(weight, mask, factor)


def update_kernel(first_ref, errors_ref, factor_ref, weight_ref, mask_ref, out_ref):
    updated = weight_ref[...].astype(jnp.float32) - lax.dot_general(
        errors_ref[0],
        factor_ref[...],
        (((1,), (0,)), ((), ())),
        precision=lax.Precision.HIGHEST,
        preferred_element_type=jnp.float32,
    )
    width = mask_ref.shape[1]
    kept = jnp.where(first_ref[0] == 1, mask_ref[...].astype(jnp.float32), 1.0)
    out_ref[:, :width] = (updated[:, :width] * kept).astype(jnp.bfloat16)
    out_ref[:, width:] = updated[:, width:].astype(jnp.bfloat16)


def updated_weight(is_first, errors, factor, weight, mask):
    return pl.pallas_call(
        update_kernel,
        grid=(1,),
        out_shape=jax.ShapeDtypeStruct(weight.shape, jnp.bfloat16),
        in_specs=[
            SMEM,
            corner((1, *errors.shape[1:])),
            corner(factor.shape),
            corner(weight.shape),
            corner(mask.shape),
        ],
        out_specs=corner(weight.shape),
        name="update",
        compiler_params=params(12),
        cost_estimate=pl.CostEstimate(flops=400_000_000, bytes_accessed=2_200_000, transcendentals=0),
    )(is_first, errors, factor, weight, mask)


def columns_at(ref, block):
    return ref[:, pl.ds(pl.multiple_of(block * LANES, LANES), LANES)]


def ordered_columns(ref, from_ref):
    return jnp.concatenate(
        [columns_at(ref, z * 4 + from_ref[r]) for r in range(4) for z in range(4)], axis=1
    )


def project_kernel(from_ref, core_ref, *refs):
    mine, other, weight_ref, out_ref = refs[:4], refs[4:8], refs[8], refs[9]
    weight = ordered_columns(weight_ref, from_ref)
    for low in range(2):
        for source, core in ((mine, core_ref[0]), (other, 1 - core_ref[0])):
            tokens = jnp.concatenate(
                [source[r][z * 2 + low] for r in range(4) for z in range(4)], axis=1
            )
            out_ref[low * 2 + core] = lax.dot_general(
                tokens, weight, NT, preferred_element_type=jnp.float32
            ).astype(out_ref.dtype)


def stream_kernel(parts_ref, residual_ref, stream_ref, block_ref):
    rows = stream_ref.shape[0]
    total = residual_ref[:rows].astype(jnp.float32)
    for k in range(4):
        total = total + parts_ref[k].astype(jnp.float32)
    stream = total.astype(jnp.bfloat16)
    stream_ref[...] = stream
    wide = stream.astype(jnp.float32)
    gain = residual_ref[rows : rows + 16].astype(jnp.float32)[:1]
    square = lax.dot_general(
        jnp.ones((8, LANES), jnp.float32),
        wide * wide,
        NT,
        precision=lax.Precision.HIGHEST,
        preferred_element_type=jnp.float32,
    )
    high = square.astype(jnp.bfloat16).astype(jnp.float32)
    first = lax.broadcasted_iota(jnp.int32, square.shape, 0) == 0
    pair = jnp.where(first, high, square - high)
    block_ref[...] = jnp.concatenate([wide * gain, pair], axis=0).astype(jnp.bfloat16)


def copy_kernel(in_ref, out_ref):
    rows = out_ref.shape[0]
    out_ref[...] = in_ref[in_ref.shape[0] - rows :]


def order_kernel(from_ref, weight_ref, out_ref):
    out_ref[...] = ordered_columns(weight_ref, from_ref)


def gate_up_kernel(group_ref, core_ref, *refs):
    upper, lower, weight_ref = refs[:4], refs[4:8], refs[8]
    keep_ref, send_ref, part_ref = refs[9:]
    half = upper[0].shape[2]
    weight = weight_ref[...]
    units = weight.shape[0]
    places = [(r, z) for r in range(4) for z in range(4)]
    for k in range(4):
        high = jnp.concatenate([upper[r][k, z] for r, z in places], axis=1)
        low = jnp.concatenate([lower[k][r, z, :half] for r, z in places], axis=1)
        square = jnp.zeros((8, LANES), jnp.float32)
        for r, z in places:
            square = square + lower[k][r, z, half:].astype(jnp.float32)
        group = group_ref[k]
        part_ref[group, :units, :] = lax.dot_general(
            weight,
            jnp.concatenate([high, low], axis=0),
            NT,
            preferred_element_type=jnp.float32,
        )
        total = jnp.broadcast_to(square[0:1] + square[1:2], square.shape)
        big = total.astype(jnp.bfloat16).astype(jnp.float32)
        part_ref[group, units:, :] = jnp.concatenate([big, total - big], axis=0)
    for low_z in range(2):
        keep_ref[low_z] = part_ref[low_z * 2 + core_ref[0]]
        send_ref[low_z] = part_ref[low_z * 2 + 1 - core_ref[0]].astype(jnp.bfloat16)


def pair_kernel(low_ref, keep_ref, got_ref, next_keep_ref, next_send_ref):
    for ref, place in ((next_keep_ref, low_ref[0]), (next_send_ref, 1 - low_ref[0])):
        total = keep_ref[place] + got_ref[place].astype(jnp.float32)
        rows = total.shape[0] - 16
        ref[:rows] = total[:rows].astype(ref.dtype)
        square = total[rows : rows + 8] + total[rows + 8 :]
        big = square.astype(jnp.bfloat16).astype(jnp.float32)
        ref[rows:] = jnp.concatenate([big, square - big], axis=0).astype(ref.dtype)


def hidden_kernel(keep_ref, got_ref, stream_ref, hidden_ref, both_ref):
    units = hidden_ref.shape[0]
    sums = keep_ref[...] + got_ref[...].astype(jnp.float32)
    square = sums[2 * units : 2 * units + 8] + sums[2 * units + 8 :]
    inverse = lax.rsqrt(square / 8192 + 1e-05)[:1]
    gate = sums[:units] * inverse
    up = sums[units : 2 * units] * inverse
    hidden = (gate / (1.0 + jnp.exp(-gate)) * up).astype(jnp.bfloat16)
    hidden_ref[...] = hidden
    both_ref[:units] = hidden
    both_ref[units:] = stream_ref[...]


def hessian_kernel(from_ref, group_ref, rows_ref, *refs):
    upper, lower, out_ref, right_ref = refs[:4], refs[4:8], refs[8], refs[9]
    units = rows_ref.shape[1]
    half = units // 2
    for r in range(4):
        base = from_ref[r] * units
        for k in range(4):
            lanes = slice(k * LANES, (k + 1) * LANES)
            right_ref[pl.ds(pl.multiple_of(base, 16), half), lanes] = upper[r][k, 0]
            right_ref[pl.ds(pl.multiple_of(base + half, 16), half), lanes] = lower[k][r, 0]
    left = jnp.concatenate([rows_ref[group_ref[k]] for k in range(4)], axis=1)
    out_ref[...] = (2.0 / 512) * lax.dot_general(
        left, right_ref[...], NT, preferred_element_type=jnp.float32
    )


def body(attn_out, residual, output_weight, prune_mask, inverse_factor, norm_gain, gate_up_weight):
    units = gate_up_weight.shape[2]
    is_first = (lax.axis_index(DP) == 0).astype(jnp.int32)[None]
    order = senders("x")
    groups = senders("y")
    core = lax.axis_index("core").astype(jnp.int32)[None]
    low_z = lax.axis_index("z_low").astype(jnp.int32)[None]

    mine = copy_for_each(attn_out, ("z_high", "z_low"))
    mine = round_trip(mine, "x")
    other = [lax.ppermute(block, "core", [(0, 1), (1, 0)]) for block in mine]
    gain_rows = jnp.broadcast_to(norm_gain[None], (16, norm_gain.shape[0]))
    residual_turned = turned(jnp.concatenate([residual, gain_rows], axis=0))

    solved = solved_errors(output_weight, prune_mask, inverse_factor)
    errors = lax.all_gather(solved, DP)
    pruned_weight = updated_weight(is_first, errors, inverse_factor, output_weight, prune_mask)
    weight_turned = turned(pruned_weight)

    parts = pl.pallas_call(
        project_kernel,
        out_shape=jax.ShapeDtypeStruct((4, 128, 128), jnp.bfloat16),
        in_specs=[SMEM] * 2 + [VMEM] * 9,
        out_specs=VMEM,
        name="project",
        compiler_params=params(10),
        cost_estimate=pl.CostEstimate(flops=268_000_000, bytes_accessed=2_700_000, transcendentals=0),
    )(order, core, *mine, *other, weight_turned)
    parts = lax.all_to_all(parts, "y", 0, 0, tiled=True)
    stream_turned, block = pl.pallas_call(
        stream_kernel,
        out_shape=(
            jax.ShapeDtypeStruct((128, 128), jnp.bfloat16),
            jax.ShapeDtypeStruct((136, 128), jnp.bfloat16),
        ),
        in_specs=[VMEM] * 2,
        out_specs=[VMEM] * 2,
        name="stream",
        compiler_params=params(4),
        cost_estimate=pl.CostEstimate(flops=300_000, bytes_accessed=250_000, transcendentals=0),
    )(parts, residual_turned)
    flat_weight = gate_up_weight.transpose(1, 2, 0).reshape(2 * units, -1)
    flat_weight = pl.pallas_call(
        order_kernel,
        out_shape=jax.ShapeDtypeStruct(flat_weight.shape, jnp.bfloat16),
        in_specs=[SMEM, VMEM],
        out_specs=VMEM,
        name="order",
        compiler_params=params(8),
        cost_estimate=pl.CostEstimate(flops=0, bytes_accessed=3_700_000, transcendentals=0),
    )(order, flat_weight)
    upper, lower = over_y_and_x(over_z(block), 64)
    sums = (2, 2 * units + 16, 128)
    keep, send = pl.pallas_call(
        gate_up_kernel,
        out_shape=(
            jax.ShapeDtypeStruct(sums, jnp.float32),
            jax.ShapeDtypeStruct(sums, jnp.bfloat16),
        ),
        in_specs=[SMEM] * 2 + [VMEM] * 9,
        out_specs=[VMEM] * 2,
        scratch_shapes=[pltpu.VMEM((4, *sums[1:]), jnp.float32)],
        name="gate_up",
        compiler_params=params(14),
        cost_estimate=pl.CostEstimate(
            flops=940_000_000, bytes_accessed=4_300_000, transcendentals=0
        ),
    )(groups, core, *upper, *lower, flat_weight)
    got = lax.ppermute(send, "core", [(0, 1), (1, 0)])
    keep, send = pl.pallas_call(
        pair_kernel,
        out_shape=(
            jax.ShapeDtypeStruct(sums[1:], jnp.float32),
            jax.ShapeDtypeStruct(sums[1:], jnp.bfloat16),
        ),
        in_specs=[SMEM] + [VMEM] * 2,
        out_specs=[VMEM] * 2,
        name="pair",
        compiler_params=params(6),
        cost_estimate=pl.CostEstimate(flops=300_000, bytes_accessed=1_000_000, transcendentals=0),
    )(low_z, keep, got)
    got = lax.ppermute(send, "z_low", [(0, 1), (1, 0)])
    hidden, both = pl.pallas_call(
        hidden_kernel,
        out_shape=(
            jax.ShapeDtypeStruct((units, 128), jnp.bfloat16),
            jax.ShapeDtypeStruct((units + 128, 128), jnp.bfloat16),
        ),
        in_specs=[VMEM] * 3,
        out_specs=[VMEM] * 2,
        name="hidden",
        compiler_params=params(6),
        cost_estimate=pl.CostEstimate(
            flops=1_000_000, bytes_accessed=700_000, transcendentals=60_000
        ),
    )(keep, got, stream_turned)

    both = turned(both)
    stream = pl.pallas_call(
        copy_kernel,
        out_shape=jax.ShapeDtypeStruct((128, 128), jnp.bfloat16),
        in_specs=[VMEM],
        out_specs=VMEM,
        compiler_params=params(1),
    )(both)
    hidden_turned = both[:units]
    upper, lower = over_y_and_x(over_z(hidden_turned), units // 2)
    hidden_rows = lax.all_gather(hidden, DP)
    piece = pl.BlockSpec((4, 1, units // 2, 128), lambda z: (0, z, 0, 0))
    hessian = pl.pallas_call(
        hessian_kernel,
        grid=(4,),
        out_shape=jax.ShapeDtypeStruct((units, 16 * units), jnp.float32),
        in_specs=[
            SMEM,
            SMEM,
            pl.BlockSpec((4, units, 128), lambda z: (0, 0, 0)),
            *[piece] * 8,
        ],
        out_specs=pl.BlockSpec((units, 4 * units), lambda z: (0, z)),
        scratch_shapes=[pltpu.VMEM((4 * units, 4 * LANES), jnp.bfloat16)],
        name="hessian",
        compiler_params=params(14),
        cost_estimate=pl.CostEstimate(flops=822_000_000, bytes_accessed=7_100_000, transcendentals=0),
    )(order, groups, hidden_rows, *upper, *lower)
    return (pruned_weight, stream, hessian)


def solution(mesh):
    split = Mesh(mesh.devices.reshape(2, 2, 4, 4, 4), (*DP, *MP))
    return jax.shard_map(
        body,
        mesh=split,
        in_specs=(
            P(DP, MP),
            P(DP, MP),
            P(MP, DP),
            P(MP, None),
            P(None, DP),
            P(MP),
            P(DP, None, MP),
        ),
        out_specs=(P(MP, DP), P(DP, MP), P(MP, DP)),
        check_vma=False,
    )
```

```python
import jax
import jax.numpy as jnp
from jax import lax
from jax.experimental import pallas as pl
from jax.experimental.pallas import tpu as pltpu
from jax.sharding import Mesh
from jax.sharding import PartitionSpec as P


DP = ("z_low", "core")
MP = ("y", "z_high", "x")
NT = (((1,), (1,)), ((), ()))
VMEM = pl.BlockSpec(memory_space=pltpu.VMEM)
SMEM = pl.BlockSpec(memory_space=pltpu.SMEM)
LANES = 128
STEPS = (1, 3, 2)


def params(mib):
    return pltpu.CompilerParams(vmem_limit_bytes=mib << 20)


def copy_for_each(x, axis):
    size = lax.axis_size(axis)
    return lax.all_to_all(jnp.broadcast_to(x[None], (size, *x.shape)), axis, 0, 0, tiled=True)


def turned(x):
    pairs = [(d * 4 + y, y * 4 + d) for d in range(4) for y in range(4)]
    return lax.ppermute(x, (*DP, "y"), pairs)


def round_trip(x, axis):
    blocks = [x]
    for step in STEPS:
        blocks.append(lax.ppermute(x, axis, [(k, (k + step) % 4) for k in range(4)]))
    return blocks


def over_y_and_x(x, half):
    lower = jnp.stack(round_trip(x[:, half:], "x"))
    upper = jnp.stack(round_trip(x[:, :half], "y"))
    upper = round_trip(upper, "x")
    lower = round_trip(lower, "y")
    return upper, lower


def over_z(x):
    return copy_for_each(x, "z_high")


def senders(axis):
    here = lax.axis_index(axis)
    return jnp.stack([here] + [(here + 4 - step) % 4 for step in STEPS]).astype(jnp.int32)


def solve_kernel(weight_hbm, mask_hbm, factor_hbm, errors_ref, weight_ref, mask_ref, factor_ref, sems):
    size = factor_ref.shape[0]
    copies = [
        pltpu.make_async_copy(source.at[:, pl.ds(0, size)], target, sems.at[k])
        for k, (source, target) in enumerate(
            ((weight_hbm, weight_ref), (mask_hbm, mask_ref), (factor_hbm, factor_ref))
        )
    ]
    for copy in copies:
        copy.start()
    for copy in copies:
        copy.wait()
    step = 8
    count = size // step
    factor = factor_ref[...]
    row = lax.broadcasted_iota(jnp.int32, (size, size), 0)
    col = lax.broadcasted_iota(jnp.int32, (size, size), 1)
    pivots = jnp.sum(jnp.where(row == col, factor, 0.0), axis=1, keepdims=True)
    kept = mask_ref[...].astype(jnp.float32).T
    cutting = (1.0 - kept) / pivots
    current = weight_ref[...].astype(jnp.float32).T
    turned_factor = factor.T
    cur = [current[b * step : (b + 1) * step] for b in range(count)]
    fac = [turned_factor[b * step : (b + 1) * step] for b in range(count)]
    wide = (step, current.shape[1])
    place = lax.broadcasted_iota(jnp.int32, wide, 0)
    done = []
    for b in range(count):
        block = cur[b]
        cut_block = cutting[b * step : (b + 1) * step]
        fresh = []
        for i in range(step):
            j = b * step + i
            value = jnp.broadcast_to(cut_block[i : i + 1] * block[i : i + 1], wide)
            fresh.append(value)
            if i + 1 < step:
                reach = jnp.broadcast_to(fac[b][:, j : j + 1], wide)
                block = block - jnp.where(place > i, reach, 0.0) * value
        for v in range(b + 1, count):
            total = cur[v]
            for i in range(step):
                j = b * step + i
                total = total - jnp.broadcast_to(fac[v][:, j : j + 1], wide) * fresh[i]
            cur[v] = total
        rows = fresh[0]
        for i in range(1, step):
            rows = jnp.where(place == i, fresh[i], rows)
        done.append(rows)
    errors_ref[...] = jnp.concatenate(done, axis=0).T


def corner(shape):
    return pl.BlockSpec(shape, lambda i: (0,) * len(shape))


def solved_errors(weight, mask, factor):
    return pl.pallas_call(
        solve_kernel,
        out_shape=jax.ShapeDtypeStruct(mask.shape, jnp.float32),
        in_specs=[pl.BlockSpec(memory_space=pltpu.HBM)] * 3,
        out_specs=VMEM,
        scratch_shapes=[
            pltpu.VMEM(mask.shape, weight.dtype),
            pltpu.VMEM(mask.shape, mask.dtype),
            pltpu.VMEM(mask.shape, factor.dtype),
            pltpu.SemaphoreType.DMA((3,)),
        ],
        name="solve",
        compiler_params=params(60),
        cost_estimate=pl.CostEstimate(flops=20_000_000, bytes_accessed=300_000, transcendentals=0),
    )(weight, mask, factor)


def update_kernel(
    place_ref, solved_ref, e1, e2, e3, factor_ref, weight_ref, mask_ref, out_ref
):
    is_first = place_ref[0] == 0
    errors = jnp.where(is_first, solved_ref[...], e1[...] + e2[...] + e3[...])
    updated = weight_ref[...].astype(jnp.float32) - lax.dot_general(
        errors,
        factor_ref[...],
        (((1,), (0,)), ((), ())),
        precision=lax.Precision.HIGHEST,
        preferred_element_type=jnp.float32,
    )
    width = mask_ref.shape[1]
    kept = jnp.where(is_first, mask_ref[...].astype(jnp.float32), 1.0)
    out_ref[:, :width] = (updated[:, :width] * kept).astype(jnp.bfloat16)
    out_ref[:, width:] = updated[:, width:].astype(jnp.bfloat16)


def updated_weight(place, errors, factor, weight, mask):
    return pl.pallas_call(
        update_kernel,
        grid=(1,),
        out_shape=jax.ShapeDtypeStruct(weight.shape, jnp.bfloat16),
        in_specs=[
            SMEM,
            *[corner(mask.shape)] * 4,
            corner(factor.shape),
            corner(weight.shape),
            corner(mask.shape),
        ],
        out_specs=corner(weight.shape),
        name="update",
        compiler_params=params(12),
        cost_estimate=pl.CostEstimate(flops=400_000_000, bytes_accessed=2_200_000, transcendentals=0),
    )(place, *errors, factor, weight, mask)


def columns_at(ref, block):
    return ref[:, pl.ds(pl.multiple_of(block * LANES, LANES), LANES)]


def ordered_columns(ref, from_ref):
    return jnp.concatenate(
        [columns_at(ref, z * 4 + from_ref[r]) for r in range(4) for z in range(4)], axis=1
    )


def project_kernel(from_ref, core_ref, *refs):
    mine, other, weight_ref, out_ref = refs[:4], refs[4:8], refs[8], refs[9]
    weight = ordered_columns(weight_ref, from_ref)
    for low in range(2):
        for source, core in ((mine, core_ref[0]), (other, 1 - core_ref[0])):
            tokens = jnp.concatenate(
                [source[r][z * 2 + low] for r in range(4) for z in range(4)], axis=1
            )
            out_ref[low * 2 + core] = lax.dot_general(
                tokens, weight, NT, preferred_element_type=jnp.float32
            ).astype(out_ref.dtype)


def stream_kernel(parts_ref, residual_ref, stream_ref, block_ref):
    rows = stream_ref.shape[0]
    total = residual_ref[:rows].astype(jnp.float32)
    for k in range(4):
        total = total + parts_ref[k].astype(jnp.float32)
    stream = total.astype(jnp.bfloat16)
    stream_ref[...] = stream
    wide = stream.astype(jnp.float32)
    gain = residual_ref[rows : rows + 16].astype(jnp.float32)[:1]
    square = lax.dot_general(
        jnp.ones((8, LANES), jnp.float32),
        wide * wide,
        NT,
        precision=lax.Precision.HIGHEST,
        preferred_element_type=jnp.float32,
    )
    high = square.astype(jnp.bfloat16).astype(jnp.float32)
    first = lax.broadcasted_iota(jnp.int32, square.shape, 0) == 0
    pair = jnp.where(first, high, square - high)
    block_ref[...] = jnp.concatenate([wide * gain, pair], axis=0).astype(jnp.bfloat16)


def copy_kernel(in_ref, out_ref):
    rows = out_ref.shape[0]
    out_ref[...] = in_ref[in_ref.shape[0] - rows :]


def order_kernel(from_ref, weight_ref, out_ref):
    out_ref[...] = ordered_columns(weight_ref, from_ref)


def gate_up_kernel(group_ref, core_ref, *refs):
    upper, lower, weight_ref = refs[:4], refs[4:8], refs[8]
    keep_ref, send_ref, part_ref = refs[9:]
    half = upper[0].shape[2]
    weight = weight_ref[...]
    units = weight.shape[0]
    places = [(r, z) for r in range(4) for z in range(4)]
    for k in range(4):
        high = jnp.concatenate([upper[r][k, z] for r, z in places], axis=1)
        low = jnp.concatenate([lower[k][r, z, :half] for r, z in places], axis=1)
        square = jnp.zeros((8, LANES), jnp.float32)
        for r, z in places:
            square = square + lower[k][r, z, half:].astype(jnp.float32)
        group = group_ref[k]
        part_ref[group, :units, :] = lax.dot_general(
            weight,
            jnp.concatenate([high, low], axis=0),
            NT,
            preferred_element_type=jnp.float32,
        )
        total = jnp.broadcast_to(square[0:1] + square[1:2], square.shape)
        big = total.astype(jnp.bfloat16).astype(jnp.float32)
        part_ref[group, units:, :] = jnp.concatenate([big, total - big], axis=0)
    for low_z in range(2):
        keep_ref[low_z] = part_ref[low_z * 2 + core_ref[0]]
        send_ref[low_z] = part_ref[low_z * 2 + 1 - core_ref[0]].astype(jnp.bfloat16)


def pair_kernel(low_ref, keep_ref, got_ref, next_keep_ref, next_send_ref):
    for ref, place in ((next_keep_ref, low_ref[0]), (next_send_ref, 1 - low_ref[0])):
        total = keep_ref[place] + got_ref[place].astype(jnp.float32)
        rows = total.shape[0] - 16
        ref[:rows] = total[:rows].astype(ref.dtype)
        square = total[rows : rows + 8] + total[rows + 8 :]
        big = square.astype(jnp.bfloat16).astype(jnp.float32)
        ref[rows:] = jnp.concatenate([big, square - big], axis=0).astype(ref.dtype)


def hidden_kernel(keep_ref, got_ref, stream_ref, hidden_ref, both_ref):
    units = hidden_ref.shape[0]
    sums = keep_ref[...] + got_ref[...].astype(jnp.float32)
    square = sums[2 * units : 2 * units + 8] + sums[2 * units + 8 :]
    inverse = lax.rsqrt(square / 8192 + 1e-05)[:1]
    gate = sums[:units] * inverse
    up = sums[units : 2 * units] * inverse
    hidden = (gate / (1.0 + jnp.exp(-gate)) * up).astype(jnp.bfloat16)
    hidden_ref[...] = hidden
    both_ref[:units] = hidden
    both_ref[units:] = stream_ref[...]


def hessian_kernel(from_ref, group_ref, place_ref, near_ref, far_ref, *refs):
    upper, lower, out_ref, left_ref, right_ref = refs[:4], refs[4:8], *refs[8:]
    units = near_ref.shape[1]
    half = units // 2
    z = pl.program_id(0)
    part = pl.program_id(1)

    def lanes(group):
        return pl.ds(pl.multiple_of(group * LANES, LANES), LANES)

    @pl.when((z == 0) & (part == 0))
    def _():
        place = place_ref[0]
        for k in range(2):
            left_ref[:, lanes(jnp.bitwise_xor(place, k))] = near_ref[k]
            left_ref[:, lanes(jnp.bitwise_xor(place, 2 + k))] = far_ref[k]

    @pl.when(part == 0)
    def _():
        for r in range(4):
            base = from_ref[r] * units
            for k in range(4):
                group = lanes(group_ref[k])
                right_ref[pl.ds(pl.multiple_of(base, 16), half), group] = upper[r][k, z]
                right_ref[pl.ds(pl.multiple_of(base + half, 16), half), group] = lower[k][r, z]

    rows = pl.ds(pl.multiple_of(part * half, 16), half)
    out_ref[...] = (2.0 / 512) * lax.dot_general(
        left_ref[rows, :], right_ref[...], NT, preferred_element_type=jnp.float32
    )


def body(attn_out, residual, output_weight, prune_mask, inverse_factor, norm_gain, gate_up_weight):
    units = gate_up_weight.shape[2]
    place = lax.axis_index(DP).astype(jnp.int32)[None]
    order = senders("x")
    groups = senders("y")
    core = lax.axis_index("core").astype(jnp.int32)[None]
    low_z = lax.axis_index("z_low").astype(jnp.int32)[None]

    mine = copy_for_each(attn_out, ("z_high", "z_low"))
    mine = round_trip(mine, "x")
    other = [lax.ppermute(block, "core", [(0, 1), (1, 0)]) for block in mine]
    gain_rows = jnp.broadcast_to(norm_gain[None], (16, norm_gain.shape[0]))
    residual_turned = turned(jnp.concatenate([residual, gain_rows], axis=0))

    solved = solved_errors(output_weight, prune_mask, inverse_factor)
    errors = [solved] + [lax.ppermute(solved, DP, [(0, k)]) for k in range(1, 4)]
    pruned_weight = updated_weight(place, errors, inverse_factor, output_weight, prune_mask)
    weight_turned = turned(pruned_weight)

    parts = pl.pallas_call(
        project_kernel,
        out_shape=jax.ShapeDtypeStruct((4, 128, 128), jnp.bfloat16),
        in_specs=[SMEM] * 2 + [VMEM] * 9,
        out_specs=VMEM,
        name="project",
        compiler_params=params(10),
        cost_estimate=pl.CostEstimate(flops=268_000_000, bytes_accessed=2_700_000, transcendentals=0),
    )(order, core, *mine, *other, weight_turned)
    parts = lax.all_to_all(parts, "y", 0, 0, tiled=True)
    stream_turned, block = pl.pallas_call(
        stream_kernel,
        out_shape=(
            jax.ShapeDtypeStruct((128, 128), jnp.bfloat16),
            jax.ShapeDtypeStruct((136, 128), jnp.bfloat16),
        ),
        in_specs=[VMEM] * 2,
        out_specs=[VMEM] * 2,
        name="stream",
        compiler_params=params(4),
        cost_estimate=pl.CostEstimate(flops=300_000, bytes_accessed=250_000, transcendentals=0),
    )(parts, residual_turned)
    flat_weight = gate_up_weight.transpose(1, 2, 0).reshape(2 * units, -1)
    flat_weight = pl.pallas_call(
        order_kernel,
        out_shape=jax.ShapeDtypeStruct(flat_weight.shape, jnp.bfloat16),
        in_specs=[SMEM, VMEM],
        out_specs=VMEM,
        name="order",
        compiler_params=params(8),
        cost_estimate=pl.CostEstimate(flops=0, bytes_accessed=3_700_000, transcendentals=0),
    )(order, flat_weight)
    upper, lower = over_y_and_x(over_z(block), 64)
    sums = (2, 2 * units + 16, 128)
    keep, send = pl.pallas_call(
        gate_up_kernel,
        out_shape=(
            jax.ShapeDtypeStruct(sums, jnp.float32),
            jax.ShapeDtypeStruct(sums, jnp.bfloat16),
        ),
        in_specs=[SMEM] * 2 + [VMEM] * 9,
        out_specs=[VMEM] * 2,
        scratch_shapes=[pltpu.VMEM((4, *sums[1:]), jnp.float32)],
        name="gate_up",
        compiler_params=params(14),
        cost_estimate=pl.CostEstimate(
            flops=940_000_000, bytes_accessed=4_300_000, transcendentals=0
        ),
    )(groups, core, *upper, *lower, flat_weight)
    got = lax.ppermute(send, "core", [(0, 1), (1, 0)])
    keep, send = pl.pallas_call(
        pair_kernel,
        out_shape=(
            jax.ShapeDtypeStruct(sums[1:], jnp.float32),
            jax.ShapeDtypeStruct(sums[1:], jnp.bfloat16),
        ),
        in_specs=[SMEM] + [VMEM] * 2,
        out_specs=[VMEM] * 2,
        name="pair",
        compiler_params=params(6),
        cost_estimate=pl.CostEstimate(flops=300_000, bytes_accessed=1_000_000, transcendentals=0),
    )(low_z, keep, got)
    got = lax.ppermute(send, "z_low", [(0, 1), (1, 0)])
    hidden, both = pl.pallas_call(
        hidden_kernel,
        out_shape=(
            jax.ShapeDtypeStruct((units, 128), jnp.bfloat16),
            jax.ShapeDtypeStruct((units + 128, 128), jnp.bfloat16),
        ),
        in_specs=[VMEM] * 3,
        out_specs=[VMEM] * 2,
        name="hidden",
        compiler_params=params(6),
        cost_estimate=pl.CostEstimate(
            flops=1_000_000, bytes_accessed=700_000, transcendentals=60_000
        ),
    )(keep, got, stream_turned)

    both = turned(both)
    stream = pl.pallas_call(
        copy_kernel,
        out_shape=jax.ShapeDtypeStruct((128, 128), jnp.bfloat16),
        in_specs=[VMEM],
        out_specs=VMEM,
        compiler_params=params(1),
    )(both)
    hidden_turned = both[:units]
    upper, lower = over_y_and_x(over_z(hidden_turned), units // 2)
    other = lax.ppermute(hidden, "core", [(0, 1), (1, 0)])
    near = jnp.stack([hidden, other])
    far = lax.ppermute(near, "z_low", [(0, 1), (1, 0)])
    hessian = pl.pallas_call(
        hessian_kernel,
        grid=(4, 2),
        out_shape=jax.ShapeDtypeStruct((units, 16 * units), jnp.float32),
        in_specs=[SMEM] * 3 + [VMEM] * 10,
        out_specs=pl.BlockSpec((units // 2, 4 * units), lambda z, part: (part, z)),
        scratch_shapes=[
            pltpu.VMEM((units, 4 * LANES), jnp.bfloat16),
            pltpu.VMEM((4 * units, 4 * LANES), jnp.bfloat16),
        ],
        name="hessian",
        compiler_params=params(14),
        cost_estimate=pl.CostEstimate(flops=822_000_000, bytes_accessed=7_100_000, transcendentals=0),
    )(order, groups, place, near, far, *upper, *lower)
    return (pruned_weight, stream, hessian)


def solution(mesh):
    split = Mesh(mesh.devices.reshape(2, 2, 4, 4, 4), (*DP, *MP))
    return jax.shard_map(
        body,
        mesh=split,
        in_specs=(
            P(DP, MP),
            P(DP, MP),
            P(MP, DP),
            P(MP, None),
            P(None, DP),
            P(MP),
            P(DP, None, MP),
        ),
        out_specs=(P(MP, DP), P(DP, MP), P(MP, DP)),
        check_vma=False,
    )
```

```python
import jax
import jax.numpy as jnp
from jax import lax
from jax.experimental import pallas as pl
from jax.experimental.pallas import tpu as pltpu
from jax.sharding import Mesh
from jax.sharding import PartitionSpec as P


DP = ("z_low", "core")
MP = ("y", "z_high", "x")
NT = (((1,), (1,)), ((), ()))
VMEM = pl.BlockSpec(memory_space=pltpu.VMEM)
SMEM = pl.BlockSpec(memory_space=pltpu.SMEM)
LANES = 128
STEPS = (1, 3, 2)


def params(mib):
    return pltpu.CompilerParams(vmem_limit_bytes=mib << 20)


def copy_for_each(x, axis):
    size = lax.axis_size(axis)
    return lax.all_to_all(jnp.broadcast_to(x[None], (size, *x.shape)), axis, 0, 0, tiled=True)


def turned(x):
    pairs = [(d * 4 + y, y * 4 + d) for d in range(4) for y in range(4)]
    return lax.ppermute(x, (*DP, "y"), pairs)


def round_trip(x, axis):
    blocks = [x]
    for step in STEPS:
        blocks.append(lax.ppermute(x, axis, [(k, (k + step) % 4) for k in range(4)]))
    return blocks


def two_step_ring(x, axis):
    up = [(k, (k + 1) % 4) for k in range(4)]
    down = [(k, (k + 3) % 4) for k in range(4)]
    half = x.shape[0] // 2
    below, above = lax.ppermute(x, axis, up), lax.ppermute(x, axis, down)
    far = [lax.ppermute(below[:half], axis, up), lax.ppermute(above[half:], axis, down)]
    return [x, below, above, *far]


def over_y_and_x(x, half, large=round_trip):
    lower = jnp.stack(round_trip(x[:, half:], "x"))
    upper = jnp.stack(round_trip(x[:, :half], "y"))
    upper = large(upper, "x")
    lower = large(lower, "y")
    return upper, lower


def over_z(x):
    return copy_for_each(x, "z_high")


def senders(axis):
    here = lax.axis_index(axis)
    return jnp.stack([here] + [(here + 4 - step) % 4 for step in STEPS]).astype(jnp.int32)


def solve_kernel(weight_hbm, mask_hbm, factor_hbm, errors_ref, weight_ref, mask_ref, factor_ref, sems):
    size = factor_ref.shape[0]
    copies = [
        pltpu.make_async_copy(source.at[:, pl.ds(0, size)], target, sems.at[k])
        for k, (source, target) in enumerate(
            ((weight_hbm, weight_ref), (mask_hbm, mask_ref), (factor_hbm, factor_ref))
        )
    ]
    for copy in copies:
        copy.start()
    for copy in copies:
        copy.wait()
    step = 8
    count = size // step
    factor = factor_ref[...]
    row = lax.broadcasted_iota(jnp.int32, (size, size), 0)
    col = lax.broadcasted_iota(jnp.int32, (size, size), 1)
    pivots = jnp.sum(jnp.where(row == col, factor, 0.0), axis=1, keepdims=True)
    kept = mask_ref[...].astype(jnp.float32).T
    cutting = (1.0 - kept) / pivots
    current = weight_ref[...].astype(jnp.float32).T
    turned_factor = factor.T
    cur = [current[b * step : (b + 1) * step] for b in range(count)]
    fac = [turned_factor[b * step : (b + 1) * step] for b in range(count)]
    wide = (step, current.shape[1])
    place = lax.broadcasted_iota(jnp.int32, wide, 0)
    done = []
    for b in range(count):
        block = cur[b]
        cut_block = cutting[b * step : (b + 1) * step]
        fresh = []
        for i in range(step):
            j = b * step + i
            value = jnp.broadcast_to(cut_block[i : i + 1] * block[i : i + 1], wide)
            fresh.append(value)
            if i + 1 < step:
                reach = jnp.broadcast_to(fac[b][:, j : j + 1], wide)
                block = block - jnp.where(place > i, reach, 0.0) * value
        for v in range(b + 1, count):
            total = cur[v]
            for i in range(step):
                j = b * step + i
                total = total - jnp.broadcast_to(fac[v][:, j : j + 1], wide) * fresh[i]
            cur[v] = total
        rows = fresh[0]
        for i in range(1, step):
            rows = jnp.where(place == i, fresh[i], rows)
        done.append(rows)
    errors_ref[...] = jnp.concatenate(done, axis=0).T


def corner(shape):
    return pl.BlockSpec(shape, lambda i: (0,) * len(shape))


def solved_errors(weight, mask, factor):
    return pl.pallas_call(
        solve_kernel,
        out_shape=jax.ShapeDtypeStruct(mask.shape, jnp.float32),
        in_specs=[pl.BlockSpec(memory_space=pltpu.HBM)] * 3,
        out_specs=VMEM,
        scratch_shapes=[
            pltpu.VMEM(mask.shape, weight.dtype),
            pltpu.VMEM(mask.shape, mask.dtype),
            pltpu.VMEM(mask.shape, factor.dtype),
            pltpu.SemaphoreType.DMA((3,)),
        ],
        name="solve",
        compiler_params=params(60),
        cost_estimate=pl.CostEstimate(flops=20_000_000, bytes_accessed=300_000, transcendentals=0),
    )(weight, mask, factor)


def update_kernel(place_ref, errors_ref, factor_ref, weight_ref, mask_ref, out_ref):
    updated = weight_ref[...].astype(jnp.float32) - lax.dot_general(
        errors_ref[0],
        factor_ref[...],
        (((1,), (0,)), ((), ())),
        precision=lax.Precision.HIGHEST,
        preferred_element_type=jnp.float32,
    )
    width = mask_ref.shape[1]
    kept = jnp.where(place_ref[0] == 0, mask_ref[...].astype(jnp.float32), 1.0)
    out_ref[:, :width] = (updated[:, :width] * kept).astype(jnp.bfloat16)
    out_ref[:, width:] = updated[:, width:].astype(jnp.bfloat16)


def updated_weight(place, errors, factor, weight, mask):
    return pl.pallas_call(
        update_kernel,
        grid=(1,),
        out_shape=jax.ShapeDtypeStruct(weight.shape, jnp.bfloat16),
        in_specs=[
            SMEM,
            corner((1, *errors.shape[1:])),
            corner(factor.shape),
            corner(weight.shape),
            corner(mask.shape),
        ],
        out_specs=corner(weight.shape),
        name="update",
        compiler_params=params(12),
        cost_estimate=pl.CostEstimate(flops=400_000_000, bytes_accessed=2_200_000, transcendentals=0),
    )(place, errors, factor, weight, mask)


def columns_at(ref, block):
    return ref[:, pl.ds(pl.multiple_of(block * LANES, LANES), LANES)]


def ordered_columns(ref, from_ref):
    return jnp.concatenate(
        [columns_at(ref, z * 4 + from_ref[r]) for r in range(4) for z in range(4)], axis=1
    )


def project_kernel(from_ref, core_ref, *refs):
    mine, other, weight_ref, out_ref = refs[:4], refs[4:8], refs[8], refs[9]
    weight = ordered_columns(weight_ref, from_ref)
    for low in range(2):
        for source, core in ((mine, core_ref[0]), (other, 1 - core_ref[0])):
            tokens = jnp.concatenate(
                [source[r][z * 2 + low] for r in range(4) for z in range(4)], axis=1
            )
            out_ref[low * 2 + core] = lax.dot_general(
                tokens, weight, NT, preferred_element_type=jnp.float32
            ).astype(out_ref.dtype)


def stream_kernel(parts_ref, residual_ref, stream_ref, block_ref):
    rows = stream_ref.shape[0]
    total = residual_ref[:rows].astype(jnp.float32)
    for k in range(4):
        total = total + parts_ref[k].astype(jnp.float32)
    stream = total.astype(jnp.bfloat16)
    stream_ref[...] = stream
    wide = stream.astype(jnp.float32)
    gain = residual_ref[rows : rows + 16].astype(jnp.float32)[:1]
    square = lax.dot_general(
        jnp.ones((8, LANES), jnp.float32),
        wide * wide,
        NT,
        precision=lax.Precision.HIGHEST,
        preferred_element_type=jnp.float32,
    )
    high = square.astype(jnp.bfloat16).astype(jnp.float32)
    first = lax.broadcasted_iota(jnp.int32, square.shape, 0) == 0
    pair = jnp.where(first, high, square - high)
    block_ref[...] = jnp.concatenate([wide * gain, pair], axis=0).astype(jnp.bfloat16)


def copy_kernel(in_ref, out_ref):
    rows = out_ref.shape[0]
    out_ref[...] = in_ref[in_ref.shape[0] - rows :]


def order_kernel(from_ref, weight_ref, out_ref):
    out_ref[...] = ordered_columns(weight_ref, from_ref)


def gate_up_kernel(group_ref, core_ref, *refs):
    upper, lower, weight_ref = refs[:4], refs[4:8], refs[8]
    keep_ref, send_ref, part_ref = refs[9:]
    half = upper[0].shape[2]
    weight = weight_ref[...]
    units = weight.shape[0]
    places = [(r, z) for r in range(4) for z in range(4)]
    for k in range(4):
        high = jnp.concatenate([upper[r][k, z] for r, z in places], axis=1)
        low = jnp.concatenate([lower[k][r, z, :half] for r, z in places], axis=1)
        square = jnp.zeros((8, LANES), jnp.float32)
        for r, z in places:
            square = square + lower[k][r, z, half:].astype(jnp.float32)
        group = group_ref[k]
        part_ref[group, :units, :] = lax.dot_general(
            weight,
            jnp.concatenate([high, low], axis=0),
            NT,
            preferred_element_type=jnp.float32,
        )
        total = jnp.broadcast_to(square[0:1] + square[1:2], square.shape)
        big = total.astype(jnp.bfloat16).astype(jnp.float32)
        part_ref[group, units:, :] = jnp.concatenate([big, total - big], axis=0)
    for low_z in range(2):
        keep_ref[low_z] = part_ref[low_z * 2 + core_ref[0]]
        send_ref[low_z] = part_ref[low_z * 2 + 1 - core_ref[0]].astype(jnp.bfloat16)


def pair_kernel(low_ref, keep_ref, got_ref, next_keep_ref, next_send_ref):
    for ref, place in ((next_keep_ref, low_ref[0]), (next_send_ref, 1 - low_ref[0])):
        total = keep_ref[place] + got_ref[place].astype(jnp.float32)
        rows = total.shape[0] - 16
        ref[:rows] = total[:rows].astype(ref.dtype)
        square = total[rows : rows + 8] + total[rows + 8 :]
        big = square.astype(jnp.bfloat16).astype(jnp.float32)
        ref[rows:] = jnp.concatenate([big, square - big], axis=0).astype(ref.dtype)


def hidden_kernel(keep_ref, got_ref, stream_ref, hidden_ref, both_ref):
    units = hidden_ref.shape[0]
    sums = keep_ref[...] + got_ref[...].astype(jnp.float32)
    square = sums[2 * units : 2 * units + 8] + sums[2 * units + 8 :]
    inverse = lax.rsqrt(square / 8192 + 1e-05)[:1]
    gate = sums[:units] * inverse
    up = sums[units : 2 * units] * inverse
    hidden = (gate / (1.0 + jnp.exp(-gate)) * up).astype(jnp.bfloat16)
    hidden_ref[...] = hidden
    both_ref[:units] = hidden
    both_ref[units:] = stream_ref[...]


def hessian_kernel(from_ref, group_ref, place_ref, near_ref, far_ref, *refs):
    upper, lower, out_ref, left_ref, right_ref = refs[:5], refs[5:10], *refs[10:]
    units = near_ref.shape[1]
    half = units // 2
    z = pl.program_id(0)

    def lanes(group):
        return pl.ds(pl.multiple_of(group * LANES, LANES), LANES)

    def piece(blocks, large, small):
        if large < 3:
            return blocks[large][small, z]
        return blocks[3 + small // 2][small % 2, z]

    @pl.when(z == 0)
    def _():
        place = place_ref[0]
        for k in range(2):
            left_ref[:, lanes(jnp.bitwise_xor(place, k))] = near_ref[k]
            left_ref[:, lanes(jnp.bitwise_xor(place, 2 + k))] = far_ref[k]

    for r in range(4):
        base = from_ref[r] * units
        for k in range(4):
            group = lanes(group_ref[k])
            right_ref[pl.ds(pl.multiple_of(base, 16), half), group] = piece(upper, r, k)
            right_ref[pl.ds(pl.multiple_of(base + half, 16), half), group] = piece(lower, k, r)
    out_ref[...] = (2.0 / 512) * lax.dot_general(
        left_ref[...], right_ref[...], NT, preferred_element_type=jnp.float32
    )


def body(attn_out, residual, output_weight, prune_mask, inverse_factor, norm_gain, gate_up_weight):
    units = gate_up_weight.shape[2]
    place = lax.axis_index(DP).astype(jnp.int32)[None]
    order = senders("x")
    groups = senders("y")
    core = lax.axis_index("core").astype(jnp.int32)[None]
    low_z = lax.axis_index("z_low").astype(jnp.int32)[None]

    mine = copy_for_each(attn_out, ("z_high", "z_low"))
    mine = round_trip(mine, "x")
    other = [lax.ppermute(block, "core", [(0, 1), (1, 0)]) for block in mine]
    gain_rows = jnp.broadcast_to(norm_gain[None], (16, norm_gain.shape[0]))
    residual_turned = turned(jnp.concatenate([residual, gain_rows], axis=0))

    solved = solved_errors(output_weight, prune_mask, inverse_factor)
    errors = lax.all_gather(solved, DP)
    pruned_weight = updated_weight(place, errors, inverse_factor, output_weight, prune_mask)
    weight_turned = turned(pruned_weight)

    parts = pl.pallas_call(
        project_kernel,
        out_shape=jax.ShapeDtypeStruct((4, 128, 128), jnp.bfloat16),
        in_specs=[SMEM] * 2 + [VMEM] * 9,
        out_specs=VMEM,
        name="project",
        compiler_params=params(10),
        cost_estimate=pl.CostEstimate(flops=268_000_000, bytes_accessed=2_700_000, transcendentals=0),
    )(order, core, *mine, *other, weight_turned)
    parts = lax.all_to_all(parts, "y", 0, 0, tiled=True)
    stream_turned, block = pl.pallas_call(
        stream_kernel,
        out_shape=(
            jax.ShapeDtypeStruct((128, 128), jnp.bfloat16),
            jax.ShapeDtypeStruct((136, 128), jnp.bfloat16),
        ),
        in_specs=[VMEM] * 2,
        out_specs=[VMEM] * 2,
        name="stream",
        compiler_params=params(4),
        cost_estimate=pl.CostEstimate(flops=300_000, bytes_accessed=250_000, transcendentals=0),
    )(parts, residual_turned)
    flat_weight = gate_up_weight.transpose(1, 2, 0).reshape(2 * units, -1)
    flat_weight = pl.pallas_call(
        order_kernel,
        out_shape=jax.ShapeDtypeStruct(flat_weight.shape, jnp.bfloat16),
        in_specs=[SMEM, VMEM],
        out_specs=VMEM,
        name="order",
        compiler_params=params(8),
        cost_estimate=pl.CostEstimate(flops=0, bytes_accessed=3_700_000, transcendentals=0),
    )(order, flat_weight)
    upper, lower = over_y_and_x(over_z(block), 64)
    sums = (2, 2 * units + 16, 128)
    keep, send = pl.pallas_call(
        gate_up_kernel,
        out_shape=(
            jax.ShapeDtypeStruct(sums, jnp.float32),
            jax.ShapeDtypeStruct(sums, jnp.bfloat16),
        ),
        in_specs=[SMEM] * 2 + [VMEM] * 9,
        out_specs=[VMEM] * 2,
        scratch_shapes=[pltpu.VMEM((4, *sums[1:]), jnp.float32)],
        name="gate_up",
        compiler_params=params(14),
        cost_estimate=pl.CostEstimate(
            flops=940_000_000, bytes_accessed=4_300_000, transcendentals=0
        ),
    )(groups, core, *upper, *lower, flat_weight)
    got = lax.ppermute(send, "core", [(0, 1), (1, 0)])
    keep, send = pl.pallas_call(
        pair_kernel,
        out_shape=(
            jax.ShapeDtypeStruct(sums[1:], jnp.float32),
            jax.ShapeDtypeStruct(sums[1:], jnp.bfloat16),
        ),
        in_specs=[SMEM] + [VMEM] * 2,
        out_specs=[VMEM] * 2,
        name="pair",
        compiler_params=params(6),
        cost_estimate=pl.CostEstimate(flops=300_000, bytes_accessed=1_000_000, transcendentals=0),
    )(low_z, keep, got)
    got = lax.ppermute(send, "z_low", [(0, 1), (1, 0)])
    hidden, both = pl.pallas_call(
        hidden_kernel,
        out_shape=(
            jax.ShapeDtypeStruct((units, 128), jnp.bfloat16),
            jax.ShapeDtypeStruct((units + 128, 128), jnp.bfloat16),
        ),
        in_specs=[VMEM] * 3,
        out_specs=[VMEM] * 2,
        name="hidden",
        compiler_params=params(6),
        cost_estimate=pl.CostEstimate(
            flops=1_000_000, bytes_accessed=700_000, transcendentals=60_000
        ),
    )(keep, got, stream_turned)

    both = turned(both)
    stream = pl.pallas_call(
        copy_kernel,
        out_shape=jax.ShapeDtypeStruct((128, 128), jnp.bfloat16),
        in_specs=[VMEM],
        out_specs=VMEM,
        compiler_params=params(1),
    )(both)
    hidden_turned = both[:units]
    upper, lower = over_y_and_x(over_z(hidden_turned), units // 2, two_step_ring)
    other = lax.ppermute(hidden, "core", [(0, 1), (1, 0)])
    near = jnp.stack([hidden, other])
    far = lax.ppermute(near, "z_low", [(0, 1), (1, 0)])
    hessian = pl.pallas_call(
        hessian_kernel,
        grid=(4,),
        out_shape=jax.ShapeDtypeStruct((units, 16 * units), jnp.float32),
        in_specs=[SMEM] * 3 + [VMEM] * 12,
        out_specs=pl.BlockSpec((units, 4 * units), lambda z: (0, z)),
        scratch_shapes=[
            pltpu.VMEM((units, 4 * LANES), jnp.bfloat16),
            pltpu.VMEM((4 * units, 4 * LANES), jnp.bfloat16),
        ],
        name="hessian",
        compiler_params=params(14),
        cost_estimate=pl.CostEstimate(flops=822_000_000, bytes_accessed=7_100_000, transcendentals=0),
    )(order, groups, place, near, far, *upper, *lower)
    return (pruned_weight, stream, hessian)


def solution(mesh):
    split = Mesh(mesh.devices.reshape(2, 2, 4, 4, 4), (*DP, *MP))
    return jax.shard_map(
        body,
        mesh=split,
        in_specs=(
            P(DP, MP),
            P(DP, MP),
            P(MP, DP),
            P(MP, None),
            P(None, DP),
            P(MP),
            P(DP, None, MP),
        ),
        out_specs=(P(MP, DP), P(DP, MP), P(MP, DP)),
        check_vma=False,
    )
```

```python
import jax
import jax.numpy as jnp
from jax import lax
from jax.experimental import pallas as pl
from jax.experimental.pallas import tpu as pltpu
from jax.sharding import Mesh
from jax.sharding import PartitionSpec as P


DP = ("z_low", "core")
MP = ("y", "z_high", "x")
NT = (((1,), (1,)), ((), ()))
VMEM = pl.BlockSpec(memory_space=pltpu.VMEM)
SMEM = pl.BlockSpec(memory_space=pltpu.SMEM)
LANES = 128
STEPS = (1, 3, 2)


def params(mib):
    return pltpu.CompilerParams(vmem_limit_bytes=mib << 20)


def copy_for_each(x, axis):
    size = lax.axis_size(axis)
    return lax.all_to_all(jnp.broadcast_to(x[None], (size, *x.shape)), axis, 0, 0, tiled=True)


def turned(x):
    pairs = [(d * 4 + y, y * 4 + d) for d in range(4) for y in range(4)]
    return lax.ppermute(x, (*DP, "y"), pairs)


def round_trip(x, axis):
    blocks = [x]
    for step in STEPS:
        blocks.append(lax.ppermute(x, axis, [(k, (k + step) % 4) for k in range(4)]))
    return blocks


def two_step_ring(x, axis):
    up = [(k, (k + 1) % 4) for k in range(4)]
    down = [(k, (k + 3) % 4) for k in range(4)]
    half = x.shape[0] // 2
    below, above = lax.ppermute(x, axis, up), lax.ppermute(x, axis, down)
    far = [lax.ppermute(below[:half], axis, up), lax.ppermute(above[half:], axis, down)]
    return [x, below, above, *far]


def over_y_and_x(x, half, large=round_trip):
    lower = jnp.stack(round_trip(x[:, half:], "x"))
    upper = jnp.stack(round_trip(x[:, :half], "y"))
    upper = large(upper, "x")
    lower = large(lower, "y")
    return upper, lower


def over_z(x):
    return copy_for_each(x, "z_high")


def senders(axis):
    here = lax.axis_index(axis)
    return jnp.stack([here] + [(here + 4 - step) % 4 for step in STEPS]).astype(jnp.int32)


def solve_kernel(weight_hbm, mask_hbm, factor_hbm, errors_ref, weight_ref, mask_ref, factor_ref, sems):
    size = factor_ref.shape[0]
    copies = [
        pltpu.make_async_copy(source.at[:, pl.ds(0, size)], target, sems.at[k])
        for k, (source, target) in enumerate(
            ((weight_hbm, weight_ref), (mask_hbm, mask_ref), (factor_hbm, factor_ref))
        )
    ]
    for copy in copies:
        copy.start()
    for copy in copies:
        copy.wait()
    step = 8
    count = size // step
    factor = factor_ref[...]
    row = lax.broadcasted_iota(jnp.int32, (size, size), 0)
    col = lax.broadcasted_iota(jnp.int32, (size, size), 1)
    pivots = jnp.sum(jnp.where(row == col, factor, 0.0), axis=1, keepdims=True)
    kept = mask_ref[...].astype(jnp.float32).T
    cutting = (1.0 - kept) / pivots
    current = weight_ref[...].astype(jnp.float32).T
    turned_factor = factor.T
    cur = [current[b * step : (b + 1) * step] for b in range(count)]
    fac = [turned_factor[b * step : (b + 1) * step] for b in range(count)]
    wide = (step, current.shape[1])
    place = lax.broadcasted_iota(jnp.int32, wide, 0)
    done = []
    for b in range(count):
        block = cur[b]
        cut_block = cutting[b * step : (b + 1) * step]
        fresh = []
        for i in range(step):
            j = b * step + i
            value = jnp.broadcast_to(cut_block[i : i + 1] * block[i : i + 1], wide)
            fresh.append(value)
            if i + 1 < step:
                reach = jnp.broadcast_to(fac[b][:, j : j + 1], wide)
                block = block - jnp.where(place > i, reach, 0.0) * value
        for v in range(b + 1, count):
            total = cur[v]
            for i in range(step):
                j = b * step + i
                total = total - jnp.broadcast_to(fac[v][:, j : j + 1], wide) * fresh[i]
            cur[v] = total
        rows = fresh[0]
        for i in range(1, step):
            rows = jnp.where(place == i, fresh[i], rows)
        done.append(rows)
    errors_ref[...] = jnp.concatenate(done, axis=0).T


def corner(shape):
    return pl.BlockSpec(shape, lambda i: (0,) * len(shape))


def solved_errors(weight, mask, factor):
    return pl.pallas_call(
        solve_kernel,
        out_shape=jax.ShapeDtypeStruct(mask.shape, jnp.float32),
        in_specs=[pl.BlockSpec(memory_space=pltpu.HBM)] * 3,
        out_specs=VMEM,
        scratch_shapes=[
            pltpu.VMEM(mask.shape, weight.dtype),
            pltpu.VMEM(mask.shape, mask.dtype),
            pltpu.VMEM(mask.shape, factor.dtype),
            pltpu.SemaphoreType.DMA((3,)),
        ],
        name="solve",
        compiler_params=params(60),
        cost_estimate=pl.CostEstimate(flops=20_000_000, bytes_accessed=300_000, transcendentals=0),
    )(weight, mask, factor)


def update_kernel(place_ref, errors_ref, factor_ref, weight_ref, mask_ref, out_ref):
    updated = weight_ref[...].astype(jnp.float32) - lax.dot_general(
        errors_ref[0],
        factor_ref[...],
        (((1,), (0,)), ((), ())),
        precision=lax.Precision.HIGHEST,
        preferred_element_type=jnp.float32,
    )
    width = mask_ref.shape[1]
    kept = jnp.where(place_ref[0] == 0, mask_ref[...].astype(jnp.float32), 1.0)
    out_ref[:, :width] = (updated[:, :width] * kept).astype(jnp.bfloat16)
    out_ref[:, width:] = updated[:, width:].astype(jnp.bfloat16)


def updated_weight(place, errors, factor, weight, mask):
    return pl.pallas_call(
        update_kernel,
        grid=(1,),
        out_shape=jax.ShapeDtypeStruct(weight.shape, jnp.bfloat16),
        in_specs=[
            SMEM,
            corner((1, *errors.shape[1:])),
            corner(factor.shape),
            corner(weight.shape),
            corner(mask.shape),
        ],
        out_specs=corner(weight.shape),
        name="update",
        compiler_params=params(12),
        cost_estimate=pl.CostEstimate(flops=400_000_000, bytes_accessed=2_200_000, transcendentals=0),
    )(place, errors, factor, weight, mask)


def columns_at(ref, block):
    return ref[:, pl.ds(pl.multiple_of(block * LANES, LANES), LANES)]


def ordered_columns(ref, from_ref):
    return jnp.concatenate(
        [columns_at(ref, z * 4 + from_ref[r]) for r in range(4) for z in range(4)], axis=1
    )


def project_kernel(from_ref, core_ref, *refs):
    mine, other, weight_ref, out_ref = refs[:4], refs[4:8], refs[8], refs[9]
    weight = ordered_columns(weight_ref, from_ref)
    for low in range(2):
        for source, core in ((mine, core_ref[0]), (other, 1 - core_ref[0])):
            tokens = jnp.concatenate(
                [source[r][z * 2 + low] for r in range(4) for z in range(4)], axis=1
            )
            out_ref[low * 2 + core] = lax.dot_general(
                tokens, weight, NT, preferred_element_type=jnp.float32
            ).astype(out_ref.dtype)


def stream_kernel(parts_ref, residual_ref, stream_ref, block_ref):
    rows = stream_ref.shape[0]
    total = residual_ref[:rows].astype(jnp.float32)
    for k in range(4):
        total = total + parts_ref[k].astype(jnp.float32)
    stream = total.astype(jnp.bfloat16)
    stream_ref[...] = stream
    wide = stream.astype(jnp.float32)
    gain = residual_ref[rows : rows + 16].astype(jnp.float32)[:1]
    square = lax.dot_general(
        jnp.ones((8, LANES), jnp.float32),
        wide * wide,
        NT,
        precision=lax.Precision.HIGHEST,
        preferred_element_type=jnp.float32,
    )
    high = square.astype(jnp.bfloat16).astype(jnp.float32)
    first = lax.broadcasted_iota(jnp.int32, square.shape, 0) == 0
    pair = jnp.where(first, high, square - high)
    block_ref[...] = jnp.concatenate([wide * gain, pair], axis=0).astype(jnp.bfloat16)


def copy_kernel(in_ref, out_ref):
    rows = out_ref.shape[0]
    out_ref[...] = in_ref[in_ref.shape[0] - rows :]


def order_kernel(from_ref, weight_ref, out_ref):
    out_ref[...] = ordered_columns(weight_ref, from_ref)


def gate_up_kernel(group_ref, core_ref, *refs):
    upper, lower, weight_ref = refs[:4], refs[4:8], refs[8]
    keep_ref, send_ref = refs[9:]
    half = upper[0].shape[2]
    weight = weight_ref[...]
    units = weight.shape[0]
    places = [(r, z) for r in range(4) for z in range(4)]
    for k in range(4):
        high = jnp.concatenate([upper[r][k, z] for r, z in places], axis=1)
        low = jnp.concatenate([lower[k][r, z, :half] for r, z in places], axis=1)
        square = jnp.zeros((8, LANES), jnp.float32)
        for r, z in places:
            square = square + lower[k][r, z, half:].astype(jnp.float32)
        part = lax.dot_general(
            weight,
            jnp.concatenate([high, low], axis=0),
            NT,
            preferred_element_type=jnp.float32,
        )
        total = jnp.broadcast_to(square[0:1] + square[1:2], square.shape)
        big = total.astype(jnp.bfloat16).astype(jnp.float32)
        extra = jnp.concatenate([big, total - big], axis=0)
        low_z = jnp.right_shift(group_ref[k], 1)
        stays = jnp.bitwise_and(group_ref[k], 1) == core_ref[0]
        for ref, mine in ((keep_ref, stays), (send_ref, jnp.logical_not(stays))):

            @pl.when(mine)
            def _():
                ref[low_z, :units, :] = part.astype(ref.dtype)
                ref[low_z, units:, :] = extra.astype(ref.dtype)


def pair_kernel(low_ref, keep_ref, got_ref, next_keep_ref, next_send_ref):
    for ref, place in ((next_keep_ref, low_ref[0]), (next_send_ref, 1 - low_ref[0])):
        total = keep_ref[place] + got_ref[place].astype(jnp.float32)
        rows = total.shape[0] - 16
        ref[:rows] = total[:rows].astype(ref.dtype)
        square = total[rows : rows + 8] + total[rows + 8 :]
        big = square.astype(jnp.bfloat16).astype(jnp.float32)
        ref[rows:] = jnp.concatenate([big, square - big], axis=0).astype(ref.dtype)


def hidden_kernel(keep_ref, got_ref, stream_ref, hidden_ref, both_ref):
    units = hidden_ref.shape[0]
    sums = keep_ref[...] + got_ref[...].astype(jnp.float32)
    square = sums[2 * units : 2 * units + 8] + sums[2 * units + 8 :]
    inverse = lax.rsqrt(square / 8192 + 1e-05)[:1]
    gate = sums[:units] * inverse
    up = sums[units : 2 * units] * inverse
    hidden = (gate / (1.0 + jnp.exp(-gate)) * up).astype(jnp.bfloat16)
    hidden_ref[...] = hidden
    both_ref[:units] = hidden
    both_ref[units:] = stream_ref[...]


def hessian_kernel(from_ref, group_ref, place_ref, near_ref, far_ref, *refs):
    upper, lower, out_hbm = refs[:5], refs[5:10], refs[10]
    left_ref, right_ref, result_ref, sems = refs[11:]
    units = near_ref.shape[1]
    half = units // 2
    wide = 4 * units

    def lanes(group):
        return pl.ds(pl.multiple_of(group * LANES, LANES), LANES)

    def piece(blocks, large, small, z):
        if large < 3:
            return blocks[large][small, z]
        return blocks[3 + small // 2][small % 2, z]

    place = place_ref[0]
    for k in range(2):
        left_ref[:, lanes(jnp.bitwise_xor(place, k))] = near_ref[k]
        left_ref[:, lanes(jnp.bitwise_xor(place, 2 + k))] = far_ref[k]
    copies = []
    for z in range(4):
        right = right_ref.at[z % 2]
        for r in range(4):
            base = from_ref[r] * units
            for k in range(4):
                group = lanes(group_ref[k])
                right[pl.ds(pl.multiple_of(base, 16), half), group] = piece(upper, r, k, z)
                right[pl.ds(pl.multiple_of(base + half, 16), half), group] = piece(lower, k, r, z)
        result_ref[z] = (2.0 / 512) * lax.dot_general(
            left_ref[...], right[...], NT, preferred_element_type=jnp.float32
        )
        for part in range(2):
            rows = slice(part * half, (part + 1) * half)
            copy = pltpu.make_async_copy(
                result_ref.at[z, rows, :],
                out_hbm.at[rows, z * wide : (z + 1) * wide],
                sems.at[z * 2 + part],
            )
            copy.start()
            copies.append(copy)
    for copy in copies:
        copy.wait()


def body(attn_out, residual, output_weight, prune_mask, inverse_factor, norm_gain, gate_up_weight):
    units = gate_up_weight.shape[2]
    place = lax.axis_index(DP).astype(jnp.int32)[None]
    order = senders("x")
    groups = senders("y")
    core = lax.axis_index("core").astype(jnp.int32)[None]
    low_z = lax.axis_index("z_low").astype(jnp.int32)[None]

    mine = copy_for_each(attn_out, ("z_high", "z_low"))
    mine = round_trip(mine, "x")
    other = [lax.ppermute(block, "core", [(0, 1), (1, 0)]) for block in mine]
    gain_rows = jnp.broadcast_to(norm_gain[None], (16, norm_gain.shape[0]))
    residual_turned = turned(jnp.concatenate([residual, gain_rows], axis=0))

    solved = solved_errors(output_weight, prune_mask, inverse_factor)
    errors = lax.all_gather(solved, DP)
    pruned_weight = updated_weight(place, errors, inverse_factor, output_weight, prune_mask)
    weight_turned = turned(pruned_weight)

    parts = pl.pallas_call(
        project_kernel,
        out_shape=jax.ShapeDtypeStruct((4, 128, 128), jnp.bfloat16),
        in_specs=[SMEM] * 2 + [VMEM] * 9,
        out_specs=VMEM,
        name="project",
        compiler_params=params(10),
        cost_estimate=pl.CostEstimate(flops=268_000_000, bytes_accessed=2_700_000, transcendentals=0),
    )(order, core, *mine, *other, weight_turned)
    parts = lax.all_to_all(parts, "y", 0, 0, tiled=True)
    stream_turned, block = pl.pallas_call(
        stream_kernel,
        out_shape=(
            jax.ShapeDtypeStruct((128, 128), jnp.bfloat16),
            jax.ShapeDtypeStruct((136, 128), jnp.bfloat16),
        ),
        in_specs=[VMEM] * 2,
        out_specs=[VMEM] * 2,
        name="stream",
        compiler_params=params(4),
        cost_estimate=pl.CostEstimate(flops=300_000, bytes_accessed=250_000, transcendentals=0),
    )(parts, residual_turned)
    flat_weight = gate_up_weight.transpose(1, 2, 0).reshape(2 * units, -1)
    flat_weight = pl.pallas_call(
        order_kernel,
        out_shape=jax.ShapeDtypeStruct(flat_weight.shape, jnp.bfloat16),
        in_specs=[SMEM, VMEM],
        out_specs=VMEM,
        name="order",
        compiler_params=params(8),
        cost_estimate=pl.CostEstimate(flops=0, bytes_accessed=3_700_000, transcendentals=0),
    )(order, flat_weight)
    upper, lower = over_y_and_x(over_z(block), 64)
    sums = (2, 2 * units + 16, 128)
    keep, send = pl.pallas_call(
        gate_up_kernel,
        out_shape=(
            jax.ShapeDtypeStruct(sums, jnp.float32),
            jax.ShapeDtypeStruct(sums, jnp.bfloat16),
        ),
        in_specs=[SMEM] * 2 + [VMEM] * 9,
        out_specs=[VMEM] * 2,
        name="gate_up",
        compiler_params=params(14),
        cost_estimate=pl.CostEstimate(
            flops=940_000_000, bytes_accessed=4_300_000, transcendentals=0
        ),
    )(groups, core, *upper, *lower, flat_weight)
    got = lax.ppermute(send, "core", [(0, 1), (1, 0)])
    keep, send = pl.pallas_call(
        pair_kernel,
        out_shape=(
            jax.ShapeDtypeStruct(sums[1:], jnp.float32),
            jax.ShapeDtypeStruct(sums[1:], jnp.bfloat16),
        ),
        in_specs=[SMEM] + [VMEM] * 2,
        out_specs=[VMEM] * 2,
        name="pair",
        compiler_params=params(6),
        cost_estimate=pl.CostEstimate(flops=300_000, bytes_accessed=1_000_000, transcendentals=0),
    )(low_z, keep, got)
    got = lax.ppermute(send, "z_low", [(0, 1), (1, 0)])
    hidden, both = pl.pallas_call(
        hidden_kernel,
        out_shape=(
            jax.ShapeDtypeStruct((units, 128), jnp.bfloat16),
            jax.ShapeDtypeStruct((units + 128, 128), jnp.bfloat16),
        ),
        in_specs=[VMEM] * 3,
        out_specs=[VMEM] * 2,
        name="hidden",
        compiler_params=params(6),
        cost_estimate=pl.CostEstimate(
            flops=1_000_000, bytes_accessed=700_000, transcendentals=60_000
        ),
    )(keep, got, stream_turned)

    both = turned(both)
    stream = pl.pallas_call(
        copy_kernel,
        out_shape=jax.ShapeDtypeStruct((128, 128), jnp.bfloat16),
        in_specs=[VMEM],
        out_specs=VMEM,
        compiler_params=params(1),
    )(both)
    hidden_turned = both[:units]
    upper, lower = over_y_and_x(over_z(hidden_turned), units // 2, two_step_ring)
    other = lax.ppermute(hidden, "core", [(0, 1), (1, 0)])
    near = jnp.stack([hidden, other])
    far = lax.ppermute(near, "z_low", [(0, 1), (1, 0)])
    hessian = pl.pallas_call(
        hessian_kernel,
        out_shape=jax.ShapeDtypeStruct((units, 16 * units), jnp.float32),
        in_specs=[SMEM] * 3 + [VMEM] * 12,
        out_specs=pl.BlockSpec(memory_space=pltpu.HBM),
        scratch_shapes=[
            pltpu.VMEM((units, 4 * LANES), jnp.bfloat16),
            pltpu.VMEM((2, 4 * units, 4 * LANES), jnp.bfloat16),
            pltpu.VMEM((4, units, 4 * units), jnp.float32),
            pltpu.SemaphoreType.DMA((8,)),
        ],
        name="hessian",
        compiler_params=params(14),
        cost_estimate=pl.CostEstimate(flops=822_000_000, bytes_accessed=7_100_000, transcendentals=0),
    )(order, groups, place, near, far, *upper, *lower)
    return (pruned_weight, stream, hessian)


def solution(mesh):
    split = Mesh(mesh.devices.reshape(2, 2, 4, 4, 4), (*DP, *MP))
    return jax.shard_map(
        body,
        mesh=split,
        in_specs=(
            P(DP, MP),
            P(DP, MP),
            P(MP, DP),
            P(MP, None),
            P(None, DP),
            P(MP),
            P(DP, None, MP),
        ),
        out_specs=(P(MP, DP), P(DP, MP), P(MP, DP)),
        check_vma=False,
    )
```

```python
import jax
import jax.numpy as jnp
from jax import lax
from jax.experimental import pallas as pl
from jax.experimental.pallas import tpu as pltpu
from jax.sharding import Mesh
from jax.sharding import PartitionSpec as P


DP = ("z_low", "core")
MP = ("y", "z_high", "x")
NT = (((1,), (1,)), ((), ()))
VMEM = pl.BlockSpec(memory_space=pltpu.VMEM)
SMEM = pl.BlockSpec(memory_space=pltpu.SMEM)
LANES = 128
STEPS = (1, 3, 2)


def params(mib):
    return pltpu.CompilerParams(vmem_limit_bytes=mib << 20)


def copy_for_each(x, axis):
    size = lax.axis_size(axis)
    return lax.all_to_all(jnp.broadcast_to(x[None], (size, *x.shape)), axis, 0, 0, tiled=True)


def turned(x):
    pairs = [(d * 4 + y, y * 4 + d) for d in range(4) for y in range(4)]
    return lax.ppermute(x, (*DP, "y"), pairs)


def round_trip(x, axis):
    blocks = [x]
    for step in STEPS:
        blocks.append(lax.ppermute(x, axis, [(k, (k + step) % 4) for k in range(4)]))
    return blocks


def two_step_ring(x, axis):
    up = [(k, (k + 1) % 4) for k in range(4)]
    down = [(k, (k + 3) % 4) for k in range(4)]
    half = x.shape[0] // 2
    below, above = lax.ppermute(x, axis, up), lax.ppermute(x, axis, down)
    far = [lax.ppermute(below[:half], axis, up), lax.ppermute(above[half:], axis, down)]
    return [x, below, above, *far]


def over_y_and_x(x, half, large=round_trip):
    lower = jnp.stack(round_trip(x[:, half:], "x"))
    upper = jnp.stack(round_trip(x[:, :half], "y"))
    upper = large(upper, "x")
    lower = large(lower, "y")
    return upper, lower


def over_z(x):
    pair = jnp.stack([x, lax.ppermute(x, "z_high", [(k, k ^ 1) for k in range(4)])])
    return jnp.concatenate(
        [pair, lax.ppermute(pair, "z_high", [(k, k ^ 2) for k in range(4)])]
    )


def senders(axis):
    here = lax.axis_index(axis)
    return jnp.stack([here] + [(here + 4 - step) % 4 for step in STEPS]).astype(jnp.int32)


def solve_kernel(weight_hbm, mask_hbm, factor_hbm, errors_ref, weight_ref, mask_ref, factor_ref, sems):
    size = factor_ref.shape[0]
    copies = [
        pltpu.make_async_copy(source.at[:, pl.ds(0, size)], target, sems.at[k])
        for k, (source, target) in enumerate(
            ((weight_hbm, weight_ref), (mask_hbm, mask_ref), (factor_hbm, factor_ref))
        )
    ]
    for copy in copies:
        copy.start()
    for copy in copies:
        copy.wait()
    step = 8
    count = size // step
    factor = factor_ref[...]
    row = lax.broadcasted_iota(jnp.int32, (size, size), 0)
    col = lax.broadcasted_iota(jnp.int32, (size, size), 1)
    pivots = jnp.sum(jnp.where(row == col, factor, 0.0), axis=1, keepdims=True)
    kept = mask_ref[...].astype(jnp.float32).T
    cutting = (1.0 - kept) / pivots
    current = weight_ref[...].astype(jnp.float32).T
    turned_factor = factor.T
    cur = [current[b * step : (b + 1) * step] for b in range(count)]
    fac = [turned_factor[b * step : (b + 1) * step] for b in range(count)]
    wide = (step, current.shape[1])
    place = lax.broadcasted_iota(jnp.int32, wide, 0)
    done = []
    for b in range(count):
        block = cur[b]
        cut_block = cutting[b * step : (b + 1) * step]
        fresh = []
        for i in range(step):
            j = b * step + i
            value = jnp.broadcast_to(cut_block[i : i + 1] * block[i : i + 1], wide)
            fresh.append(value)
            if i + 1 < step:
                reach = jnp.broadcast_to(fac[b][:, j : j + 1], wide)
                block = block - jnp.where(place > i, reach, 0.0) * value
        for v in range(b + 1, count):
            total = cur[v]
            for i in range(step):
                j = b * step + i
                total = total - jnp.broadcast_to(fac[v][:, j : j + 1], wide) * fresh[i]
            cur[v] = total
        rows = fresh[0]
        for i in range(1, step):
            rows = jnp.where(place == i, fresh[i], rows)
        done.append(rows)
    errors_ref[...] = jnp.concatenate(done, axis=0).T


def corner(shape):
    return pl.BlockSpec(shape, lambda i: (0,) * len(shape))


def solved_errors(weight, mask, factor):
    return pl.pallas_call(
        solve_kernel,
        out_shape=jax.ShapeDtypeStruct(mask.shape, jnp.float32),
        in_specs=[pl.BlockSpec(memory_space=pltpu.HBM)] * 3,
        out_specs=VMEM,
        scratch_shapes=[
            pltpu.VMEM(mask.shape, weight.dtype),
            pltpu.VMEM(mask.shape, mask.dtype),
            pltpu.VMEM(mask.shape, factor.dtype),
            pltpu.SemaphoreType.DMA((3,)),
        ],
        name="solve",
        compiler_params=params(60),
        cost_estimate=pl.CostEstimate(flops=20_000_000, bytes_accessed=300_000, transcendentals=0),
    )(weight, mask, factor)


def update_kernel(place_ref, errors_ref, factor_ref, weight_ref, mask_ref, out_ref):
    updated = weight_ref[...].astype(jnp.float32) - lax.dot_general(
        errors_ref[0],
        factor_ref[...],
        (((1,), (0,)), ((), ())),
        precision=lax.Precision.HIGHEST,
        preferred_element_type=jnp.float32,
    )
    width = mask_ref.shape[1]
    kept = jnp.where(place_ref[0] == 0, mask_ref[...].astype(jnp.float32), 1.0)
    out_ref[:, :width] = (updated[:, :width] * kept).astype(jnp.bfloat16)
    out_ref[:, width:] = updated[:, width:].astype(jnp.bfloat16)


def updated_weight(place, errors, factor, weight, mask):
    return pl.pallas_call(
        update_kernel,
        grid=(1,),
        out_shape=jax.ShapeDtypeStruct(weight.shape, jnp.bfloat16),
        in_specs=[
            SMEM,
            corner((1, *errors.shape[1:])),
            corner(factor.shape),
            corner(weight.shape),
            corner(mask.shape),
        ],
        out_specs=corner(weight.shape),
        name="update",
        compiler_params=params(12),
        cost_estimate=pl.CostEstimate(flops=400_000_000, bytes_accessed=2_200_000, transcendentals=0),
    )(place, errors, factor, weight, mask)


def columns_at(ref, block):
    return ref[:, pl.ds(pl.multiple_of(block * LANES, LANES), LANES)]


def ordered_columns(ref, from_ref, z_here):
    return jnp.concatenate(
        [
            columns_at(ref, jnp.bitwise_xor(z_here, z) * 4 + from_ref[r])
            for r in range(4)
            for z in range(4)
        ],
        axis=1,
    )


def project_kernel(from_ref, core_ref, *refs):
    mine, other, weight_ref, out_ref = refs[:4], refs[4:8], refs[8], refs[9]
    weight = ordered_columns(weight_ref, from_ref, 0)
    for low in range(2):
        for source, core in ((mine, core_ref[0]), (other, 1 - core_ref[0])):
            tokens = jnp.concatenate(
                [source[r][z * 2 + low] for r in range(4) for z in range(4)], axis=1
            )
            out_ref[low * 2 + core] = lax.dot_general(
                tokens, weight, NT, preferred_element_type=jnp.float32
            ).astype(out_ref.dtype)


def stream_kernel(parts_ref, residual_ref, stream_ref, block_ref):
    rows = stream_ref.shape[0]
    total = residual_ref[:rows].astype(jnp.float32)
    for k in range(4):
        total = total + parts_ref[k].astype(jnp.float32)
    stream = total.astype(jnp.bfloat16)
    stream_ref[...] = stream
    wide = stream.astype(jnp.float32)
    gain = residual_ref[rows : rows + 16].astype(jnp.float32)[:1]
    square = lax.dot_general(
        jnp.ones((8, LANES), jnp.float32),
        wide * wide,
        NT,
        precision=lax.Precision.HIGHEST,
        preferred_element_type=jnp.float32,
    )
    high = square.astype(jnp.bfloat16).astype(jnp.float32)
    first = lax.broadcasted_iota(jnp.int32, square.shape, 0) == 0
    pair = jnp.where(first, high, square - high)
    block_ref[...] = jnp.concatenate([wide * gain, pair], axis=0).astype(jnp.bfloat16)


def copy_kernel(in_ref, out_ref):
    rows = out_ref.shape[0]
    out_ref[...] = in_ref[in_ref.shape[0] - rows :]


def order_kernel(from_ref, high_ref, weight_ref, out_ref):
    out_ref[...] = ordered_columns(weight_ref, from_ref, high_ref[0])


def gate_up_kernel(group_ref, core_ref, *refs):
    upper, lower, weight_ref = refs[:4], refs[4:8], refs[8]
    keep_ref, send_ref, part_ref = refs[9:]
    half = upper[0].shape[2]
    weight = weight_ref[...]
    units = weight.shape[0]
    places = [(r, z) for r in range(4) for z in range(4)]
    for k in range(4):
        high = jnp.concatenate([upper[r][k, z] for r, z in places], axis=1)
        low = jnp.concatenate([lower[k][r, z, :half] for r, z in places], axis=1)
        square = jnp.zeros((8, LANES), jnp.float32)
        for r, z in places:
            square = square + lower[k][r, z, half:].astype(jnp.float32)
        group = group_ref[k]
        part_ref[group, :units, :] = lax.dot_general(
            weight,
            jnp.concatenate([high, low], axis=0),
            NT,
            preferred_element_type=jnp.float32,
        )
        total = jnp.broadcast_to(square[0:1] + square[1:2], square.shape)
        big = total.astype(jnp.bfloat16).astype(jnp.float32)
        part_ref[group, units:, :] = jnp.concatenate([big, total - big], axis=0)
    for low_z in range(2):
        keep_ref[low_z] = part_ref[low_z * 2 + core_ref[0]]
        send_ref[low_z] = part_ref[low_z * 2 + 1 - core_ref[0]].astype(jnp.bfloat16)


def pair_kernel(low_ref, keep_ref, got_ref, next_keep_ref, next_send_ref):
    for ref, place in ((next_keep_ref, low_ref[0]), (next_send_ref, 1 - low_ref[0])):
        total = keep_ref[place] + got_ref[place].astype(jnp.float32)
        rows = total.shape[0] - 16
        ref[:rows] = total[:rows].astype(ref.dtype)
        square = total[rows : rows + 8] + total[rows + 8 :]
        big = square.astype(jnp.bfloat16).astype(jnp.float32)
        ref[rows:] = jnp.concatenate([big, square - big], axis=0).astype(ref.dtype)


def hidden_kernel(keep_ref, got_ref, stream_ref, hidden_ref, both_ref):
    units = hidden_ref.shape[0]
    sums = keep_ref[...] + got_ref[...].astype(jnp.float32)
    square = sums[2 * units : 2 * units + 8] + sums[2 * units + 8 :]
    inverse = lax.rsqrt(square / 8192 + 1e-05)[:1]
    gate = sums[:units] * inverse
    up = sums[units : 2 * units] * inverse
    hidden = (gate / (1.0 + jnp.exp(-gate)) * up).astype(jnp.bfloat16)
    hidden_ref[...] = hidden
    both_ref[:units] = hidden
    both_ref[units:] = stream_ref[...]


def hessian_kernel(from_ref, group_ref, high_ref, place_ref, near_ref, far_ref, *refs):
    upper, lower, out_hbm = refs[:5], refs[5:10], refs[10]
    left_ref, right_ref, result_ref, sems = refs[11:]
    units = near_ref.shape[1]
    half = units // 2
    wide = 4 * units

    def lanes(group):
        return pl.ds(pl.multiple_of(group * LANES, LANES), LANES)

    def piece(blocks, large, small, z):
        if large < 3:
            return blocks[large][small, z]
        return blocks[3 + small // 2][small % 2, z]

    place = place_ref[0]
    for k in range(2):
        left_ref[:, lanes(jnp.bitwise_xor(place, k))] = near_ref[k]
        left_ref[:, lanes(jnp.bitwise_xor(place, 2 + k))] = far_ref[k]

    def written(z, part):
        rows = pl.ds(part * half, half)
        base = pl.multiple_of(jnp.bitwise_xor(high_ref[0], z) * wide, LANES)
        return pltpu.make_async_copy(
            result_ref.at[z, rows, :],
            out_hbm.at[rows, pl.ds(base, wide)],
            sems.at[z * 2 + part],
        )

    @pl.loop(0, 4)
    def _(z):
        right = right_ref.at[z % 2]
        for r in range(4):
            base = from_ref[r] * units
            for k in range(4):
                group = lanes(group_ref[k])
                right[pl.ds(pl.multiple_of(base, 16), half), group] = piece(upper, r, k, z)
                right[pl.ds(pl.multiple_of(base + half, 16), half), group] = piece(lower, k, r, z)
        result_ref[z] = (2.0 / 512) * lax.dot_general(
            left_ref[...], right[...], NT, preferred_element_type=jnp.float32
        )
        for part in range(2):
            written(z, part).start()

    for z in range(4):
        for part in range(2):
            written(z, part).wait()


def body(attn_out, residual, output_weight, prune_mask, inverse_factor, norm_gain, gate_up_weight):
    units = gate_up_weight.shape[2]
    place = lax.axis_index(DP).astype(jnp.int32)[None]
    order = senders("x")
    groups = senders("y")
    core = lax.axis_index("core").astype(jnp.int32)[None]
    low_z = lax.axis_index("z_low").astype(jnp.int32)[None]
    high_z = lax.axis_index("z_high").astype(jnp.int32)[None]

    mine = copy_for_each(attn_out, ("z_high", "z_low"))
    mine = round_trip(mine, "x")
    other = [lax.ppermute(block, "core", [(0, 1), (1, 0)]) for block in mine]
    gain_rows = jnp.broadcast_to(norm_gain[None], (16, norm_gain.shape[0]))
    residual_turned = turned(jnp.concatenate([residual, gain_rows], axis=0))

    solved = solved_errors(output_weight, prune_mask, inverse_factor)
    errors = lax.all_gather(solved, DP)
    pruned_weight = updated_weight(place, errors, inverse_factor, output_weight, prune_mask)
    weight_turned = turned(pruned_weight)

    parts = pl.pallas_call(
        project_kernel,
        out_shape=jax.ShapeDtypeStruct((4, 128, 128), jnp.bfloat16),
        in_specs=[SMEM] * 2 + [VMEM] * 9,
        out_specs=VMEM,
        name="project",
        compiler_params=params(10),
        cost_estimate=pl.CostEstimate(flops=268_000_000, bytes_accessed=2_700_000, transcendentals=0),
    )(order, core, *mine, *other, weight_turned)
    parts = lax.all_to_all(parts, "y", 0, 0, tiled=True)
    stream_turned, block = pl.pallas_call(
        stream_kernel,
        out_shape=(
            jax.ShapeDtypeStruct((128, 128), jnp.bfloat16),
            jax.ShapeDtypeStruct((136, 128), jnp.bfloat16),
        ),
        in_specs=[VMEM] * 2,
        out_specs=[VMEM] * 2,
        name="stream",
        compiler_params=params(4),
        cost_estimate=pl.CostEstimate(flops=300_000, bytes_accessed=250_000, transcendentals=0),
    )(parts, residual_turned)
    flat_weight = gate_up_weight.transpose(1, 2, 0).reshape(2 * units, -1)
    flat_weight = pl.pallas_call(
        order_kernel,
        out_shape=jax.ShapeDtypeStruct(flat_weight.shape, jnp.bfloat16),
        in_specs=[SMEM, SMEM, VMEM],
        out_specs=VMEM,
        name="order",
        compiler_params=params(8),
        cost_estimate=pl.CostEstimate(flops=0, bytes_accessed=3_700_000, transcendentals=0),
    )(order, high_z, flat_weight)
    upper, lower = over_y_and_x(over_z(block), 64)
    sums = (2, 2 * units + 16, 128)
    keep, send = pl.pallas_call(
        gate_up_kernel,
        out_shape=(
            jax.ShapeDtypeStruct(sums, jnp.float32),
            jax.ShapeDtypeStruct(sums, jnp.bfloat16),
        ),
        in_specs=[SMEM] * 2 + [VMEM] * 9,
        out_specs=[VMEM] * 2,
        scratch_shapes=[pltpu.VMEM((4, *sums[1:]), jnp.float32)],
        name="gate_up",
        compiler_params=params(14),
        cost_estimate=pl.CostEstimate(
            flops=940_000_000, bytes_accessed=4_300_000, transcendentals=0
        ),
    )(groups, core, *upper, *lower, flat_weight)
    got = lax.ppermute(send, "core", [(0, 1), (1, 0)])
    keep, send = pl.pallas_call(
        pair_kernel,
        out_shape=(
            jax.ShapeDtypeStruct(sums[1:], jnp.float32),
            jax.ShapeDtypeStruct(sums[1:], jnp.bfloat16),
        ),
        in_specs=[SMEM] + [VMEM] * 2,
        out_specs=[VMEM] * 2,
        name="pair",
        compiler_params=params(6),
        cost_estimate=pl.CostEstimate(flops=300_000, bytes_accessed=1_000_000, transcendentals=0),
    )(low_z, keep, got)
    got = lax.ppermute(send, "z_low", [(0, 1), (1, 0)])
    hidden, both = pl.pallas_call(
        hidden_kernel,
        out_shape=(
            jax.ShapeDtypeStruct((units, 128), jnp.bfloat16),
            jax.ShapeDtypeStruct((units + 128, 128), jnp.bfloat16),
        ),
        in_specs=[VMEM] * 3,
        out_specs=[VMEM] * 2,
        name="hidden",
        compiler_params=params(6),
        cost_estimate=pl.CostEstimate(
            flops=1_000_000, bytes_accessed=700_000, transcendentals=60_000
        ),
    )(keep, got, stream_turned)

    both = turned(both)
    stream = pl.pallas_call(
        copy_kernel,
        out_shape=jax.ShapeDtypeStruct((128, 128), jnp.bfloat16),
        in_specs=[VMEM],
        out_specs=VMEM,
        compiler_params=params(1),
    )(both)
    hidden_turned = both[:units]
    upper, lower = over_y_and_x(over_z(hidden_turned), units // 2, two_step_ring)
    other = lax.ppermute(hidden, "core", [(0, 1), (1, 0)])
    near = jnp.stack([hidden, other])
    far = lax.ppermute(near, "z_low", [(0, 1), (1, 0)])
    hessian = pl.pallas_call(
        hessian_kernel,
        out_shape=jax.ShapeDtypeStruct((units, 16 * units), jnp.float32),
        in_specs=[SMEM] * 4 + [VMEM] * 12,
        out_specs=pl.BlockSpec(memory_space=pltpu.HBM),
        scratch_shapes=[
            pltpu.VMEM((units, 4 * LANES), jnp.bfloat16),
            pltpu.VMEM((2, 4 * units, 4 * LANES), jnp.bfloat16),
            pltpu.VMEM((4, units, 4 * units), jnp.float32),
            pltpu.SemaphoreType.DMA((8,)),
        ],
        name="hessian",
        compiler_params=params(14),
        cost_estimate=pl.CostEstimate(flops=822_000_000, bytes_accessed=7_100_000, transcendentals=0),
    )(order, groups, high_z, place, near, far, *upper, *lower)
    return (pruned_weight, stream, hessian)


def solution(mesh):
    split = Mesh(mesh.devices.reshape(2, 2, 4, 4, 4), (*DP, *MP))
    return jax.shard_map(
        body,
        mesh=split,
        in_specs=(
            P(DP, MP),
            P(DP, MP),
            P(MP, DP),
            P(MP, None),
            P(None, DP),
            P(MP),
            P(DP, None, MP),
        ),
        out_specs=(P(MP, DP), P(DP, MP), P(MP, DP)),
        check_vma=False,
    )
```

```python
import jax
import jax.numpy as jnp
from jax import lax
from jax.experimental import pallas as pl
from jax.experimental.pallas import tpu as pltpu
from jax.sharding import Mesh
from jax.sharding import PartitionSpec as P


DP = ("z_low", "core")
MP = ("y", "z_high", "x")
NT = (((1,), (1,)), ((), ()))
VMEM = pl.BlockSpec(memory_space=pltpu.VMEM)
SMEM = pl.BlockSpec(memory_space=pltpu.SMEM)
LANES = 128
STEPS = (1, 3, 2)


def params(mib):
    return pltpu.CompilerParams(vmem_limit_bytes=mib << 20)


def copy_for_each(x, axis):
    size = lax.axis_size(axis)
    return lax.all_to_all(jnp.broadcast_to(x[None], (size, *x.shape)), axis, 0, 0, tiled=True)


def turned(x):
    pairs = [(d * 4 + y, y * 4 + d) for d in range(4) for y in range(4)]
    return lax.ppermute(x, (*DP, "y"), pairs)


def round_trip(x, axis):
    blocks = [x]
    for step in STEPS:
        blocks.append(lax.ppermute(x, axis, [(k, (k + step) % 4) for k in range(4)]))
    return blocks


def two_step_ring(x, axis):
    up = [(k, (k + 1) % 4) for k in range(4)]
    down = [(k, (k + 3) % 4) for k in range(4)]
    half = x.shape[0] // 2
    below, above = lax.ppermute(x, axis, up), lax.ppermute(x, axis, down)
    far = [lax.ppermute(below[:half], axis, up), lax.ppermute(above[half:], axis, down)]
    return [x, below, above, *far]


def over_y_and_x(x, half, large=round_trip):
    lower = jnp.stack(round_trip(x[:, half:], "x"))
    upper = jnp.stack(round_trip(x[:, :half], "y"))
    upper = large(upper, "x")
    lower = large(lower, "y")
    return upper, lower


def over_z(x):
    return copy_for_each(x, "z_high")


def senders(axis):
    here = lax.axis_index(axis)
    return jnp.stack([here] + [(here + 4 - step) % 4 for step in STEPS]).astype(jnp.int32)


def solve_kernel(weight_hbm, mask_hbm, factor_hbm, errors_ref, weight_ref, mask_ref, factor_ref, sems):
    size = factor_ref.shape[0]
    copies = [
        pltpu.make_async_copy(source.at[:, pl.ds(0, size)], target, sems.at[k])
        for k, (source, target) in enumerate(
            ((weight_hbm, weight_ref), (mask_hbm, mask_ref), (factor_hbm, factor_ref))
        )
    ]
    for copy in copies:
        copy.start()
    for copy in copies:
        copy.wait()
    step = 8
    count = size // step
    factor = factor_ref[...]
    row = lax.broadcasted_iota(jnp.int32, (size, size), 0)
    col = lax.broadcasted_iota(jnp.int32, (size, size), 1)
    pivots = jnp.sum(jnp.where(row == col, factor, 0.0), axis=1, keepdims=True)
    kept = mask_ref[...].astype(jnp.float32).T
    cutting = (1.0 - kept) / pivots
    current = weight_ref[...].astype(jnp.float32).T
    turned_factor = factor.T
    cur = [current[b * step : (b + 1) * step] for b in range(count)]
    fac = [turned_factor[b * step : (b + 1) * step] for b in range(count)]
    wide = (step, current.shape[1])
    place = lax.broadcasted_iota(jnp.int32, wide, 0)
    done = []
    for b in range(count):
        block = cur[b]
        cut_block = cutting[b * step : (b + 1) * step]
        fresh = []
        for i in range(step):
            j = b * step + i
            value = jnp.broadcast_to(cut_block[i : i + 1] * block[i : i + 1], wide)
            fresh.append(value)
            if i + 1 < step:
                reach = jnp.broadcast_to(fac[b][:, j : j + 1], wide)
                block = block - jnp.where(place > i, reach, 0.0) * value
        for v in range(b + 1, count):
            total = cur[v]
            for i in range(step):
                j = b * step + i
                total = total - jnp.broadcast_to(fac[v][:, j : j + 1], wide) * fresh[i]
            cur[v] = total
        rows = fresh[0]
        for i in range(1, step):
            rows = jnp.where(place == i, fresh[i], rows)
        done.append(rows)
    errors_ref[...] = jnp.concatenate(done, axis=0).T


def corner(shape):
    return pl.BlockSpec(shape, lambda i: (0,) * len(shape))


def solved_errors(weight, mask, factor):
    return pl.pallas_call(
        solve_kernel,
        out_shape=jax.ShapeDtypeStruct(mask.shape, jnp.float32),
        in_specs=[pl.BlockSpec(memory_space=pltpu.HBM)] * 3,
        out_specs=VMEM,
        scratch_shapes=[
            pltpu.VMEM(mask.shape, weight.dtype),
            pltpu.VMEM(mask.shape, mask.dtype),
            pltpu.VMEM(mask.shape, factor.dtype),
            pltpu.SemaphoreType.DMA((3,)),
        ],
        name="solve",
        compiler_params=params(60),
        cost_estimate=pl.CostEstimate(flops=20_000_000, bytes_accessed=300_000, transcendentals=0),
    )(weight, mask, factor)


def update_kernel(place_ref, errors_ref, factor_ref, weight_ref, mask_ref, out_ref):
    updated = weight_ref[...].astype(jnp.float32) - lax.dot_general(
        errors_ref[0],
        factor_ref[...],
        (((1,), (0,)), ((), ())),
        precision=lax.Precision.HIGHEST,
        preferred_element_type=jnp.float32,
    )
    width = mask_ref.shape[1]
    kept = jnp.where(place_ref[0] == 0, mask_ref[...].astype(jnp.float32), 1.0)
    out_ref[:, :width] = (updated[:, :width] * kept).astype(jnp.bfloat16)
    out_ref[:, width:] = updated[:, width:].astype(jnp.bfloat16)


def updated_weight(place, errors, factor, weight, mask):
    return pl.pallas_call(
        update_kernel,
        grid=(1,),
        out_shape=jax.ShapeDtypeStruct(weight.shape, jnp.bfloat16),
        in_specs=[
            SMEM,
            corner((1, *errors.shape[1:])),
            corner(factor.shape),
            corner(weight.shape),
            corner(mask.shape),
        ],
        out_specs=corner(weight.shape),
        name="update",
        compiler_params=params(12),
        cost_estimate=pl.CostEstimate(flops=400_000_000, bytes_accessed=2_200_000, transcendentals=0),
    )(place, errors, factor, weight, mask)


def columns_at(ref, block):
    return ref[:, pl.ds(pl.multiple_of(block * LANES, LANES), LANES)]


def ordered_columns(ref, from_ref):
    return jnp.concatenate(
        [columns_at(ref, z * 4 + from_ref[r]) for r in range(4) for z in range(4)], axis=1
    )


def project_kernel(from_ref, core_ref, *refs):
    mine, other, weight_ref, out_ref = refs[:4], refs[4:8], refs[8], refs[9]
    weight = ordered_columns(weight_ref, from_ref)
    for low in range(2):
        for source, core in ((mine, core_ref[0]), (other, 1 - core_ref[0])):
            tokens = jnp.concatenate(
                [source[r][z * 2 + low] for r in range(4) for z in range(4)], axis=1
            )
            out_ref[low * 2 + core] = lax.dot_general(
                tokens, weight, NT, preferred_element_type=jnp.float32
            ).astype(out_ref.dtype)


def stream_kernel(parts_ref, residual_ref, stream_ref, block_ref):
    rows = stream_ref.shape[0]
    total = residual_ref[:rows].astype(jnp.float32)
    for k in range(4):
        total = total + parts_ref[k].astype(jnp.float32)
    stream = total.astype(jnp.bfloat16)
    stream_ref[...] = stream
    wide = stream.astype(jnp.float32)
    gain = residual_ref[rows : rows + 16].astype(jnp.float32)[:1]
    square = lax.dot_general(
        jnp.ones((8, LANES), jnp.float32),
        wide * wide,
        NT,
        precision=lax.Precision.HIGHEST,
        preferred_element_type=jnp.float32,
    )
    high = square.astype(jnp.bfloat16).astype(jnp.float32)
    first = lax.broadcasted_iota(jnp.int32, square.shape, 0) == 0
    pair = jnp.where(first, high, square - high)
    block_ref[...] = jnp.concatenate([wide * gain, pair], axis=0).astype(jnp.bfloat16)


def copy_kernel(in_ref, out_ref):
    rows = out_ref.shape[0]
    out_ref[...] = in_ref[in_ref.shape[0] - rows :]


def order_kernel(from_ref, weight_ref, out_ref):
    out_ref[...] = ordered_columns(weight_ref, from_ref)


def gate_up_kernel(group_ref, core_ref, *refs):
    upper, lower, weight_ref = refs[:4], refs[4:8], refs[8]
    keep_ref, send_ref, part_ref = refs[9:]
    half = upper[0].shape[2]
    weight = weight_ref[...]
    units = weight.shape[0]
    places = [(r, z) for r in range(4) for z in range(4)]
    for k in range(4):
        high = jnp.concatenate([upper[r][k, z] for r, z in places], axis=1)
        low = jnp.concatenate([lower[k][r, z, :half] for r, z in places], axis=1)
        square = jnp.zeros((8, LANES), jnp.float32)
        for r, z in places:
            square = square + lower[k][r, z, half:].astype(jnp.float32)
        group = group_ref[k]
        part_ref[group, :units, :] = lax.dot_general(
            weight,
            jnp.concatenate([high, low], axis=0),
            NT,
            preferred_element_type=jnp.float32,
        )
        total = jnp.broadcast_to(square[0:1] + square[1:2], square.shape)
        big = total.astype(jnp.bfloat16).astype(jnp.float32)
        part_ref[group, units:, :] = jnp.concatenate([big, total - big], axis=0)
    for low_z in range(2):
        keep_ref[low_z] = part_ref[low_z * 2 + core_ref[0]]
        send_ref[low_z] = part_ref[low_z * 2 + 1 - core_ref[0]].astype(jnp.bfloat16)


def pair_kernel(low_ref, keep_ref, got_ref, next_keep_ref, next_send_ref):
    for ref, place in ((next_keep_ref, low_ref[0]), (next_send_ref, 1 - low_ref[0])):
        total = keep_ref[place] + got_ref[place].astype(jnp.float32)
        rows = total.shape[0] - 16
        ref[:rows] = total[:rows].astype(ref.dtype)
        square = total[rows : rows + 8] + total[rows + 8 :]
        big = square.astype(jnp.bfloat16).astype(jnp.float32)
        ref[rows:] = jnp.concatenate([big, square - big], axis=0).astype(ref.dtype)


def hidden_kernel(keep_ref, got_ref, stream_ref, hidden_ref, both_ref):
    units = hidden_ref.shape[0]
    sums = keep_ref[...] + got_ref[...].astype(jnp.float32)
    square = sums[2 * units : 2 * units + 8] + sums[2 * units + 8 :]
    inverse = lax.rsqrt(square / 8192 + 1e-05)[:1]
    gate = sums[:units] * inverse
    up = sums[units : 2 * units] * inverse
    hidden = (gate / (1.0 + jnp.exp(-gate)) * up).astype(jnp.bfloat16)
    hidden_ref[...] = hidden
    both_ref[:units] = hidden
    both_ref[units:] = stream_ref[...]


def hessian_kernel(from_ref, group_ref, place_ref, near_ref, far_ref, *refs):
    upper, lower, out_hbm = refs[:5], refs[5:10], refs[10]
    left_ref, right_ref, result_ref, sems = refs[11:]
    units = near_ref.shape[1]
    half = units // 2
    wide = 4 * units

    def lanes(group):
        return pl.ds(pl.multiple_of(group * LANES, LANES), LANES)

    def piece(blocks, large, small, z):
        if large < 3:
            return blocks[large][small, z]
        return blocks[3 + small // 2][small % 2, z]

    place = place_ref[0]
    for k in range(2):
        left_ref[:, lanes(jnp.bitwise_xor(place, k))] = near_ref[k]
        left_ref[:, lanes(jnp.bitwise_xor(place, 2 + k))] = far_ref[k]
    copies = []
    for z in range(4):
        right = right_ref.at[z % 2]
        for r in range(4):
            base = from_ref[r] * units
            for k in range(4):
                group = lanes(group_ref[k])
                right[pl.ds(pl.multiple_of(base, 16), half), group] = piece(upper, r, k, z)
                right[pl.ds(pl.multiple_of(base + half, 16), half), group] = piece(lower, k, r, z)
        result_ref[z] = (2.0 / 512) * lax.dot_general(
            left_ref[...], right[...], NT, preferred_element_type=jnp.float32
        )
        for part in range(2):
            rows = slice(part * half, (part + 1) * half)
            copy = pltpu.make_async_copy(
                result_ref.at[z, rows, :],
                out_hbm.at[rows, z * wide : (z + 1) * wide],
                sems.at[z * 2 + part],
            )
            copy.start()
            copies.append(copy)
    for copy in copies:
        copy.wait()


def body(attn_out, residual, output_weight, prune_mask, inverse_factor, norm_gain, gate_up_weight):
    units = gate_up_weight.shape[2]
    place = lax.axis_index(DP).astype(jnp.int32)[None]
    order = senders("x")
    groups = senders("y")
    core = lax.axis_index("core").astype(jnp.int32)[None]
    low_z = lax.axis_index("z_low").astype(jnp.int32)[None]

    mine = copy_for_each(attn_out, ("z_high", "z_low"))
    mine = round_trip(mine, "x")
    other = [lax.ppermute(block, "core", [(0, 1), (1, 0)]) for block in mine]
    gain_rows = jnp.broadcast_to(norm_gain[None], (16, norm_gain.shape[0]))
    residual_turned = turned(jnp.concatenate([residual, gain_rows], axis=0))

    solved = solved_errors(output_weight, prune_mask, inverse_factor)
    errors = lax.all_gather(solved, DP)
    pruned_weight = updated_weight(place, errors, inverse_factor, output_weight, prune_mask)
    weight_turned = turned(pruned_weight)

    parts = pl.pallas_call(
        project_kernel,
        out_shape=jax.ShapeDtypeStruct((4, 128, 128), jnp.bfloat16),
        in_specs=[SMEM] * 2 + [VMEM] * 9,
        out_specs=VMEM,
        name="project",
        compiler_params=params(10),
        cost_estimate=pl.CostEstimate(flops=268_000_000, bytes_accessed=2_700_000, transcendentals=0),
    )(order, core, *mine, *other, weight_turned)
    parts = lax.all_to_all(parts, "y", 0, 0, tiled=True)
    stream_turned, block = pl.pallas_call(
        stream_kernel,
        out_shape=(
            jax.ShapeDtypeStruct((128, 128), jnp.bfloat16),
            jax.ShapeDtypeStruct((136, 128), jnp.bfloat16),
        ),
        in_specs=[VMEM] * 2,
        out_specs=[VMEM] * 2,
        name="stream",
        compiler_params=params(4),
        cost_estimate=pl.CostEstimate(flops=300_000, bytes_accessed=250_000, transcendentals=0),
    )(parts, residual_turned)
    flat_weight = gate_up_weight.transpose(1, 2, 0).reshape(2 * units, -1)
    flat_weight = pl.pallas_call(
        order_kernel,
        out_shape=jax.ShapeDtypeStruct(flat_weight.shape, jnp.bfloat16),
        in_specs=[SMEM, VMEM],
        out_specs=VMEM,
        name="order",
        compiler_params=params(8),
        cost_estimate=pl.CostEstimate(flops=0, bytes_accessed=3_700_000, transcendentals=0),
    )(order, flat_weight)
    upper, lower = over_y_and_x(over_z(block), 64)
    sums = (2, 2 * units + 16, 128)
    keep, send = pl.pallas_call(
        gate_up_kernel,
        out_shape=(
            jax.ShapeDtypeStruct(sums, jnp.float32),
            jax.ShapeDtypeStruct(sums, jnp.bfloat16),
        ),
        in_specs=[SMEM] * 2 + [VMEM] * 9,
        out_specs=[VMEM] * 2,
        scratch_shapes=[pltpu.VMEM((4, *sums[1:]), jnp.float32)],
        name="gate_up",
        compiler_params=params(14),
        cost_estimate=pl.CostEstimate(
            flops=940_000_000, bytes_accessed=4_300_000, transcendentals=0
        ),
    )(groups, core, *upper, *lower, flat_weight)
    got = lax.ppermute(send, "core", [(0, 1), (1, 0)])
    keep, send = pl.pallas_call(
        pair_kernel,
        out_shape=(
            jax.ShapeDtypeStruct(sums[1:], jnp.float32),
            jax.ShapeDtypeStruct(sums[1:], jnp.bfloat16),
        ),
        in_specs=[SMEM] + [VMEM] * 2,
        out_specs=[VMEM] * 2,
        name="pair",
        compiler_params=params(6),
        cost_estimate=pl.CostEstimate(flops=300_000, bytes_accessed=1_000_000, transcendentals=0),
    )(low_z, keep, got)
    got = lax.ppermute(send, "z_low", [(0, 1), (1, 0)])
    hidden, both = pl.pallas_call(
        hidden_kernel,
        out_shape=(
            jax.ShapeDtypeStruct((units, 128), jnp.bfloat16),
            jax.ShapeDtypeStruct((units + 128, 128), jnp.bfloat16),
        ),
        in_specs=[VMEM] * 3,
        out_specs=[VMEM] * 2,
        name="hidden",
        compiler_params=params(6),
        cost_estimate=pl.CostEstimate(
            flops=1_000_000, bytes_accessed=700_000, transcendentals=60_000
        ),
    )(keep, got, stream_turned)

    both = turned(both)
    stream = pl.pallas_call(
        copy_kernel,
        out_shape=jax.ShapeDtypeStruct((128, 128), jnp.bfloat16),
        in_specs=[VMEM],
        out_specs=VMEM,
        compiler_params=params(1),
    )(both)
    hidden_turned = both[:units]
    upper, lower = over_y_and_x(over_z(hidden_turned), units // 2, two_step_ring)
    other = lax.ppermute(hidden, "core", [(0, 1), (1, 0)])
    near = jnp.stack([hidden, other])
    far = lax.ppermute(near, "z_low", [(0, 1), (1, 0)])
    hessian = pl.pallas_call(
        hessian_kernel,
        out_shape=jax.ShapeDtypeStruct((units, 16 * units), jnp.float32),
        in_specs=[SMEM] * 3 + [VMEM] * 12,
        out_specs=pl.BlockSpec(memory_space=pltpu.HBM),
        scratch_shapes=[
            pltpu.VMEM((units, 4 * LANES), jnp.bfloat16),
            pltpu.VMEM((2, 4 * units, 4 * LANES), jnp.bfloat16),
            pltpu.VMEM((4, units, 4 * units), jnp.float32),
            pltpu.SemaphoreType.DMA((8,)),
        ],
        name="hessian",
        compiler_params=params(14),
        cost_estimate=pl.CostEstimate(flops=822_000_000, bytes_accessed=7_100_000, transcendentals=0),
    )(order, groups, place, near, far, *upper, *lower)
    return (pruned_weight, stream, hessian)


def solution(mesh):
    split = Mesh(mesh.devices.reshape(2, 2, 4, 4, 4), (*DP, *MP))
    return jax.shard_map(
        body,
        mesh=split,
        in_specs=(
            P(DP, MP),
            P(DP, MP),
            P(MP, DP),
            P(MP, None),
            P(None, DP),
            P(MP),
            P(DP, None, MP),
        ),
        out_specs=(P(MP, DP), P(DP, MP), P(MP, DP)),
        check_vma=False,
    )
```

```python
import jax
import jax.numpy as jnp
from jax import lax
from jax.experimental import pallas as pl
from jax.experimental.pallas import tpu as pltpu
from jax.sharding import Mesh
from jax.sharding import PartitionSpec as P


DP = ("z_low", "core")
MP = ("y", "z_high", "x")
NT = (((1,), (1,)), ((), ()))
VMEM = pl.BlockSpec(memory_space=pltpu.VMEM)
SMEM = pl.BlockSpec(memory_space=pltpu.SMEM)
LANES = 128
STEPS = (1, 3, 2)


def params(mib):
    return pltpu.CompilerParams(vmem_limit_bytes=mib << 20)


def copy_for_each(x, axis):
    size = lax.axis_size(axis)
    return lax.all_to_all(jnp.broadcast_to(x[None], (size, *x.shape)), axis, 0, 0, tiled=True)


def turned(x):
    pairs = [(d * 4 + y, y * 4 + d) for d in range(4) for y in range(4)]
    return lax.ppermute(x, (*DP, "y"), pairs)


def round_trip(x, axis):
    blocks = [x]
    for step in STEPS:
        blocks.append(lax.ppermute(x, axis, [(k, (k + step) % 4) for k in range(4)]))
    return blocks


def two_step_ring(x, axis):
    up = [(k, (k + 1) % 4) for k in range(4)]
    down = [(k, (k + 3) % 4) for k in range(4)]
    half = x.shape[0] // 2
    below, above = lax.ppermute(x, axis, up), lax.ppermute(x, axis, down)
    far = [lax.ppermute(below[:half], axis, up), lax.ppermute(above[half:], axis, down)]
    return [x, below, above, *far]


def over_y_and_x(x, half, large=round_trip):
    lower = jnp.stack(round_trip(x[:, half:], "x"))
    upper = jnp.stack(round_trip(x[:, :half], "y"))
    upper = large(upper, "x")
    lower = large(lower, "y")
    return upper, lower


def over_z(x):
    return copy_for_each(x, "z_high")


def senders(axis):
    here = lax.axis_index(axis)
    return jnp.stack([here] + [(here + 4 - step) % 4 for step in STEPS]).astype(jnp.int32)


def solve_kernel(weight_hbm, mask_hbm, factor_hbm, errors_ref, weight_ref, mask_ref, factor_ref, sems):
    size = factor_ref.shape[0]
    copies = [
        pltpu.make_async_copy(source.at[:, pl.ds(0, size)], target, sems.at[k])
        for k, (source, target) in enumerate(
            ((weight_hbm, weight_ref), (mask_hbm, mask_ref), (factor_hbm, factor_ref))
        )
    ]
    for copy in copies:
        copy.start()
    for copy in copies:
        copy.wait()
    step = 8
    count = size // step
    factor = factor_ref[...]
    row = lax.broadcasted_iota(jnp.int32, (size, size), 0)
    col = lax.broadcasted_iota(jnp.int32, (size, size), 1)
    pivots = jnp.sum(jnp.where(row == col, factor, 0.0), axis=1, keepdims=True)
    kept = mask_ref[...].astype(jnp.float32).T
    cutting = (1.0 - kept) / pivots
    current = weight_ref[...].astype(jnp.float32).T
    turned_factor = factor.T
    cur = [current[b * step : (b + 1) * step] for b in range(count)]
    fac = [turned_factor[b * step : (b + 1) * step] for b in range(count)]
    wide = (step, current.shape[1])
    place = lax.broadcasted_iota(jnp.int32, wide, 0)
    done = []
    for b in range(count):
        block = cur[b]
        cut_block = cutting[b * step : (b + 1) * step]
        fresh = []
        for i in range(step):
            j = b * step + i
            value = jnp.broadcast_to(cut_block[i : i + 1] * block[i : i + 1], wide)
            fresh.append(value)
            if i + 1 < step:
                reach = jnp.broadcast_to(fac[b][:, j : j + 1], wide)
                block = block - jnp.where(place > i, reach, 0.0) * value
        for v in range(b + 1, count):
            total = cur[v]
            for i in range(step):
                j = b * step + i
                total = total - jnp.broadcast_to(fac[v][:, j : j + 1], wide) * fresh[i]
            cur[v] = total
        rows = fresh[0]
        for i in range(1, step):
            rows = jnp.where(place == i, fresh[i], rows)
        done.append(rows)
    errors_ref[...] = jnp.concatenate(done, axis=0).T


def corner(shape):
    return pl.BlockSpec(shape, lambda i: (0,) * len(shape))


def solved_errors(weight, mask, factor):
    return pl.pallas_call(
        solve_kernel,
        out_shape=jax.ShapeDtypeStruct(mask.shape, jnp.float32),
        in_specs=[pl.BlockSpec(memory_space=pltpu.HBM)] * 3,
        out_specs=VMEM,
        scratch_shapes=[
            pltpu.VMEM(mask.shape, weight.dtype),
            pltpu.VMEM(mask.shape, mask.dtype),
            pltpu.VMEM(mask.shape, factor.dtype),
            pltpu.SemaphoreType.DMA((3,)),
        ],
        name="solve",
        compiler_params=params(60),
        cost_estimate=pl.CostEstimate(flops=20_000_000, bytes_accessed=300_000, transcendentals=0),
    )(weight, mask, factor)


def update_kernel(place_ref, errors_ref, factor_ref, weight_ref, mask_ref, out_ref, copy_ref):
    updated = weight_ref[...].astype(jnp.float32) - lax.dot_general(
        errors_ref[0],
        factor_ref[...],
        (((1,), (0,)), ((), ())),
        precision=lax.Precision.HIGHEST,
        preferred_element_type=jnp.float32,
    )
    width = mask_ref.shape[1]
    kept = jnp.where(place_ref[0] == 0, mask_ref[...].astype(jnp.float32), 1.0)
    for ref in (out_ref, copy_ref):
        ref[:, :width] = (updated[:, :width] * kept).astype(jnp.bfloat16)
        ref[:, width:] = updated[:, width:].astype(jnp.bfloat16)


def updated_weight(place, errors, factor, weight, mask):
    return pl.pallas_call(
        update_kernel,
        grid=(1,),
        out_shape=(jax.ShapeDtypeStruct(weight.shape, jnp.bfloat16),) * 2,
        in_specs=[
            SMEM,
            corner((1, *errors.shape[1:])),
            corner(factor.shape),
            corner(weight.shape),
            corner(mask.shape),
        ],
        out_specs=(corner(weight.shape),) * 2,
        name="update",
        compiler_params=params(12),
        cost_estimate=pl.CostEstimate(flops=400_000_000, bytes_accessed=2_200_000, transcendentals=0),
    )(place, errors, factor, weight, mask)


def columns_at(ref, block):
    return ref[:, pl.ds(pl.multiple_of(block * LANES, LANES), LANES)]


def ordered_columns(ref, from_ref):
    return jnp.concatenate(
        [columns_at(ref, z * 4 + from_ref[r]) for r in range(4) for z in range(4)], axis=1
    )


def project_kernel(from_ref, core_ref, *refs):
    mine, other, weight_ref, out_ref = refs[:4], refs[4:8], refs[8], refs[9]
    weight = ordered_columns(weight_ref, from_ref)
    for low in range(2):
        for source, core in ((mine, core_ref[0]), (other, 1 - core_ref[0])):
            tokens = jnp.concatenate(
                [source[r][z * 2 + low] for r in range(4) for z in range(4)], axis=1
            )
            out_ref[low * 2 + core] = lax.dot_general(
                tokens, weight, NT, preferred_element_type=jnp.float32
            ).astype(out_ref.dtype)


def stream_kernel(parts_ref, residual_ref, stream_ref, block_ref):
    rows = stream_ref.shape[0]
    total = residual_ref[:rows].astype(jnp.float32)
    for k in range(4):
        total = total + parts_ref[k].astype(jnp.float32)
    stream = total.astype(jnp.bfloat16)
    stream_ref[...] = stream
    wide = stream.astype(jnp.float32)
    gain = residual_ref[rows : rows + 16].astype(jnp.float32)[:1]
    square = lax.dot_general(
        jnp.ones((8, LANES), jnp.float32),
        wide * wide,
        NT,
        precision=lax.Precision.HIGHEST,
        preferred_element_type=jnp.float32,
    )
    high = square.astype(jnp.bfloat16).astype(jnp.float32)
    first = lax.broadcasted_iota(jnp.int32, square.shape, 0) == 0
    pair = jnp.where(first, high, square - high)
    block_ref[...] = jnp.concatenate([wide * gain, pair], axis=0).astype(jnp.bfloat16)


def copy_kernel(in_ref, out_ref):
    rows = out_ref.shape[0]
    out_ref[...] = in_ref[in_ref.shape[0] - rows :]


def order_kernel(from_ref, weight_ref, out_ref):
    out_ref[...] = ordered_columns(weight_ref, from_ref)


def gate_up_kernel(group_ref, core_ref, *refs):
    upper, lower, weight_ref = refs[:4], refs[4:8], refs[8]
    keep_ref, send_ref, part_ref = refs[9:]
    half = upper[0].shape[2]
    weight = weight_ref[...]
    units = weight.shape[0]
    places = [(r, z) for r in range(4) for z in range(4)]
    for k in range(4):
        high = jnp.concatenate([upper[r][k, z] for r, z in places], axis=1)
        low = jnp.concatenate([lower[k][r, z, :half] for r, z in places], axis=1)
        square = jnp.zeros((8, LANES), jnp.float32)
        for r, z in places:
            square = square + lower[k][r, z, half:].astype(jnp.float32)
        group = group_ref[k]
        part_ref[group, :units, :] = lax.dot_general(
            weight,
            jnp.concatenate([high, low], axis=0),
            NT,
            preferred_element_type=jnp.float32,
        )
        total = jnp.broadcast_to(square[0:1] + square[1:2], square.shape)
        big = total.astype(jnp.bfloat16).astype(jnp.float32)
        part_ref[group, units:, :] = jnp.concatenate([big, total - big], axis=0)
    for low_z in range(2):
        keep_ref[low_z] = part_ref[low_z * 2 + core_ref[0]]
        send_ref[low_z] = part_ref[low_z * 2 + 1 - core_ref[0]].astype(jnp.bfloat16)


def pair_kernel(low_ref, keep_ref, got_ref, next_keep_ref, next_send_ref):
    for ref, place in ((next_keep_ref, low_ref[0]), (next_send_ref, 1 - low_ref[0])):
        total = keep_ref[place] + got_ref[place].astype(jnp.float32)
        rows = total.shape[0] - 16
        ref[:rows] = total[:rows].astype(ref.dtype)
        square = total[rows : rows + 8] + total[rows + 8 :]
        big = square.astype(jnp.bfloat16).astype(jnp.float32)
        ref[rows:] = jnp.concatenate([big, square - big], axis=0).astype(ref.dtype)


def hidden_kernel(keep_ref, got_ref, stream_ref, hidden_ref, both_ref):
    units = hidden_ref.shape[0]
    sums = keep_ref[...] + got_ref[...].astype(jnp.float32)
    square = sums[2 * units : 2 * units + 8] + sums[2 * units + 8 :]
    inverse = lax.rsqrt(square / 8192 + 1e-05)[:1]
    gate = sums[:units] * inverse
    up = sums[units : 2 * units] * inverse
    hidden = (gate / (1.0 + jnp.exp(-gate)) * up).astype(jnp.bfloat16)
    hidden_ref[...] = hidden
    both_ref[:units] = hidden
    both_ref[units:] = stream_ref[...]


def hessian_kernel(from_ref, group_ref, place_ref, near_ref, far_ref, *refs):
    upper, lower, out_hbm = refs[:5], refs[5:10], refs[10]
    left_ref, right_ref, result_ref, sems = refs[11:]
    units = near_ref.shape[1]
    half = units // 2
    wide = 4 * units

    def lanes(group):
        return pl.ds(pl.multiple_of(group * LANES, LANES), LANES)

    def piece(blocks, large, small, z):
        if large < 3:
            return blocks[large][small, z]
        return blocks[3 + small // 2][small % 2, z]

    place = place_ref[0]
    for k in range(2):
        left_ref[:, lanes(jnp.bitwise_xor(place, k))] = near_ref[k]
        left_ref[:, lanes(jnp.bitwise_xor(place, 2 + k))] = far_ref[k]
    copies = []
    for z in range(4):
        right = right_ref.at[z % 2]
        for r in range(4):
            base = from_ref[r] * units
            for k in range(4):
                group = lanes(group_ref[k])
                right[pl.ds(pl.multiple_of(base, 16), half), group] = piece(upper, r, k, z)
                right[pl.ds(pl.multiple_of(base + half, 16), half), group] = piece(lower, k, r, z)
        result_ref[z] = (2.0 / 512) * lax.dot_general(
            left_ref[...], right[...], NT, preferred_element_type=jnp.float32
        )
        for part in range(2):
            rows = slice(part * half, (part + 1) * half)
            copy = pltpu.make_async_copy(
                result_ref.at[z, rows, :],
                out_hbm.at[rows, z * wide : (z + 1) * wide],
                sems.at[z * 2 + part],
            )
            copy.start()
            copies.append(copy)
    for copy in copies:
        copy.wait()


def body(attn_out, residual, output_weight, prune_mask, inverse_factor, norm_gain, gate_up_weight):
    units = gate_up_weight.shape[2]
    place = lax.axis_index(DP).astype(jnp.int32)[None]
    order = senders("x")
    groups = senders("y")
    core = lax.axis_index("core").astype(jnp.int32)[None]
    low_z = lax.axis_index("z_low").astype(jnp.int32)[None]

    mine = copy_for_each(attn_out, ("z_high", "z_low"))
    mine = round_trip(mine, "x")
    other = [lax.ppermute(block, "core", [(0, 1), (1, 0)]) for block in mine]
    gain_rows = jnp.broadcast_to(norm_gain[None], (16, norm_gain.shape[0]))
    residual_turned = turned(jnp.concatenate([residual, gain_rows], axis=0))

    solved = solved_errors(output_weight, prune_mask, inverse_factor)
    errors = lax.all_gather(solved, DP)
    pruned_weight, weight_copy = updated_weight(place, errors, inverse_factor, output_weight, prune_mask)
    weight_turned = turned(weight_copy)

    parts = pl.pallas_call(
        project_kernel,
        out_shape=jax.ShapeDtypeStruct((4, 128, 128), jnp.bfloat16),
        in_specs=[SMEM] * 2 + [VMEM] * 9,
        out_specs=VMEM,
        name="project",
        compiler_params=params(10),
        cost_estimate=pl.CostEstimate(flops=268_000_000, bytes_accessed=2_700_000, transcendentals=0),
    )(order, core, *mine, *other, weight_turned)
    parts = lax.all_to_all(parts, "y", 0, 0, tiled=True)
    stream_turned, block = pl.pallas_call(
        stream_kernel,
        out_shape=(
            jax.ShapeDtypeStruct((128, 128), jnp.bfloat16),
            jax.ShapeDtypeStruct((136, 128), jnp.bfloat16),
        ),
        in_specs=[VMEM] * 2,
        out_specs=[VMEM] * 2,
        name="stream",
        compiler_params=params(4),
        cost_estimate=pl.CostEstimate(flops=300_000, bytes_accessed=250_000, transcendentals=0),
    )(parts, residual_turned)
    flat_weight = gate_up_weight.transpose(1, 2, 0).reshape(2 * units, -1)
    flat_weight = pl.pallas_call(
        order_kernel,
        out_shape=jax.ShapeDtypeStruct(flat_weight.shape, jnp.bfloat16),
        in_specs=[SMEM, VMEM],
        out_specs=VMEM,
        name="order",
        compiler_params=params(8),
        cost_estimate=pl.CostEstimate(flops=0, bytes_accessed=3_700_000, transcendentals=0),
    )(order, flat_weight)
    upper, lower = over_y_and_x(over_z(block), 64)
    sums = (2, 2 * units + 16, 128)
    keep, send = pl.pallas_call(
        gate_up_kernel,
        out_shape=(
            jax.ShapeDtypeStruct(sums, jnp.float32),
            jax.ShapeDtypeStruct(sums, jnp.bfloat16),
        ),
        in_specs=[SMEM] * 2 + [VMEM] * 9,
        out_specs=[VMEM] * 2,
        scratch_shapes=[pltpu.VMEM((4, *sums[1:]), jnp.float32)],
        name="gate_up",
        compiler_params=params(14),
        cost_estimate=pl.CostEstimate(
            flops=940_000_000, bytes_accessed=4_300_000, transcendentals=0
        ),
    )(groups, core, *upper, *lower, flat_weight)
    got = lax.ppermute(send, "core", [(0, 1), (1, 0)])
    keep, send = pl.pallas_call(
        pair_kernel,
        out_shape=(
            jax.ShapeDtypeStruct(sums[1:], jnp.float32),
            jax.ShapeDtypeStruct(sums[1:], jnp.bfloat16),
        ),
        in_specs=[SMEM] + [VMEM] * 2,
        out_specs=[VMEM] * 2,
        name="pair",
        compiler_params=params(6),
        cost_estimate=pl.CostEstimate(flops=300_000, bytes_accessed=1_000_000, transcendentals=0),
    )(low_z, keep, got)
    got = lax.ppermute(send, "z_low", [(0, 1), (1, 0)])
    hidden, both = pl.pallas_call(
        hidden_kernel,
        out_shape=(
            jax.ShapeDtypeStruct((units, 128), jnp.bfloat16),
            jax.ShapeDtypeStruct((units + 128, 128), jnp.bfloat16),
        ),
        in_specs=[VMEM] * 3,
        out_specs=[VMEM] * 2,
        name="hidden",
        compiler_params=params(6),
        cost_estimate=pl.CostEstimate(
            flops=1_000_000, bytes_accessed=700_000, transcendentals=60_000
        ),
    )(keep, got, stream_turned)

    both = turned(both)
    stream = pl.pallas_call(
        copy_kernel,
        out_shape=jax.ShapeDtypeStruct((128, 128), jnp.bfloat16),
        in_specs=[VMEM],
        out_specs=VMEM,
        compiler_params=params(1),
    )(both)
    hidden_turned = both[:units]
    upper, lower = over_y_and_x(over_z(hidden_turned), units // 2, two_step_ring)
    other = lax.ppermute(hidden, "core", [(0, 1), (1, 0)])
    near = jnp.stack([hidden, other])
    far = lax.ppermute(near, "z_low", [(0, 1), (1, 0)])
    hessian = pl.pallas_call(
        hessian_kernel,
        out_shape=jax.ShapeDtypeStruct((units, 16 * units), jnp.float32),
        in_specs=[SMEM] * 3 + [VMEM] * 12,
        out_specs=pl.BlockSpec(memory_space=pltpu.HBM),
        scratch_shapes=[
            pltpu.VMEM((units, 4 * LANES), jnp.bfloat16),
            pltpu.VMEM((2, 4 * units, 4 * LANES), jnp.bfloat16),
            pltpu.VMEM((4, units, 4 * units), jnp.float32),
            pltpu.SemaphoreType.DMA((8,)),
        ],
        name="hessian",
        compiler_params=params(14),
        cost_estimate=pl.CostEstimate(flops=822_000_000, bytes_accessed=7_100_000, transcendentals=0),
    )(order, groups, place, near, far, *upper, *lower)
    return (pruned_weight, stream, hessian)


def solution(mesh):
    split = Mesh(mesh.devices.reshape(2, 2, 4, 4, 4), (*DP, *MP))
    return jax.shard_map(
        body,
        mesh=split,
        in_specs=(
            P(DP, MP),
            P(DP, MP),
            P(MP, DP),
            P(MP, None),
            P(None, DP),
            P(MP),
            P(DP, None, MP),
        ),
        out_specs=(P(MP, DP), P(DP, MP), P(MP, DP)),
        check_vma=False,
    )
```

```python
import jax
import jax.numpy as jnp
from jax import lax
from jax.experimental import pallas as pl
from jax.experimental.pallas import tpu as pltpu
from jax.sharding import Mesh
from jax.sharding import PartitionSpec as P


DP = ("z_low", "core")
MP = ("y", "z_high", "x")
NT = (((1,), (1,)), ((), ()))
VMEM = pl.BlockSpec(memory_space=pltpu.VMEM)
SMEM = pl.BlockSpec(memory_space=pltpu.SMEM)
LANES = 128
STEPS = (1, 3, 2)


def params(mib):
    return pltpu.CompilerParams(vmem_limit_bytes=mib << 20)


def copy_for_each(x, axis):
    size = lax.axis_size(axis)
    return lax.all_to_all(jnp.broadcast_to(x[None], (size, *x.shape)), axis, 0, 0, tiled=True)


def turned(x):
    pairs = [(d * 4 + y, y * 4 + d) for d in range(4) for y in range(4)]
    return lax.ppermute(x, (*DP, "y"), pairs)


def round_trip(x, axis):
    blocks = [x]
    for step in STEPS:
        blocks.append(lax.ppermute(x, axis, [(k, (k + step) % 4) for k in range(4)]))
    return blocks


def two_step_ring(x, axis):
    up = [(k, (k + 1) % 4) for k in range(4)]
    down = [(k, (k + 3) % 4) for k in range(4)]
    half = x.shape[0] // 2
    below, above = lax.ppermute(x, axis, up), lax.ppermute(x, axis, down)
    far = [lax.ppermute(below[:half], axis, up), lax.ppermute(above[half:], axis, down)]
    return [x, below, above, *far]


def over_y_and_x(x, half, large=round_trip):
    lower = jnp.stack(round_trip(x[:, half:], "x"))
    upper = jnp.stack(round_trip(x[:, :half], "y"))
    upper = large(upper, "x")
    lower = large(lower, "y")
    return upper, lower


def over_z(x):
    return copy_for_each(x, "z_high")


def senders(axis):
    here = lax.axis_index(axis)
    return jnp.stack([here] + [(here + 4 - step) % 4 for step in STEPS]).astype(jnp.int32)


def solve_kernel(weight_hbm, mask_hbm, factor_hbm, errors_ref, weight_ref, mask_ref, factor_ref, sems):
    size = factor_ref.shape[0]
    copies = [
        pltpu.make_async_copy(source.at[:, pl.ds(0, size)], target, sems.at[k])
        for k, (source, target) in enumerate(
            ((weight_hbm, weight_ref), (mask_hbm, mask_ref), (factor_hbm, factor_ref))
        )
    ]
    for copy in copies:
        copy.start()
    for copy in copies:
        copy.wait()
    step = 8
    count = size // step
    factor = factor_ref[...]
    row = lax.broadcasted_iota(jnp.int32, (size, size), 0)
    col = lax.broadcasted_iota(jnp.int32, (size, size), 1)
    pivots = jnp.sum(jnp.where(row == col, factor, 0.0), axis=1, keepdims=True)
    kept = mask_ref[...].astype(jnp.float32).T
    cutting = (1.0 - kept) / pivots
    current = weight_ref[...].astype(jnp.float32).T
    turned_factor = factor.T
    cur = [current[b * step : (b + 1) * step] for b in range(count)]
    fac = [turned_factor[b * step : (b + 1) * step] for b in range(count)]
    wide = (step, current.shape[1])
    place = lax.broadcasted_iota(jnp.int32, wide, 0)
    done = []
    for b in range(count):
        block = cur[b]
        cut_block = cutting[b * step : (b + 1) * step]
        fresh = []
        for i in range(step):
            j = b * step + i
            value = jnp.broadcast_to(cut_block[i : i + 1] * block[i : i + 1], wide)
            fresh.append(value)
            if i + 1 < step:
                reach = jnp.broadcast_to(fac[b][:, j : j + 1], wide)
                block = block - jnp.where(place > i, reach, 0.0) * value
        for v in range(b + 1, count):
            total = cur[v]
            for i in range(step):
                j = b * step + i
                total = total - jnp.broadcast_to(fac[v][:, j : j + 1], wide) * fresh[i]
            cur[v] = total
        rows = fresh[0]
        for i in range(1, step):
            rows = jnp.where(place == i, fresh[i], rows)
        done.append(rows)
    errors_ref[...] = jnp.concatenate(done, axis=0).T


def corner(shape):
    return pl.BlockSpec(shape, lambda i: (0,) * len(shape))


def solved_errors(weight, mask, factor):
    return pl.pallas_call(
        solve_kernel,
        out_shape=jax.ShapeDtypeStruct(mask.shape, jnp.float32),
        in_specs=[pl.BlockSpec(memory_space=pltpu.HBM)] * 3,
        out_specs=VMEM,
        scratch_shapes=[
            pltpu.VMEM(mask.shape, weight.dtype),
            pltpu.VMEM(mask.shape, mask.dtype),
            pltpu.VMEM(mask.shape, factor.dtype),
            pltpu.SemaphoreType.DMA((3,)),
        ],
        name="solve",
        compiler_params=params(60),
        cost_estimate=pl.CostEstimate(flops=20_000_000, bytes_accessed=300_000, transcendentals=0),
    )(weight, mask, factor)


def update_kernel(place_ref, errors_ref, factor_ref, weight_ref, mask_ref, out_ref, copy_ref):
    updated = weight_ref[...].astype(jnp.float32) - lax.dot_general(
        errors_ref[0],
        factor_ref[...],
        (((1,), (0,)), ((), ())),
        precision=lax.Precision.HIGHEST,
        preferred_element_type=jnp.float32,
    )
    width = mask_ref.shape[1]
    kept = jnp.where(place_ref[0] == 0, mask_ref[...].astype(jnp.float32), 1.0)
    for ref in (out_ref, copy_ref):
        ref[:, :width] = (updated[:, :width] * kept).astype(jnp.bfloat16)
        ref[:, width:] = updated[:, width:].astype(jnp.bfloat16)


def updated_weight(place, errors, factor, weight, mask):
    return pl.pallas_call(
        update_kernel,
        grid=(1,),
        out_shape=(jax.ShapeDtypeStruct(weight.shape, jnp.bfloat16),) * 2,
        in_specs=[
            SMEM,
            corner((1, *errors.shape[1:])),
            corner(factor.shape),
            corner(weight.shape),
            corner(mask.shape),
        ],
        out_specs=(corner(weight.shape),) * 2,
        name="update",
        compiler_params=params(12),
        cost_estimate=pl.CostEstimate(flops=400_000_000, bytes_accessed=2_200_000, transcendentals=0),
    )(place, errors, factor, weight, mask)


def columns_at(ref, block):
    return ref[:, pl.ds(pl.multiple_of(block * LANES, LANES), LANES)]


def ordered_columns(ref, from_ref):
    return jnp.concatenate(
        [columns_at(ref, z * 4 + from_ref[r]) for r in range(4) for z in range(4)], axis=1
    )


def project_kernel(from_ref, core_ref, *refs):
    mine, other, weight_ref, out_ref = refs[:4], refs[4:8], refs[8], refs[9]
    weight = ordered_columns(weight_ref, from_ref)
    for low in range(2):
        for source, core in ((mine, core_ref[0]), (other, 1 - core_ref[0])):
            tokens = jnp.concatenate(
                [source[r][z * 2 + low] for r in range(4) for z in range(4)], axis=1
            )
            out_ref[low * 2 + core] = lax.dot_general(
                tokens, weight, NT, preferred_element_type=jnp.float32
            ).astype(out_ref.dtype)


def stream_kernel(parts_ref, residual_ref, stream_ref, block_ref):
    rows = stream_ref.shape[0]
    total = residual_ref[:rows].astype(jnp.float32)
    for k in range(4):
        total = total + parts_ref[k].astype(jnp.float32)
    stream = total.astype(jnp.bfloat16)
    stream_ref[...] = stream
    wide = stream.astype(jnp.float32)
    gain = residual_ref[rows : rows + 16].astype(jnp.float32)[:1]
    square = lax.dot_general(
        jnp.ones((8, LANES), jnp.float32),
        wide * wide,
        NT,
        precision=lax.Precision.HIGHEST,
        preferred_element_type=jnp.float32,
    )
    high = square.astype(jnp.bfloat16).astype(jnp.float32)
    first = lax.broadcasted_iota(jnp.int32, square.shape, 0) == 0
    pair = jnp.where(first, high, square - high)
    block_ref[...] = jnp.concatenate([wide * gain, pair], axis=0).astype(jnp.bfloat16)


def copy_kernel(in_ref, out_ref):
    rows = out_ref.shape[0]
    out_ref[...] = in_ref[in_ref.shape[0] - rows :]


def order_kernel(from_ref, weight_ref, out_ref):
    out_ref[...] = ordered_columns(weight_ref, from_ref)


def gate_up_kernel(group_ref, core_ref, *refs):
    upper, lower, weight_ref = refs[:4], refs[4:8], refs[8]
    keep_ref, send_ref, part_ref = refs[9:]
    half = upper[0].shape[2]
    weight = weight_ref[...]
    units = weight.shape[0]
    places = [(r, z) for r in range(4) for z in range(4)]
    for first in (0, 2):
        tokens = []
        for k in (first, first + 1):
            tokens.append(jnp.concatenate([upper[r][k, z] for r, z in places], axis=1))
            tokens.append(jnp.concatenate([lower[k][r, z, :half] for r, z in places], axis=1))
        both = lax.dot_general(
            weight, jnp.concatenate(tokens, axis=0), NT, preferred_element_type=jnp.float32
        )
        for k in (first, first + 1):
            square = jnp.zeros((8, LANES), jnp.float32)
            for r, z in places:
                square = square + lower[k][r, z, half:].astype(jnp.float32)
            group = group_ref[k]
            at = (k - first) * LANES
            part_ref[group, :units, :] = both[:, at : at + LANES]
            total = jnp.broadcast_to(square[0:1] + square[1:2], square.shape)
            big = total.astype(jnp.bfloat16).astype(jnp.float32)
            part_ref[group, units:, :] = jnp.concatenate([big, total - big], axis=0)
    for low_z in range(2):
        keep_ref[low_z] = part_ref[low_z * 2 + core_ref[0]]
        send_ref[low_z] = part_ref[low_z * 2 + 1 - core_ref[0]].astype(jnp.bfloat16)


def pair_kernel(low_ref, keep_ref, got_ref, next_keep_ref, next_send_ref):
    for ref, place in ((next_keep_ref, low_ref[0]), (next_send_ref, 1 - low_ref[0])):
        total = keep_ref[place] + got_ref[place].astype(jnp.float32)
        rows = total.shape[0] - 16
        ref[:rows] = total[:rows].astype(ref.dtype)
        square = total[rows : rows + 8] + total[rows + 8 :]
        big = square.astype(jnp.bfloat16).astype(jnp.float32)
        ref[rows:] = jnp.concatenate([big, square - big], axis=0).astype(ref.dtype)


def hidden_kernel(keep_ref, got_ref, stream_ref, hidden_ref, both_ref):
    units = hidden_ref.shape[0]
    sums = keep_ref[...] + got_ref[...].astype(jnp.float32)
    square = sums[2 * units : 2 * units + 8] + sums[2 * units + 8 :]
    inverse = lax.rsqrt(square / 8192 + 1e-05)[:1]
    gate = sums[:units] * inverse
    up = sums[units : 2 * units] * inverse
    hidden = (gate / (1.0 + jnp.exp(-gate)) * up).astype(jnp.bfloat16)
    hidden_ref[...] = hidden
    both_ref[:units] = hidden
    both_ref[units:] = stream_ref[...]


def hessian_kernel(from_ref, group_ref, place_ref, near_ref, far_ref, *refs):
    upper, lower, out_hbm = refs[:5], refs[5:10], refs[10]
    left_ref, right_ref, result_ref, sems = refs[11:]
    units = near_ref.shape[1]
    half = units // 2
    wide = 4 * units

    def lanes(group):
        return pl.ds(pl.multiple_of(group * LANES, LANES), LANES)

    def piece(blocks, large, small, z):
        if large < 3:
            return blocks[large][small, z]
        return blocks[3 + small // 2][small % 2, z]

    place = place_ref[0]
    for k in range(2):
        left_ref[:, lanes(jnp.bitwise_xor(place, k))] = near_ref[k]
        left_ref[:, lanes(jnp.bitwise_xor(place, 2 + k))] = far_ref[k]
    copies = []
    for z in range(4):
        right = right_ref.at[z % 2]
        for r in range(4):
            base = from_ref[r] * units
            for k in range(4):
                group = lanes(group_ref[k])
                right[pl.ds(pl.multiple_of(base, 16), half), group] = piece(upper, r, k, z)
                right[pl.ds(pl.multiple_of(base + half, 16), half), group] = piece(lower, k, r, z)
        result_ref[z] = (2.0 / 512) * lax.dot_general(
            left_ref[...], right[...], NT, preferred_element_type=jnp.float32
        )
        for part in range(2):
            rows = slice(part * half, (part + 1) * half)
            copy = pltpu.make_async_copy(
                result_ref.at[z, rows, :],
                out_hbm.at[rows, z * wide : (z + 1) * wide],
                sems.at[z * 2 + part],
            )
            copy.start()
            copies.append(copy)
    for copy in copies:
        copy.wait()


def body(attn_out, residual, output_weight, prune_mask, inverse_factor, norm_gain, gate_up_weight):
    units = gate_up_weight.shape[2]
    place = lax.axis_index(DP).astype(jnp.int32)[None]
    order = senders("x")
    groups = senders("y")
    core = lax.axis_index("core").astype(jnp.int32)[None]
    low_z = lax.axis_index("z_low").astype(jnp.int32)[None]

    mine = copy_for_each(attn_out, ("z_high", "z_low"))
    mine = round_trip(mine, "x")
    other = [lax.ppermute(block, "core", [(0, 1), (1, 0)]) for block in mine]
    gain_rows = jnp.broadcast_to(norm_gain[None], (16, norm_gain.shape[0]))
    residual_turned = turned(jnp.concatenate([residual, gain_rows], axis=0))

    solved = solved_errors(output_weight, prune_mask, inverse_factor)
    errors = lax.all_gather(solved, DP)
    pruned_weight, weight_copy = updated_weight(place, errors, inverse_factor, output_weight, prune_mask)
    weight_turned = turned(weight_copy)

    parts = pl.pallas_call(
        project_kernel,
        out_shape=jax.ShapeDtypeStruct((4, 128, 128), jnp.bfloat16),
        in_specs=[SMEM] * 2 + [VMEM] * 9,
        out_specs=VMEM,
        name="project",
        compiler_params=params(10),
        cost_estimate=pl.CostEstimate(flops=268_000_000, bytes_accessed=2_700_000, transcendentals=0),
    )(order, core, *mine, *other, weight_turned)
    parts = lax.all_to_all(parts, "y", 0, 0, tiled=True)
    stream_turned, block = pl.pallas_call(
        stream_kernel,
        out_shape=(
            jax.ShapeDtypeStruct((128, 128), jnp.bfloat16),
            jax.ShapeDtypeStruct((136, 128), jnp.bfloat16),
        ),
        in_specs=[VMEM] * 2,
        out_specs=[VMEM] * 2,
        name="stream",
        compiler_params=params(4),
        cost_estimate=pl.CostEstimate(flops=300_000, bytes_accessed=250_000, transcendentals=0),
    )(parts, residual_turned)
    flat_weight = gate_up_weight.transpose(1, 2, 0).reshape(2 * units, -1)
    flat_weight = pl.pallas_call(
        order_kernel,
        out_shape=jax.ShapeDtypeStruct(flat_weight.shape, jnp.bfloat16),
        in_specs=[SMEM, VMEM],
        out_specs=VMEM,
        name="order",
        compiler_params=params(8),
        cost_estimate=pl.CostEstimate(flops=0, bytes_accessed=3_700_000, transcendentals=0),
    )(order, flat_weight)
    upper, lower = over_y_and_x(over_z(block), 64)
    sums = (2, 2 * units + 16, 128)
    keep, send = pl.pallas_call(
        gate_up_kernel,
        out_shape=(
            jax.ShapeDtypeStruct(sums, jnp.float32),
            jax.ShapeDtypeStruct(sums, jnp.bfloat16),
        ),
        in_specs=[SMEM] * 2 + [VMEM] * 9,
        out_specs=[VMEM] * 2,
        scratch_shapes=[pltpu.VMEM((4, *sums[1:]), jnp.float32)],
        name="gate_up",
        compiler_params=params(14),
        cost_estimate=pl.CostEstimate(
            flops=940_000_000, bytes_accessed=4_300_000, transcendentals=0
        ),
    )(groups, core, *upper, *lower, flat_weight)
    got = lax.ppermute(send, "core", [(0, 1), (1, 0)])
    keep, send = pl.pallas_call(
        pair_kernel,
        out_shape=(
            jax.ShapeDtypeStruct(sums[1:], jnp.float32),
            jax.ShapeDtypeStruct(sums[1:], jnp.bfloat16),
        ),
        in_specs=[SMEM] + [VMEM] * 2,
        out_specs=[VMEM] * 2,
        name="pair",
        compiler_params=params(6),
        cost_estimate=pl.CostEstimate(flops=300_000, bytes_accessed=1_000_000, transcendentals=0),
    )(low_z, keep, got)
    got = lax.ppermute(send, "z_low", [(0, 1), (1, 0)])
    hidden, both = pl.pallas_call(
        hidden_kernel,
        out_shape=(
            jax.ShapeDtypeStruct((units, 128), jnp.bfloat16),
            jax.ShapeDtypeStruct((units + 128, 128), jnp.bfloat16),
        ),
        in_specs=[VMEM] * 3,
        out_specs=[VMEM] * 2,
        name="hidden",
        compiler_params=params(6),
        cost_estimate=pl.CostEstimate(
            flops=1_000_000, bytes_accessed=700_000, transcendentals=60_000
        ),
    )(keep, got, stream_turned)

    both = turned(both)
    stream = pl.pallas_call(
        copy_kernel,
        out_shape=jax.ShapeDtypeStruct((128, 128), jnp.bfloat16),
        in_specs=[VMEM],
        out_specs=VMEM,
        compiler_params=params(1),
    )(both)
    hidden_turned = both[:units]
    upper, lower = over_y_and_x(over_z(hidden_turned), units // 2, two_step_ring)
    other = lax.ppermute(hidden, "core", [(0, 1), (1, 0)])
    near = jnp.stack([hidden, other])
    far = lax.ppermute(near, "z_low", [(0, 1), (1, 0)])
    hessian = pl.pallas_call(
        hessian_kernel,
        out_shape=jax.ShapeDtypeStruct((units, 16 * units), jnp.float32),
        in_specs=[SMEM] * 3 + [VMEM] * 12,
        out_specs=pl.BlockSpec(memory_space=pltpu.HBM),
        scratch_shapes=[
            pltpu.VMEM((units, 4 * LANES), jnp.bfloat16),
            pltpu.VMEM((2, 4 * units, 4 * LANES), jnp.bfloat16),
            pltpu.VMEM((4, units, 4 * units), jnp.float32),
            pltpu.SemaphoreType.DMA((8,)),
        ],
        name="hessian",
        compiler_params=params(14),
        cost_estimate=pl.CostEstimate(flops=822_000_000, bytes_accessed=7_100_000, transcendentals=0),
    )(order, groups, place, near, far, *upper, *lower)
    return (pruned_weight, stream, hessian)


def solution(mesh):
    split = Mesh(mesh.devices.reshape(2, 2, 4, 4, 4), (*DP, *MP))
    return jax.shard_map(
        body,
        mesh=split,
        in_specs=(
            P(DP, MP),
            P(DP, MP),
            P(MP, DP),
            P(MP, None),
            P(None, DP),
            P(MP),
            P(DP, None, MP),
        ),
        out_specs=(P(MP, DP), P(DP, MP), P(MP, DP)),
        check_vma=False,
    )
```
